32 devices in a mesh: data: 32 (over z, y, x, core).
Axes of the slice: x: 2, y: 2, z: 4, core: 2. Of those that a mesh axis runs over, the one named last changes fastest.
Arguments:
- x_in: bfloat16 [32, 384, 1024], P('data')
- grad_y: bfloat16 [32, 384, 1024], P('data')
- gain_one: float32 [2, 1024], replicated
- gain_two: float32 [2, 1024], replicated
- w_qkv: bfloat16 [2, 1024, 3072], replicated
- w_out: bfloat16 [2, 1024, 1024], replicated
- w_up: bfloat16 [2, 1024, 4096], replicated
- w_down: bfloat16 [2, 4096, 1024], replicated
Outputs:
- output 1: bfloat16 [32, 384, 1024], P('data')
- output 2: float32 [2, 1024], replicated
- output 3: float32 [2, 1024], replicated
- output 4: float32 [2, 1024, 3072], replicated
- output 5: float32 [2, 1024, 1024], replicated
- output 6: float32 [2, 1024, 4096], replicated
- output 7: float32 [2, 4096, 1024], replicated
All inputs are finite; a program needn't handle non-finite values.
Results may differ from the reference program's by a relative error of at most 0.02.
Values are sent between devices in bfloat16 or wider.
A program may use at most 1 GiB of HBM per device.

```python
import jax
import jax.numpy as jnp
from jax import lax

D = 1024
FF = 4096
HEADS = 16
LAYERS = 2
SEQ = 384
BATCH = 32
GROUP = 32
HEAD_DIM = D // HEADS
NORM_EPS = 1e-6


def setup_inputs(seed: int = 0) -> dict:
    root_key = jax.random.key(seed)
    sub_keys = jax.random.split(root_key, 8)
    x_in = jax.random.normal(sub_keys[0], (BATCH, SEQ, D), jnp.float32)
    grad_y = jax.random.normal(sub_keys[1], (BATCH, SEQ, D), jnp.float32)
    gain_one = 1.0 + 0.3 * jax.random.normal(sub_keys[2], (LAYERS, D), jnp.float32)
    gain_two = 1.0 + 0.3 * jax.random.normal(sub_keys[3], (LAYERS, D), jnp.float32)
    w_qkv = jax.random.normal(sub_keys[4], (LAYERS, D, 3 * D), jnp.float32) * D ** -0.5
    w_out = jax.random.normal(sub_keys[5], (LAYERS, D, D), jnp.float32) * D ** -0.5
    w_up = jax.random.normal(sub_keys[6], (LAYERS, D, FF), jnp.float32) * D ** -0.5
    w_down = jax.random.normal(sub_keys[7], (LAYERS, FF, D), jnp.float32) * FF ** -0.5
    return {'x_in': x_in.astype(jnp.bfloat16), 'grad_y': grad_y.astype(jnp.bfloat16), 'gain_one': gain_one, 'gain_two': gain_two, 'w_qkv': w_qkv.astype(jnp.bfloat16), 'w_out': w_out.astype(jnp.bfloat16), 'w_up': w_up.astype(jnp.bfloat16), 'w_down': w_down.astype(jnp.bfloat16)}


def rms_gain(rows_f, gain_vec):
    return rows_f * lax.rsqrt(jnp.mean(rows_f * rows_f, axis=-1, keepdims=True) + NORM_EPS) * gain_vec


def gelu_tanh(pre_act):
    return jax.nn.gelu(pre_act, approximate=True)


def mat_lo(lhs_mat, rhs_mat):
    return jnp.dot(lhs_mat, rhs_mat, preferred_element_type=jnp.float32).astype(jnp.bfloat16)


def mat_nt(lhs_mat, rhs_mat):
    return lax.dot_general(lhs_mat, rhs_mat, (((1,), (1,)), ((), ())), preferred_element_type=jnp.float32).astype(jnp.bfloat16)


def mat_tn(lhs_mat, rhs_mat):
    return lax.dot_general(lhs_mat, rhs_mat, (((0,), (0,)), ((), ())), preferred_element_type=jnp.float32)


def head_mix(einsum_spec, lhs_arr, rhs_arr):
    return jnp.einsum(einsum_spec, lhs_arr.astype(jnp.float32), rhs_arr.astype(jnp.float32))


def seq_forward(seq_rows, gain_a, gain_b, w_qkv, w_out, w_up):
    norm_a, norm_a_back = jax.vjp(rms_gain, seq_rows.astype(jnp.float32), gain_a)
    u_one = norm_a.astype(jnp.bfloat16)
    qkv_lo = mat_lo(u_one, w_qkv)
    q_all = qkv_lo[:, :D].reshape(SEQ, HEADS, HEAD_DIM)
    k_all = qkv_lo[:, D:2 * D].reshape(SEQ, HEADS, HEAD_DIM)
    v_all = qkv_lo[:, 2 * D:].reshape(SEQ, HEADS, HEAD_DIM)
    scores = head_mix('qhe,khe->hqk', q_all, k_all) * HEAD_DIM ** -0.5
    causal = jnp.arange(SEQ)[:, None] >= jnp.arange(SEQ)[None, :]
    prob_full = jax.nn.softmax(jnp.where(causal, scores, -1e30), axis=-1)
    prob_lo = prob_full.astype(jnp.bfloat16)
    attn_out = head_mix('hqk,khe->qhe', prob_lo, v_all).astype(jnp.bfloat16).reshape(SEQ, D)
    hidden = seq_rows + mat_lo(attn_out, w_out)
    norm_b, norm_b_back = jax.vjp(rms_gain, hidden.astype(jnp.float32), gain_b)
    u_two = norm_b.astype(jnp.bfloat16)
    pre_lo = mat_lo(u_two, w_up)
    act_f, gelu_back = jax.vjp(gelu_tanh, pre_lo.astype(jnp.float32))
    act_lo = act_f.astype(jnp.bfloat16)
    saved_vals = (norm_a_back, u_one, q_all, k_all, v_all, prob_full, prob_lo, attn_out, norm_b_back, u_two, gelu_back, act_lo)
    return hidden, act_lo, saved_vals


def seq_backward(grad_blk, saved_vals, w_qkv, w_out, w_up, w_down):
    (norm_a_back, u_one, q_all, k_all, v_all, prob_full, prob_lo, attn_out, norm_b_back, u_two, gelu_back, act_lo) = saved_vals
    grad_down_w = mat_tn(act_lo, grad_blk)
    grad_act = mat_nt(grad_blk, w_down)
    (grad_pre_f,) = gelu_back(grad_act.astype(jnp.float32))
    grad_pre = grad_pre_f.astype(jnp.bfloat16)
    grad_up_w = mat_tn(u_two, grad_pre)
    grad_u_two = mat_nt(grad_pre, w_up)
    grad_h_norm, grad_gain_b = norm_b_back(grad_u_two.astype(jnp.float32))
    grad_hidden = (grad_blk.astype(jnp.float32) + grad_h_norm).astype(jnp.bfloat16)
    grad_out_w = mat_tn(attn_out, grad_hidden)
    grad_attn = mat_nt(grad_hidden, w_out).reshape(SEQ, HEADS, HEAD_DIM)
    grad_probs = head_mix('qhe,khe->hqk', grad_attn, v_all)
    grad_scores = (prob_full * (grad_probs - jnp.sum(prob_full * grad_probs, axis=-1, keepdims=True)) * HEAD_DIM ** -0.5).astype(jnp.bfloat16)
    grad_v = head_mix('hqk,qhe->khe', prob_lo, grad_attn).astype(jnp.bfloat16)
    grad_q = head_mix('hqk,khe->qhe', grad_scores, k_all).astype(jnp.bfloat16)
    grad_k = head_mix('hqk,qhe->khe', grad_scores, q_all).astype(jnp.bfloat16)
    grad_qkv = jnp.concatenate([grad_q.reshape(SEQ, D), grad_k.reshape(SEQ, D), grad_v.reshape(SEQ, D)], axis=-1)
    grad_qkv_w = mat_tn(u_one, grad_qkv)
    grad_u_one = mat_nt(grad_qkv, w_qkv)
    grad_x_norm, grad_gain_a = norm_a_back(grad_u_one.astype(jnp.float32))
    grad_x_blk = (grad_hidden.astype(jnp.float32) + grad_x_norm).astype(jnp.bfloat16)
    return grad_x_blk, (grad_gain_a, grad_gain_b, grad_qkv_w, grad_out_w, grad_up_w, grad_down_w)


def reference(x_in, grad_y, gain_one, gain_two, w_qkv, w_out, w_up, w_down):
    def one_seq(grad_acc, seq_pair):
        seq_rows, seq_grad = seq_pair
        hidden_x = seq_rows
        saved_all = []
        for layer_idx in range(LAYERS):
            hidden, act_lo, saved_vals = seq_forward(hidden_x, gain_one[layer_idx], gain_two[layer_idx], w_qkv[layer_idx], w_out[layer_idx], w_up[layer_idx])
            saved_all.append(saved_vals)
            if layer_idx + 1 < LAYERS:
                hidden_x = hidden + mat_lo(act_lo, w_down[layer_idx])
        grad_cur = seq_grad
        grads_rev = []
        for layer_idx in reversed(range(LAYERS)):
            grad_cur, layer_grads = seq_backward(grad_cur, saved_all[layer_idx], w_qkv[layer_idx], w_out[layer_idx], w_up[layer_idx], w_down[layer_idx])
            grads_rev.append(layer_grads)
        grads_fwd = grads_rev[::-1]
        new_acc = tuple(grad_acc[grad_idx] + jnp.stack([layer_set[grad_idx] for layer_set in grads_fwd]) for grad_idx in range(6))
        return new_acc, grad_cur

    init_acc = (jnp.zeros((LAYERS, D), jnp.float32), jnp.zeros((LAYERS, D), jnp.float32), jnp.zeros((LAYERS, D, 3 * D), jnp.float32), jnp.zeros((LAYERS, D, D), jnp.float32), jnp.zeros((LAYERS, D, FF), jnp.float32), jnp.zeros((LAYERS, FF, D), jnp.float32))
    grad_sums, grad_x = lax.scan(one_seq, init_acc, (x_in, grad_y))
    return (grad_x, grad_sums[0] / GROUP, grad_sums[1] / GROUP, grad_sums[2] / GROUP, grad_sums[3] / GROUP, grad_sums[4] / GROUP, grad_sums[5] / GROUP)
```

```python
import functools

import jax
import jax.numpy as jnp
from jax import lax
from jax.experimental import pallas as pl
from jax.experimental.pallas import tpu as pltpu
from jax.sharding import PartitionSpec as P

NORM_EPS = 1e-6
HEAD_DIM = 64
AXIS = 'data'
CHUNKS = ((3, 1, 0), (0, 1, 0), (1, 1, 0), (2, 1, 0), (3, 1, 1), (0, 1, 1), (1, 1, 1), (0, 0, 0), (1, 0, 0), (2, 0, 0), (3, 0, 0), (0, 0, 1), (1, 0, 1), (3, 0, 1))
ORDER = (0, 10, 1, 20, 11, 30, 2, 31, 40, 21, 50, 3, 12, 41, 60, 51, 70, 32, 13, 4, 61, 80, 22, 5, 33, 71, 90, 6, 42, 100, 81, 14, 91, 110, 52, 23, 7, 101, 120, 8, 43, 15, 62, 34, 111, 130, 53, 16, 35, 72, 63, 24, 92, 121, 17, 18, 73, 54, 36, 26, 82, 44, 131, 93, 37, 38, 102, 55, 64, 112, 45, 25, 83, 46, 66, 122, 103, 74, 56, 132, 94, 113, 27, 28, 75, 47, 48, 65, 57, 58, 123, 95, 133, 84, 76, 114, 96, 86, 67, 68, 124, 77, 78, 115, 104, 97, 98, 106, 85, 126, 105, 116, 87, 107, 88, 108, 134, 125, 136, 135, 117, 127, 118, 128, 137, 138)


def rms_gain(rows_f, gain_vec):
    return rows_f * lax.rsqrt(jnp.mean(rows_f * rows_f, axis=-1, keepdims=True) + NORM_EPS) * gain_vec


def gelu_tanh(pre_act):
    return jax.nn.gelu(pre_act, approximate=True)


def mix_lo(einsum_spec, lhs_arr, rhs_arr):
    return jnp.einsum(einsum_spec, lhs_arr, rhs_arr, preferred_element_type=jnp.float32).astype(jnp.bfloat16)


def mix_f32(einsum_spec, lhs_arr, rhs_arr):
    return jnp.einsum(einsum_spec, lhs_arr, rhs_arr, preferred_element_type=jnp.float32)


def block_forward(x_blk, gain_a, gain_b, w_qkv, w_out, w_up):
    seq_len, width = x_blk.shape
    head_shape = (seq_len, width // HEAD_DIM, HEAD_DIM)
    norm_a, norm_a_back = jax.vjp(rms_gain, x_blk.astype(jnp.float32), gain_a)
    u_one = norm_a.astype(jnp.bfloat16)
    qkv_lo = mix_lo('sd,de->se', u_one, w_qkv)
    q_all = qkv_lo[:, :width].reshape(head_shape)
    k_all = qkv_lo[:, width:2 * width].reshape(head_shape)
    v_all = qkv_lo[:, 2 * width:].reshape(head_shape)
    scores = mix_f32('qhe,khe->hqk', q_all, k_all) * HEAD_DIM ** -0.5
    causal = jnp.arange(seq_len)[:, None] >= jnp.arange(seq_len)[None, :]
    prob_full = jax.nn.softmax(jnp.where(causal, scores, -1e30), axis=-1)
    prob_lo = prob_full.astype(jnp.bfloat16)
    attn_out = mix_lo('hqk,khe->qhe', prob_lo, v_all).reshape(seq_len, width)
    hidden = x_blk + mix_lo('sd,de->se', attn_out, w_out)
    norm_b, norm_b_back = jax.vjp(rms_gain, hidden.astype(jnp.float32), gain_b)
    u_two = norm_b.astype(jnp.bfloat16)
    pre_lo = mix_lo('sd,df->sf', u_two, w_up)
    act_f, gelu_back = jax.vjp(gelu_tanh, pre_lo.astype(jnp.float32))
    act_lo = act_f.astype(jnp.bfloat16)
    saved_vals = (norm_a_back, u_one, q_all, k_all, v_all, prob_full, prob_lo, attn_out, norm_b_back, u_two, gelu_back, act_lo)
    return hidden, act_lo, saved_vals


class Place:
    def __init__(self, n_dev):
        me = lax.axis_index(AXIS)
        self.core = me % 2
        self.x = (me // 2) % 2
        self.y = (me // 4) % 2
        self.swap = {name: [(i, i ^ bit) for i in range(n_dev)] for name, bit in (('core', 1), ('x', 2), ('y', 4))}

    def at(self, name):
        return {'core': self.core, 'x': self.x, 'y': self.y}[name]


def send(val, pairs):
    return lax.ppermute(val, AXIS, pairs)


def part(val, which, count, axis):
    size = val.shape[axis] // count
    return lax.dynamic_slice_in_dim(val, which * size, size, axis)


def chip_group_sum(place, color, split, lhs, rhs):
    wide, thin = (lhs, rhs) if split == 0 else (rhs, lhs)
    mine, mate = place.at(color), place.core
    wide_in = send(part(wide, 1 - mine, 2, 1), place.swap[color])
    thin_in = send(thin, place.swap[color])
    wide_two = jnp.concatenate([part(wide, mine, 2, 1), wide_in], axis=0)
    thin_two = jnp.concatenate([thin, thin_in], axis=0)
    wide_core = send(part(wide_two, 1 - mate, 2, 1), place.swap['core'])
    thin_core = send(thin_two, place.swap['core'])
    wide_own = part(wide_two, mate, 2, 1)

    def prod(wide_v, thin_v):
        return mix_f32('sm,sn->mn', wide_v, thin_v) if split == 0 else mix_f32('sn,sm->nm', thin_v, wide_v)
    return prod(wide_own, thin_two) + prod(wide_core, thin_core)


MATRICES = (
    (1024, 1024, 2, 'x', 0, False),
    (1024, 1024, 2, 'y', 1, False),
    (256, 1024, 1, 'x', 0, False),
    (1024, 768, 2, 'y', 1, True),
)
N_SEMS = 16
ADD_ROWS = 32


def add_rows(dst, src, cols, scale=None):
    rows = dst.shape[0]

    @pl.loop(0, rows // ADD_ROWS)
    def _(step):
        at = pl.ds(pl.multiple_of(step * ADD_ROWS, ADD_ROWS), ADD_ROWS)
        val = dst[at, cols] + src[at, :]
        dst[at, cols] = val if scale is None else val * scale


def flip(bit, by):
    return 1 - bit if by else bit


def combine_kernel(n_dev, n_layers, *refs):
    n_in = n_layers * len(MATRICES)
    n_chunk = len(CHUNKS)
    part_refs, gain_in = refs[:n_in], refs[n_in]
    outs, gain_out = refs[n_in + 1:n_in + 5], refs[n_in + 5]
    scratch = refs[n_in + 6:]
    own, land_q, land_z, land_h = (scratch[i * n_chunk:(i + 1) * n_chunk] for i in range(4))
    gain_buf, gain_land, send_sems, recv_sems, local_sems, gain_send, gain_recv = scratch[4 * n_chunk:]

    me = lax.axis_index(AXIS)
    core, x_at, y_at, z_at = lax.rem(me, 2), lax.rem(lax.div(me, 2), 2), lax.rem(lax.div(me, 4), 2), lax.div(me, 8)
    half = lax.div(z_at, 2)
    middle = lax.div(z_at + 1, 2) == 1
    edge = lax.div(z_at + 1, 2) != 1
    place = {'x': x_at, 'y': y_at}
    to = {'core': me + 1 - 2 * core, 'x': me + 2 * (1 - 2 * x_at), 'y': me + 4 * (1 - 2 * y_at),
          'mid': me + 8 * (1 - 2 * half), 'end': me - 8 * (1 - 2 * half)}

    def remote(src, dst, i, sem, dev):
        return pltpu.make_async_remote_copy(src_ref=src, dst_ref=dst, send_sem=send_sems.at[i, sem], recv_sem=recv_sems.at[i, sem],
                                            device_id=(dev,), device_id_type=pl.DeviceIdType.MESH)

    def out_block(i, p_at, c_at, q_at, h_at):
        mat, layer, k = CHUNKS[i]
        rows_all, cols, count, _, split, _ = MATRICES[mat]
        rows = rows_all // count
        row = k * rows
        col = 0
        if split == 0:
            row = row + (p_at * 2 + c_at) * rows_all
        else:
            col = (p_at * 2 + c_at) * cols
        n_rows, n_cols = rows, cols
        if q_at is not None:
            n_rows = rows // 2
            row = row + q_at * n_rows
        if h_at is not None:
            n_cols = cols // 2
            col = col + h_at * n_cols
        if not isinstance(row, int):
            row = pl.multiple_of(row, 8)
        if not isinstance(col, int):
            col = pl.multiple_of(col, 128)
        return outs[mat].at[layer, pl.ds(row, n_rows), pl.ds(col, n_cols)]

    def run(i, stage, pending):
        mat, layer, k = CHUNKS[i]
        rows_all, cols, count, p_name, _, z_last = MATRICES[mat]
        q_name = 'y' if p_name == 'x' else 'x'
        p_at, q_at = place[p_name], place[q_name]
        rows = rows_all // count
        part = part_refs[layer * len(MATRICES) + mat]

        def go(src, dst, sem, dest, cond=None):
            remote(src(), dst(), i, sem, to[dest]).start()
            pending.append((cond, src, i, sem))

        def block(dp=0, dq=0, dc=0, dh=None, q_whole=False):
            return lambda: out_block(i, flip(p_at, dp), flip(core, dc), None if q_whole else flip(q_at, dq), None if dh is None else flip(half, dh))

        def pass_on(blk, sems, cond=None):
            for dest, sem in sems:
                go(blk, blk, sem, dest, cond)

        def arrived(blk, sem):
            remote(blk(), blk(), i, sem, me).wait_recv()

        def half_cols(h):
            return pl.ds(pl.multiple_of(h * (cols // 2), 128), cols // 2)

        def own_half(by):
            return lambda: own[i].at[:, half_cols(flip(half, by))]

        def rows_of(q):
            return lambda: part.at[pl.ds(pl.multiple_of(k * rows + q * (rows // 2), 8), rows // 2), :]

        def load():
            return pltpu.make_async_copy(rows_of(q_at)(), own[i], local_sems.at[i, 0])

        def keep():
            return pltpu.make_async_copy(own_half(0)(), block(dh=0)(), local_sems.at[i, 1])

        def whole(buf):
            return lambda: buf[i]
        if stage == 0:
            go(rows_of(1 - q_at), whole(land_q), 0, q_name)
            load().start()
        elif stage == 1:
            load().wait()
            arrived(whole(land_q), 0)
            add_rows(own[i], land_q[i], slice(None))

            @pl.when(edge)
            def _():
                go(whole(own), whole(land_z), 1, 'mid', edge)
        elif stage == 2:
            @pl.when(middle)
            def _():
                arrived(whole(land_z), 1)
                add_rows(own[i], land_z[i], slice(None))
                go(own_half(1), whole(land_h), 2, 'mid', middle)
        elif stage == 3:
            @pl.when(middle)
            def _():
                arrived(whole(land_h), 2)
                add_rows(own[i], land_h[i], half_cols(half), 1.0 / n_dev)
                keep().start()
                go(own_half(0), block(dh=0), 3, q_name if z_last else 'mid', middle)
        elif not z_last:
            if stage == 4:
                @pl.when(middle)
                def _():
                    keep().wait()
                    arrived(block(dh=1), 3)
                    pass_on(block(), (('end', 4),), middle)

                @pl.when(edge)
                def _():
                    arrived(block(), 4)
                pass_on(block(), ((q_name, 5), (p_name, 6), ('core', 8)))
            elif stage == 5:
                arrived(block(dq=1), 5)
                pass_on(block(dq=1), ((p_name, 7), ('core', 9)))
            elif stage == 6:
                arrived(block(dp=1), 6)
                pass_on(block(dp=1), (('core', 10),))
            elif stage == 7:
                arrived(block(dp=1, dq=1), 7)
                pass_on(block(dp=1, dq=1), (('core', 11),))
            else:
                for dp in range(2):
                    for dq in range(2):
                        arrived(block(dp=dp, dq=dq, dc=1), 8 + 2 * dp + dq)
        else:
            spots = {4: dict(dp=0, dh=0), 5: dict(dp=1, dh=0), 6: dict(dp=0, dh=1), 7: dict(dp=1, dh=1)}
            if stage < 8:
                blk = block(q_whole=True, **spots[stage])
                onward = {4: ((p_name, 4), ('mid', 5), ('end', 7)), 5: (('mid', 6), ('end', 8)), 6: (('end', 9),), 7: (('end', 10),)}[stage]

                @pl.when(middle)
                def _():
                    if stage == 4:
                        keep().wait()
                        arrived(block(dq=1, dh=0), 3)
                    else:
                        arrived(blk, stage - 1)
                    pass_on(blk, onward, middle)

                @pl.when(edge)
                def _():
                    arrived(blk, stage + 3)
                pass_on(blk, (('core', stage + 7),))
            else:
                for order, spot in enumerate((spots[4], spots[5], spots[6], spots[7])):
                    arrived(block(q_whole=True, dc=1, **spot), 11 + order)

    gain_steps = ('core', 'x', 'y', 'mid', 'far')
    far = lax.rem(z_at + 2, 4)
    gain_to = dict(to, mid=me + 8 * (1 - 2 * lax.rem(z_at, 2)), far=me + 8 * (far - z_at))

    def gain_copy(step):
        return pltpu.make_async_remote_copy(src_ref=gain_buf.at[step], dst_ref=gain_land.at[step], send_sem=gain_send.at[step],
                                            recv_sem=gain_recv.at[step], device_id=(gain_to[gain_steps[step]],), device_id_type=pl.DeviceIdType.MESH)

    def gain_next(step):
        copy = gain_copy(step)
        copy.wait()
        total = gain_buf[step] + gain_land[step]
        if step + 1 < len(gain_steps):
            gain_buf[step + 1] = total
            gain_copy(step + 1).start()
        else:
            gain_out[...] = total * (1.0 / n_dev)

    pending = []
    gain_buf[0] = gain_in[...]
    step = 0
    for count, code in enumerate(ORDER):
        run(code // 10, code % 10, pending)
        if count == 1:
            gain_copy(0).start()
        if count >= 8 and count % 6 == 0 and step < len(gain_steps):
            gain_next(step)
            step += 1
    for cond, src, i, sem in pending:
        def finish(src=src, i=i, sem=sem):
            remote(src(), src(), i, sem, me).wait_send()
        if cond is None:
            finish()
        else:
            pl.when(cond)(finish)


def combine(part_sums, gains, n_dev, n_layers):
    f32 = jnp.float32
    outs = []
    for rows, cols, _, _, split, _ in MATRICES:
        outs.append(jax.ShapeDtypeStruct((n_layers, rows * (4 if split == 0 else 1), cols * (4 if split == 1 else 1)), f32))
    outs.append(jax.ShapeDtypeStruct(gains.shape, f32))
    halves = [(MATRICES[mat][0] // MATRICES[mat][2] // 2, MATRICES[mat][1]) for mat, _, _ in CHUNKS]
    scratch = [pltpu.VMEM(s, f32) for _ in range(3) for s in halves] + [pltpu.VMEM((r, c // 2), f32) for r, c in halves]
    n_chunk = len(CHUNKS)
    scratch += [pltpu.VMEM((5,) + gains.shape, f32), pltpu.VMEM((5,) + gains.shape, f32),
                pltpu.SemaphoreType.DMA((n_chunk, N_SEMS)), pltpu.SemaphoreType.DMA((n_chunk, N_SEMS)), pltpu.SemaphoreType.DMA((n_chunk, 2)),
                pltpu.SemaphoreType.DMA((5,)), pltpu.SemaphoreType.DMA((5,))]
    hbm, vmem = pl.BlockSpec(memory_space=pl.ANY), pl.BlockSpec(memory_space=pltpu.VMEM)
    return pl.pallas_call(
        functools.partial(combine_kernel, n_dev, n_layers),
        out_shape=tuple(outs),
        in_specs=[hbm] * len(part_sums) + [vmem],
        out_specs=tuple([hbm] * 4 + [vmem]),
        scratch_shapes=scratch,
        compiler_params=pltpu.CompilerParams(has_side_effects=True, vmem_limit_bytes=60 * 1024 * 1024),
    )(*part_sums, gains)


def solution(mesh):
    n_dev = mesh.shape[AXIS]

    def local_step(x_loc, grad_y_loc, gain_one, gain_two, w_qkv, w_out, w_up, w_down):
        place = Place(n_dev)
        n_layers = w_qkv.shape[0]
        hidden_x = x_loc[0]
        saved_all = []
        for layer_idx in range(n_layers):
            hidden, act_lo, saved_vals = block_forward(hidden_x, gain_one[layer_idx], gain_two[layer_idx], w_qkv[layer_idx], w_out[layer_idx], w_up[layer_idx])
            saved_all.append(saved_vals)
            if layer_idx + 1 < n_layers:
                hidden_x = hidden + mix_lo('sf,fd->sd', act_lo, w_down[layer_idx])
        part_sums = [None] * (n_layers * len(MATRICES))

        def reduce_grad(mat, layer_idx, lhs, rhs):
            _, _, _, color, split, _ = MATRICES[mat]
            part_sums[layer_idx * len(MATRICES) + mat] = chip_group_sum(place, color, split, lhs, rhs)

        gain_grads = [None] * (2 * n_layers)
        grad_blk = grad_y_loc[0]
        for layer_idx in reversed(range(n_layers)):
            (norm_a_back, u_one, q_all, k_all, v_all, prob_full, prob_lo, attn_out, norm_b_back, u_two, gelu_back, act_lo) = saved_all[layer_idx]
            seq_len, width = grad_blk.shape
            head_shape = (seq_len, width // HEAD_DIM, HEAD_DIM)
            reduce_grad(0, layer_idx, act_lo, grad_blk)
            grad_act = mix_lo('sd,fd->sf', grad_blk, w_down[layer_idx])
            (grad_pre_f,) = gelu_back(grad_act.astype(jnp.float32))
            grad_pre = grad_pre_f.astype(jnp.bfloat16)
            reduce_grad(1, layer_idx, u_two, grad_pre)
            grad_u_two = mix_lo('sf,df->sd', grad_pre, w_up[layer_idx])
            grad_h_norm, gain_grads[n_layers + layer_idx] = norm_b_back(grad_u_two.astype(jnp.float32))
            grad_hidden = (grad_blk.astype(jnp.float32) + grad_h_norm).astype(jnp.bfloat16)
            reduce_grad(2, layer_idx, attn_out, grad_hidden)
            grad_attn = mix_lo('se,de->sd', grad_hidden, w_out[layer_idx]).reshape(head_shape)
            grad_probs = mix_f32('qhe,khe->hqk', grad_attn, v_all)
            grad_scores = (prob_full * (grad_probs - jnp.sum(prob_full * grad_probs, axis=-1, keepdims=True)) * HEAD_DIM ** -0.5).astype(jnp.bfloat16)
            grad_v = mix_lo('hqk,qhe->khe', prob_lo, grad_attn)
            grad_q = mix_lo('hqk,khe->qhe', grad_scores, k_all)
            grad_k = mix_lo('hqk,qhe->khe', grad_scores, q_all)
            flat_shape = (seq_len, width)
            grad_qkv = jnp.concatenate([grad_q.reshape(flat_shape), grad_k.reshape(flat_shape), grad_v.reshape(flat_shape)], axis=-1)
            reduce_grad(3, layer_idx, u_one, grad_qkv)
            grad_u_one = mix_lo('se,de->sd', grad_qkv, w_qkv[layer_idx])
            grad_x_norm, gain_grads[layer_idx] = norm_a_back(grad_u_one.astype(jnp.float32))
            grad_blk = (grad_hidden.astype(jnp.float32) + grad_x_norm).astype(jnp.bfloat16)
        gains = jnp.concatenate([jnp.stack(gain_grads), jnp.zeros((8 - 2 * n_layers, gain_grads[0].shape[0]), jnp.float32)])
        down, up, out, qkv, gains = combine(part_sums, gains, n_dev, n_layers)
        return (grad_blk[None], gains[:n_layers], gains[n_layers:2 * n_layers], qkv, out, up, down)

    batch_spec = P(AXIS)
    full_spec = P()
    return jax.shard_map(local_step, mesh=mesh, in_specs=(batch_spec, batch_spec) + (full_spec,) * 6, out_specs=(batch_spec,) + (full_spec,) * 6, check_vma=False)
```

```python
import functools

import jax
import jax.numpy as jnp
from jax import lax
from jax.experimental import pallas as pl
from jax.experimental.pallas import tpu as pltpu
from jax.sharding import PartitionSpec as P


NORM_EPS = 1e-6
HEAD_DIM = 64
AXIS = 'data'
CHUNKS = ((3, 1, 0), (1, 1, 0), (0, 0, 0), (1, 1, 1), (1, 1, 2), (2, 1, 0), (0, 1, 0), (3, 0, 0), (3, 0, 1), (1, 1, 3), (3, 1, 1), (1, 0, 0), (0, 0, 1), (2, 0, 0), (1, 0, 1), (0, 1, 1))
ORDER = (
    'a9a0b9c9b0c0d0nfa1hff9e0b1g9f0a2d1h9c1g0h0b2a3e1f1i0j0b3d2h1',
    'b4l9d3g1k0l0c2a4b6i1n9m0d4e2j1n0f2c3a6e3a5h2k1o0d6m1p0b5n1f3',
    'g2l1a7a8d5i2b7h3c4b8p1j2e4g3o1f4k2i3d7c5j3d8c6h4m2e6e5n2k3g4',
    'f6f5i4l2m3j4h6n3h5c7e7c8l3e8p2g5m4o2g6i6p3f7l4f8o3i5j6h7k4h8',
    'j5p4m5n4g7g8k6m6o4l6i7n6i8l5k5j7j8p5p6k7k8m7n5m8o5l7o6n7n8l8',
    'p7o7p8o8',
)


def rms_gain(rows_f, gain_vec):
    return rows_f * lax.rsqrt(jnp.mean(rows_f * rows_f, axis=-1, keepdims=True) + NORM_EPS) * gain_vec


def gelu_tanh(pre_act):
    return jax.nn.gelu(pre_act, approximate=True)


def mix_lo(einsum_spec, lhs_arr, rhs_arr):
    return jnp.einsum(einsum_spec, lhs_arr, rhs_arr, preferred_element_type=jnp.float32).astype(jnp.bfloat16)


def block_forward(x_blk, gain_a, gain_b, w_qkv, w_out, w_up):
    norm_a, norm_a_back = jax.vjp(rms_gain, x_blk.astype(jnp.float32), gain_a)
    u_one = norm_a.astype(jnp.bfloat16)
    qkv_lo = mix_lo('sd,de->se', u_one, w_qkv)
    attn_out = attn_forward(qkv_lo)
    hidden = x_blk + mix_lo('sd,de->se', attn_out, w_out)
    norm_b, norm_b_back = jax.vjp(rms_gain, hidden.astype(jnp.float32), gain_b)
    u_two = norm_b.astype(jnp.bfloat16)
    pre_lo = mix_lo('sd,df->sf', u_two, w_up)
    act_f, gelu_back = jax.vjp(gelu_tanh, pre_lo.astype(jnp.float32))
    act_lo = act_f.astype(jnp.bfloat16)
    saved_vals = (norm_a_back, u_one, qkv_lo, attn_out, norm_b_back, u_two, gelu_back, act_lo)
    return hidden, act_lo, saved_vals


class Place:
    def __init__(self, n_dev):
        me = lax.axis_index(AXIS)
        self.core = me % 2
        self.x = (me // 2) % 2
        self.y = (me // 4) % 2
        self.swap = {name: [(i, i ^ bit) for i in range(n_dev)] for name, bit in (('core', 1), ('x', 2), ('y', 4))}

    def at(self, name):
        return {'core': self.core, 'x': self.x, 'y': self.y}[name]


def send(val, pairs):
    return lax.ppermute(val, AXIS, pairs)


def part(val, which, count, axis):
    size = val.shape[axis] // count
    return lax.dynamic_slice_in_dim(val, which * size, size, axis)


def neighbour_operands(place, axis, split, lhs, rhs):
    away = part(lhs if split == 0 else rhs, 1 - place.at(axis), 2, 1)
    if split == 1:
        away, rhs = lax.optimization_barrier((away, rhs))
    wide, thin = (lhs, rhs) if split == 0 else (rhs, lhs)
    wide_in = send(away, place.swap[axis])
    thin_in = send(thin, place.swap[axis])
    return rhs, (wide, thin, wide_in, thin_in)


PAIR = 2 * HEAD_DIM
Q_BLOCK = 128


def two_heads(rows):
    first = lax.broadcasted_iota(jnp.int32, rows.shape, 1) < HEAD_DIM
    zero = jnp.zeros_like(rows)
    return jnp.concatenate([jnp.where(first, rows, zero), jnp.where(first, zero, rows)], axis=0)


def one_pair(rows):
    half = rows.shape[0] // 2
    first = lax.broadcasted_iota(jnp.int32, (half, PAIR), 1) < HEAD_DIM
    return jnp.where(first, rows[:half], rows[half:])


def dot_f32(lhs, rhs, lhs_dim, rhs_dim):
    return lax.dot_general(lhs, rhs, (((lhs_dim,), (rhs_dim,)), ((), ())), preferred_element_type=jnp.float32)


def softmax_block(q_two, k_rows, block):
    scores = dot_f32(q_two, k_rows, 1, 1) * HEAD_DIM ** -0.5
    row = lax.rem(lax.broadcasted_iota(jnp.int32, scores.shape, 0), Q_BLOCK) + block * Q_BLOCK
    scores = jnp.where(row >= lax.broadcasted_iota(jnp.int32, scores.shape, 1), scores, -1e30)
    weights = jnp.exp(scores - jnp.max(scores, axis=-1, keepdims=True))
    return weights / jnp.sum(weights, axis=-1, keepdims=True)


def attn_forward_kernel(qkv_ref, out_ref):
    seq_len, width = out_ref.shape

    @pl.loop(0, width // PAIR)
    def _(pair):
        def lanes(which):
            return pl.ds(pl.multiple_of(which * width + pair * PAIR, PAIR), PAIR)

        for block in range(seq_len // Q_BLOCK):
            rows, keys = pl.ds(block * Q_BLOCK, Q_BLOCK), pl.ds(0, (block + 1) * Q_BLOCK)
            prob = softmax_block(two_heads(qkv_ref[rows, lanes(0)]), qkv_ref[keys, lanes(1)], block)
            mixed = dot_f32(prob.astype(jnp.bfloat16), qkv_ref[keys, lanes(2)], 1, 0)
            out_ref[rows, lanes(0)] = one_pair(mixed).astype(jnp.bfloat16)


def attn_backward_kernel(qkv_ref, grad_ref, out_ref, k_acc, v_acc):
    seq_len, width = grad_ref.shape

    @pl.loop(0, width // PAIR)
    def _(pair):
        def lanes(which):
            return pl.ds(pl.multiple_of(which * width + pair * PAIR, PAIR), PAIR)

        n_block = seq_len // Q_BLOCK
        for block in reversed(range(n_block)):
            rows, keys = pl.ds(block * Q_BLOCK, Q_BLOCK), pl.ds(0, (block + 1) * Q_BLOCK)
            q_two, g_two = two_heads(qkv_ref[rows, lanes(0)]), two_heads(grad_ref[rows, lanes(0)])
            k_rows = qkv_ref[keys, lanes(1)]
            prob = softmax_block(q_two, k_rows, block)
            grad_prob = dot_f32(g_two, qkv_ref[keys, lanes(2)], 1, 1)
            mean = jnp.sum(prob * grad_prob, axis=-1, keepdims=True)
            grad_s = (prob * (grad_prob - mean) * HEAD_DIM ** -0.5).astype(jnp.bfloat16)
            out_ref[rows, lanes(0)] = one_pair(dot_f32(grad_s, k_rows, 1, 0)).astype(jnp.bfloat16)
            k_part, v_part = dot_f32(grad_s, q_two, 0, 0), dot_f32(prob.astype(jnp.bfloat16), g_two, 0, 0)
            if block == n_block - 1:
                k_acc[...] = k_part
                v_acc[...] = v_part
            else:
                k_acc[keys, :] += k_part
                v_acc[keys, :] += v_part
        out_ref[:, lanes(1)] = k_acc[...].astype(jnp.bfloat16)
        out_ref[:, lanes(2)] = v_acc[...].astype(jnp.bfloat16)


def attn_forward(qkv):
    seq_len, width3 = qkv.shape
    width = width3 // 3
    vmem = pl.BlockSpec(memory_space=pltpu.VMEM)
    return pl.pallas_call(
        attn_forward_kernel, out_shape=jax.ShapeDtypeStruct((seq_len, width), jnp.bfloat16), in_specs=[vmem], out_specs=vmem,
        cost_estimate=pl.CostEstimate(flops=6 * seq_len * seq_len * width, bytes_accessed=8 * seq_len * width, transcendentals=0))(qkv)


def attn_backward(qkv, grad):
    seq_len, width = grad.shape
    vmem = pl.BlockSpec(memory_space=pltpu.VMEM)
    return pl.pallas_call(
        attn_backward_kernel, out_shape=jax.ShapeDtypeStruct(qkv.shape, jnp.bfloat16), in_specs=[vmem, vmem], out_specs=vmem,
        scratch_shapes=[pltpu.VMEM((seq_len, PAIR), jnp.float32)] * 2,
        cost_estimate=pl.CostEstimate(flops=16 * seq_len * seq_len * width, bytes_accessed=14 * seq_len * width, transcendentals=0))(qkv, grad)


MATRICES = (
    (1024, 1024, 'x', 0),
    (1024, 1024, 'y', 1),
    (256, 1024, 'x', 0),
    (1024, 768, 'y', 1),
)
Z_LAST = ((2, 0), (3, 1))

LATE = ((2, 0), (3, 0))
SEQ_LEN = 384
TOKENS = 4 * SEQ_LEN
TILE_ROWS = 256
N_SEMS = 16
ADD_ROWS = 32


def chunk_count(mat, layer):
    return sum(chunk[:2] == (mat, layer) for chunk in CHUNKS)


def add_rows(dst, src, cols, scale=None):
    rows = dst.shape[0]

    @pl.loop(0, rows // ADD_ROWS)
    def _(step):
        at = pl.ds(pl.multiple_of(step * ADD_ROWS, ADD_ROWS), ADD_ROWS)
        val = dst[at, cols] + src[at, :]
        dst[at, cols] = val if scale is None else val * scale


def flip(bit, by):
    return 1 - bit if by else bit


def combine_kernel(n_dev, n_layers, *refs):
    units = [(mat, layer) for layer in range(n_layers) for mat in range(len(MATRICES))]
    n_chunk = len(CHUNKS)
    refs = list(refs)

    def take(count):
        head, refs[:] = refs[:count], refs[count:]
        return head

    given = [take(2 if unit in LATE else 4) for unit in units]
    gain_in, = take(1)
    outs, (gain_out,) = take(len(MATRICES)), take(1)
    from_core, part_refs, from_chip = take(2 * len(units)), take(len(units)), take(2 * len(LATE))
    own, land_q, land_z, land_h = (take(n_chunk) for _ in range(4))
    row_op, col_op, product, gain_buf, gain_land, send_sems, recv_sems, local_sems, gain_send, gain_recv, op_send, op_recv, op_local = refs

    me = lax.axis_index(AXIS)
    core, x_at, y_at, z_at = lax.rem(me, 2), lax.rem(lax.div(me, 2), 2), lax.rem(lax.div(me, 4), 2), lax.div(me, 8)
    half = lax.div(z_at, 2)
    middle = lax.div(z_at + 1, 2) == 1
    edge = lax.div(z_at + 1, 2) != 1
    place = {'x': x_at, 'y': y_at}
    to = {'core': me + 1 - 2 * core, 'x': me + 2 * (1 - 2 * x_at), 'y': me + 4 * (1 - 2 * y_at),
          'mid': me + 8 * (1 - 2 * half), 'end': me - 8 * (1 - 2 * half)}

    def remote(src, dst, i, sem, dev):
        return pltpu.make_async_remote_copy(src_ref=src, dst_ref=dst, send_sem=send_sems.at[i, sem], recv_sem=recv_sems.at[i, sem],
                                            device_id=(dev,), device_id_type=pl.DeviceIdType.MESH)

    def out_block(i, p_at, c_at, q_at, h_at):
        mat, layer, k = CHUNKS[i]
        rows_all, cols, _, split = MATRICES[mat]
        rows = rows_all // chunk_count(mat, layer)
        row = k * rows
        col = 0
        if split == 0:
            row = row + (p_at * 2 + c_at) * rows_all
        else:
            col = (p_at * 2 + c_at) * cols
        n_rows, n_cols = rows, cols
        if q_at is not None:
            n_rows = rows // 2
            row = row + q_at * n_rows
        if h_at is not None:
            n_cols = cols // 2
            col = col + h_at * n_cols
        if not isinstance(row, int):
            row = pl.multiple_of(row, 8)
        if not isinstance(col, int):
            col = pl.multiple_of(col, 128)
        return outs[mat].at[layer, pl.ds(row, n_rows), pl.ds(col, n_cols)]

    def run(i, stage, pending):
        mat, layer, k = CHUNKS[i]
        rows_all, cols, p_name, _ = MATRICES[mat]
        z_last = (mat, layer) in Z_LAST
        q_name = 'y' if p_name == 'x' else 'x'
        p_at, q_at = place[p_name], place[q_name]
        rows = rows_all // chunk_count(mat, layer)
        part = part_refs[layer * len(MATRICES) + mat]

        def go(src, dst, sem, dest, cond=None):
            remote(src(), dst(), i, sem, to[dest]).start()
            pending.append((cond, src, i, sem))

        def block(dp=0, dq=0, dc=0, dh=None, q_whole=False):
            return lambda: out_block(i, flip(p_at, dp), flip(core, dc), None if q_whole else flip(q_at, dq), None if dh is None else flip(half, dh))

        def pass_on(blk, sems, cond=None):
            for dest, sem in sems:
                go(blk, blk, sem, dest, cond)

        def arrived(blk, sem):
            remote(blk(), blk(), i, sem, me).wait_recv()

        def half_cols(h):
            return pl.ds(pl.multiple_of(h * (cols // 2), 128), cols // 2)

        def own_half(by):
            return lambda: own[i].at[:, half_cols(flip(half, by))]

        def rows_of(q):
            return lambda: part.at[pl.ds(pl.multiple_of(k * rows + q * (rows // 2), 8), rows // 2), :]

        def load():
            return pltpu.make_async_copy(rows_of(q_at)(), own[i], local_sems.at[i, 0])

        def keep():
            return pltpu.make_async_copy(own_half(0)(), block(dh=0)(), local_sems.at[i, 1])

        def whole(buf):
            return lambda: buf[i]

        if stage == 0:
            go(rows_of(1 - q_at), whole(land_q), 0, q_name)
            load().start()
        elif stage == 1:
            load().wait()
            arrived(whole(land_q), 0)
            add_rows(own[i], land_q[i], slice(None))

            @pl.when(edge)
            def _():
                go(whole(own), whole(land_z), 1, 'mid', edge)
        elif stage == 2:
            @pl.when(middle)
            def _():
                arrived(whole(land_z), 1)
                add_rows(own[i], land_z[i], slice(None))
                go(own_half(1), whole(land_h), 2, 'mid', middle)
        elif stage == 3:
            @pl.when(middle)
            def _():
                arrived(whole(land_h), 2)
                add_rows(own[i], land_h[i], half_cols(half), 1.0 / n_dev)
                keep().start()
                go(own_half(0), block(dh=0), 3, q_name if z_last else 'mid', middle)
        elif not z_last:
            if stage == 4:
                @pl.when(middle)
                def _():
                    keep().wait()
                    arrived(block(dh=1), 3)
                    pass_on(block(), (('end', 4),), middle)

                @pl.when(edge)
                def _():
                    arrived(block(), 4)

                pass_on(block(), ((q_name, 5), (p_name, 6), ('core', 8)))
            elif stage == 5:
                arrived(block(dq=1), 5)
                pass_on(block(dq=1), ((p_name, 7), ('core', 9)))
            elif stage == 6:
                arrived(block(dp=1), 6)
                pass_on(block(dp=1), (('core', 10),))
            elif stage == 7:
                arrived(block(dp=1, dq=1), 7)
                pass_on(block(dp=1, dq=1), (('core', 11),))
            else:
                for dp in range(2):
                    for dq in range(2):
                        arrived(block(dp=dp, dq=dq, dc=1), 8 + 2 * dp + dq)
        else:
            spots = {4: dict(dp=0, dh=0), 5: dict(dp=1, dh=0), 6: dict(dp=0, dh=1), 7: dict(dp=1, dh=1)}
            if stage < 8:
                blk = block(q_whole=True, **spots[stage])
                onward = {4: ((p_name, 4), ('mid', 5), ('end', 7)), 5: (('mid', 6), ('end', 8)), 6: (('end', 9),), 7: (('end', 10),)}[stage]

                @pl.when(middle)
                def _():
                    if stage == 4:
                        keep().wait()
                        arrived(block(dq=1, dh=0), 3)
                    else:
                        arrived(blk, stage - 1)
                    pass_on(blk, onward, middle)

                @pl.when(edge)
                def _():
                    arrived(blk, stage + 3)

                pass_on(blk, (('core', stage + 7),))
            else:
                for order, spot in enumerate((spots[4], spots[5], spots[6], spots[7])):
                    arrived(block(q_whole=True, dc=1, **spot), 11 + order)

    def unit_sizes(unit):
        rows, cols, p_name, split = MATRICES[unit[0]]
        return (rows, cols, p_name, split) + ((rows, cols) if split == 0 else (cols, rows))

    def operand_copy(u, which, src, dst, dest):
        return pltpu.make_async_remote_copy(src_ref=src, dst_ref=dst, send_sem=op_send.at[u, which], recv_sem=op_recv.at[u, which],
                                            device_id=(to[dest],), device_id_type=pl.DeviceIdType.MESH)

    def operand_copies(u):
        unit = units[u]
        _, _, p_name, split, wide_w, _ = unit_sizes(unit)
        p_at = place[p_name]
        wide, thin = given[u][:2]
        core_wide, core_thin = from_core[2 * u:2 * u + 2]
        if unit in LATE:
            late = LATE.index(unit)
            chip_wide, chip_thin = from_chip[2 * late:2 * late + 2]
        else:
            chip_wide, chip_thin = given[u][2:]
        first, second = pl.ds(0, SEQ_LEN), pl.ds(SEQ_LEN, SEQ_LEN)

        def lanes(at, count):
            return pl.ds(pl.multiple_of(at, 128), count)

        other = 1 - core
        copies = {
            'own': (operand_copy(u, 0, wide.at[:, lanes((p_at * 2 + other) * wide_w, wide_w)], core_wide.at[first, :], 'core'),
                    operand_copy(u, 1, thin, core_thin.at[first, :], 'core')),
            'next': (operand_copy(u, 2, chip_wide.at[:, lanes(other * wide_w, wide_w)], core_wide.at[second, :], 'core'),
                     operand_copy(u, 3, chip_thin, core_thin.at[second, :], 'core')),
        }
        if unit in LATE:
            copies['chip'] = (operand_copy(u, 4, wide.at[:, lanes((1 - p_at) * 2 * wide_w, 2 * wide_w)], chip_wide, p_name),
                              operand_copy(u, 5, thin, chip_thin, p_name))
        wide_op, thin_op = (row_op, col_op) if split == 0 else (col_op, row_op)
        thin_w = thin.shape[1]
        loads = []
        for start, src in ((0, wide.at[:, lanes((p_at * 2 + core) * wide_w, wide_w)]), (SEQ_LEN, chip_wide.at[:, lanes(core * wide_w, wide_w)]),
                           (2 * SEQ_LEN, core_wide)):
            loads.append((src, wide_op.at[pl.ds(start, src.shape[0]), pl.ds(0, wide_w)]))
        for start, src in ((0, thin), (SEQ_LEN, chip_thin), (2 * SEQ_LEN, core_thin)):
            loads.append((src, thin_op.at[pl.ds(start, src.shape[0]), pl.ds(0, thin_w)]))
        copies['load'] = tuple(pltpu.make_async_copy(src, dst, op_local.at[u, n]) for n, (src, dst) in enumerate(loads))
        return copies

    def start_operands(u):
        copies = operand_copies(u)
        if units[u] in LATE:
            for copy in copies['chip']:
                copy.start()
        for copy in copies['own']:
            copy.start()
        if units[u] not in LATE:
            for copy in copies['next']:
                copy.start()

    def forward_operands(u):
        copies = operand_copies(u)
        for copy in copies['chip']:
            copy.wait_recv()
        for copy in copies['next']:
            copy.start()

    def multiply(u):
        rows, cols, _, _, _, _ = unit_sizes(units[u])
        copies = operand_copies(u)
        for copy in copies['own'] + copies['next']:
            copy.wait_recv()
        for copy in copies['load']:
            copy.start()
        for copy in copies['load']:
            copy.wait()
        tile = min(TILE_ROWS, rows)
        half_w = cols // 2

        @pl.loop(0, rows // tile)
        def _(step):
            at = pl.ds(pl.multiple_of(step * tile, tile), tile)
            for side in range(2):
                lanes = pl.ds(side * half_w, half_w)
                product[at, lanes] = dot_f32(row_op[:, at], col_op[:, lanes], 0, 0)

        store = pltpu.make_async_copy(product.at[pl.ds(0, rows), pl.ds(0, cols)], part_refs[u], op_local.at[u, 6])
        store.start()
        store.wait()

    def finish_operands(u):
        copies = operand_copies(u)
        for copy in copies['own'] + copies['next'] + copies.get('chip', ()):
            copy.wait_send()

    gain_steps = ('core', 'x', 'y', 'mid', 'far')
    far = lax.rem(z_at + 2, 4)
    gain_to = dict(to, mid=me + 8 * (1 - 2 * lax.rem(z_at, 2)), far=me + 8 * (far - z_at))

    def gain_copy(step):
        return pltpu.make_async_remote_copy(src_ref=gain_buf.at[step], dst_ref=gain_land.at[step], send_sem=gain_send.at[step],
                                            recv_sem=gain_recv.at[step], device_id=(gain_to[gain_steps[step]],), device_id_type=pl.DeviceIdType.MESH)

    def gain_next(step):
        copy = gain_copy(step)
        copy.wait()
        total = gain_buf[step] + gain_land[step]
        if step + 1 < len(gain_steps):
            gain_buf[step + 1] = total
            gain_copy(step + 1).start()
        else:
            gain_out[...] = total * (1.0 / n_dev)

    pending = []
    gain_buf[0] = gain_in[...]
    step = 0
    first_use = []
    for mat, layer, _ in CHUNKS:
        if units.index((mat, layer)) not in first_use:
            first_use.append(units.index((mat, layer)))
    for u in first_use:
        start_operands(u)
    for count, (letter, digit) in enumerate(zip(*[iter(''.join(ORDER))] * 2)):
        i, stage = ord(letter) - ord('a'), int(digit, 16)
        u = units.index(CHUNKS[i][:2])
        if stage == 9:
            multiply(u)
        elif stage == 15:
            forward_operands(u)
        else:
            run(i, stage, pending)
        if count == 1:
            gain_copy(0).start()
        if count >= 8 and count % 6 == 0 and step < len(gain_steps):
            gain_next(step)
            step += 1
    for u in range(len(units)):
        finish_operands(u)
    for cond, src, i, sem in pending:
        def finish(src=src, i=i, sem=sem):
            remote(src(), src(), i, sem, me).wait_send()

        if cond is None:
            finish()
        else:
            pl.when(cond)(finish)


def combine(operands, gains, n_dev, n_layers):
    f32, bf16 = jnp.float32, jnp.bfloat16
    units = [(mat, layer) for layer in range(n_layers) for mat in range(len(MATRICES))]
    outs = []
    for rows, cols, _, split in MATRICES:
        outs.append(jax.ShapeDtypeStruct((n_layers, rows * (4 if split == 0 else 1), cols * (4 if split == 1 else 1)), f32))
    outs.append(jax.ShapeDtypeStruct(gains.shape, f32))
    widths = [MATRICES[mat][:2] if MATRICES[mat][3] == 0 else MATRICES[mat][1::-1] for mat, _ in units]
    for wide_w, thin_w in widths:
        outs += [jax.ShapeDtypeStruct((2 * SEQ_LEN, wide_w), bf16), jax.ShapeDtypeStruct((2 * SEQ_LEN, thin_w), bf16)]
    outs += [jax.ShapeDtypeStruct(MATRICES[mat][:2], f32) for mat, _ in units]
    for unit in LATE:
        wide_w, thin_w = widths[units.index(unit)]
        outs += [jax.ShapeDtypeStruct((SEQ_LEN, 2 * wide_w), bf16), jax.ShapeDtypeStruct((SEQ_LEN, thin_w), bf16)]
    halves = [(MATRICES[mat][0] // chunk_count(mat, layer) // 2, MATRICES[mat][1]) for mat, layer, _ in CHUNKS]
    scratch = [pltpu.VMEM(s, f32) for _ in range(3) for s in halves] + [pltpu.VMEM((r, c // 2), f32) for r, c in halves]
    n_chunk, n_unit = len(CHUNKS), len(units)
    most_rows, most_cols = max(m[0] for m in MATRICES), max(m[1] for m in MATRICES)
    scratch += [pltpu.VMEM((TOKENS, most_rows), bf16), pltpu.VMEM((TOKENS, most_cols), bf16), pltpu.VMEM((most_rows, most_cols), f32),
                pltpu.VMEM((5,) + gains.shape, f32), pltpu.VMEM((5,) + gains.shape, f32),
                pltpu.SemaphoreType.DMA((n_chunk, N_SEMS)), pltpu.SemaphoreType.DMA((n_chunk, N_SEMS)), pltpu.SemaphoreType.DMA((n_chunk, 2)),
                pltpu.SemaphoreType.DMA((5,)), pltpu.SemaphoreType.DMA((5,)),
                pltpu.SemaphoreType.DMA((n_unit, 6)), pltpu.SemaphoreType.DMA((n_unit, 6)), pltpu.SemaphoreType.DMA((n_unit, 7))]
    hbm, vmem = pl.BlockSpec(memory_space=pl.ANY), pl.BlockSpec(memory_space=pltpu.VMEM)
    flat = [val for group in operands for val in group]
    results = pl.pallas_call(
        functools.partial(combine_kernel, n_dev, n_layers),
        out_shape=tuple(outs),
        in_specs=[hbm] * len(flat) + [vmem],
        out_specs=tuple([hbm] * 4 + [vmem] + [hbm] * (len(outs) - 5)),
        scratch_shapes=scratch,
        compiler_params=pltpu.CompilerParams(has_side_effects=True, vmem_limit_bytes=63 * 1024 * 1024),
    )(*flat, gains)
    return results[:5]


def solution(mesh):
    n_dev = mesh.shape[AXIS]

    def whole_step(x_loc, grad_y_loc, gain_one, gain_two, w_qkv, w_out, w_up, w_down):
        place = Place(n_dev)
        n_layers = w_qkv.shape[0]
        hidden_x = x_loc[0]
        saved_all = []
        for layer_idx in range(n_layers):
            hidden, act_lo, saved_vals = block_forward(hidden_x, gain_one[layer_idx], gain_two[layer_idx], w_qkv[layer_idx], w_out[layer_idx], w_up[layer_idx])
            saved_all.append(saved_vals)
            if layer_idx + 1 < n_layers:
                hidden_x = hidden + mix_lo('sf,fd->sd', act_lo, w_down[layer_idx])
        operands = [None] * (n_layers * len(MATRICES))

        def reduce_grad(mat, layer_idx, lhs, rhs):
            _, _, color, split = MATRICES[mat]
            if (mat, layer_idx) in LATE:
                operands[layer_idx * len(MATRICES) + mat] = (lhs, rhs) if split == 0 else (rhs, lhs)
            else:
                rhs, operands[layer_idx * len(MATRICES) + mat] = neighbour_operands(place, color, split, lhs, rhs)
            return rhs

        gain_grads = [None] * (2 * n_layers)
        grad_blk = grad_y_loc[0]
        for layer_idx in reversed(range(n_layers)):
            (norm_a_back, u_one, qkv_lo, attn_out, norm_b_back, u_two, gelu_back, act_lo) = saved_all[layer_idx]
            grad_blk = reduce_grad(0, layer_idx, act_lo, grad_blk)
            grad_act = mix_lo('sd,fd->sf', grad_blk, w_down[layer_idx])
            (grad_pre_f,) = gelu_back(grad_act.astype(jnp.float32))
            grad_pre = grad_pre_f.astype(jnp.bfloat16)
            grad_pre = reduce_grad(1, layer_idx, u_two, grad_pre)
            grad_u_two = mix_lo('sf,df->sd', grad_pre, w_up[layer_idx])
            grad_h_norm, gain_grads[n_layers + layer_idx] = norm_b_back(grad_u_two.astype(jnp.float32))
            grad_hidden = (grad_blk.astype(jnp.float32) + grad_h_norm).astype(jnp.bfloat16)
            grad_hidden = reduce_grad(2, layer_idx, attn_out, grad_hidden)
            grad_attn = mix_lo('se,de->sd', grad_hidden, w_out[layer_idx])
            grad_qkv = attn_backward(qkv_lo, grad_attn)
            grad_qkv = reduce_grad(3, layer_idx, u_one, grad_qkv)
            grad_u_one = mix_lo('se,de->sd', grad_qkv, w_qkv[layer_idx])
            grad_x_norm, gain_grads[layer_idx] = norm_a_back(grad_u_one.astype(jnp.float32))
            grad_blk = (grad_hidden.astype(jnp.float32) + grad_x_norm).astype(jnp.bfloat16)
        gains = jnp.concatenate([jnp.stack(gain_grads), jnp.zeros((8 - 2 * n_layers, gain_grads[0].shape[0]), jnp.float32)])
        down, up, out, qkv, gains = combine(operands, gains, n_dev, n_layers)
        return (grad_blk[None], gains[:n_layers], gains[n_layers:2 * n_layers], qkv, out, up, down)

    batch_spec = P(AXIS)
    full_spec = P()
    return jax.shard_map(whole_step, mesh=mesh, in_specs=(batch_spec, batch_spec) + (full_spec,) * 6, out_specs=(batch_spec,) + (full_spec,) * 6, check_vma=False)
```

```python
import functools

import jax
import jax.numpy as jnp
from jax import lax
from jax.experimental import pallas as pl
from jax.experimental.pallas import tpu as pltpu
from jax.sharding import PartitionSpec as P


NORM_EPS = 1e-6
HEAD_DIM = 64
AXIS = 'data'
CHUNK_UNITS = '003010111100300001102000313110102101'
ORDER = (
    'a9a0c9d9kaa1c0d0e0baa2c1f0b9b0a3c2f1g0d1a4i9c3h0f2b1i0f3c4e1',
    'k9g1j0k0d2f4a5h1a6d3b2i1m9l0m0c5j1b3e2d4n0c6k1o0f5g2f6b4e3l1',
    'q9p0h2g3a7a8m1q0h3i2e4c7c8j2d5k2g4l2n1f7h4f8r0d6i3b6j3o1k3l3',
    'm2b5o2p1k4e5i4p2j4n2o3m3l4q1p3e6g6n3m4h6r1o4d7n4r2d8p4g5b7r3',
    'b8h5i5r4q2j6q3i6e7q4k5e8l6m5j5o6k7l5n5m7p6o5g7g8p5n7h7h8r6i7',
    'q5i8r5k6q7j7j8m6kel7l8n6mem8o7k8o8p7p8q6ner7n8r8qeq8',
)


class Place:
    def __init__(self, n_dev):
        me = lax.axis_index(AXIS)
        self.core = me % 2
        self.x = (me // 2) % 2
        self.y = (me // 4) % 2
        self.z = (me // 8) % 2
        self.swap = {name: [(i, i ^ bit) for i in range(n_dev)] for name, bit in (('core', 1), ('x', 2), ('y', 4), ('z', 8))}

    def at(self, name):
        return {'core': self.core, 'x': self.x, 'y': self.y, 'z': self.z}[name]


def send(val, pairs):
    return lax.ppermute(val, AXIS, pairs)


def part(val, which, count, axis):
    size = val.shape[axis] // count
    return lax.dynamic_slice_in_dim(val, which * size, size, axis)


def neighbour_operands(place, axis, split, lhs, rhs):
    away = part(lhs if split == 0 else rhs, 1 - place.at(axis), 2, 1)
    wide, thin = (lhs, rhs) if split == 0 else (rhs, lhs)
    wide_in = send(away, place.swap[axis])
    thin_in = send(thin, place.swap[axis])
    return wide, thin, wide_in, thin_in


PAIR = 2 * HEAD_DIM
GROUP = 2 * PAIR
Q_BLOCK = 128
FF_BLOCK = 512
GELU_C = 0.7978845608028654
GELU_D = 0.044715


def dot_with(dims):
    return lambda lhs, rhs: lax.dot_general(lhs, rhs, (dims, ((), ())), preferred_element_type=jnp.float32)


dot_nn, dot_nt, dot_tn = (dot_with(((left,), (right,))) for left, right in ((1, 0), (1, 1), (0, 0)))


def rounded(val):
    return val.astype(jnp.bfloat16)


def inverse_rms(rows_f):
    return lax.rsqrt(jnp.mean(rows_f * rows_f, axis=-1, keepdims=True) + NORM_EPS)


def norm_forward(src, gain, dst):
    @pl.loop(0, src.shape[0] // 64)
    def _(step):
        at = pl.ds(pl.multiple_of(step * 64, 64), 64)
        rows_f = src[at, :].astype(jnp.float32)
        dst[at, :] = (rows_f * inverse_rms(rows_f) * gain[...]).astype(jnp.bfloat16)


def norm_backward(src, gain, grad_norm, grad_res, dst, gain_dst):
    gain_dst[...] = jnp.zeros_like(gain_dst)

    @pl.loop(0, src.shape[0] // 64)
    def _(step):
        at = pl.ds(pl.multiple_of(step * 64, 64), 64)
        rows_f = src[at, :].astype(jnp.float32)
        scale = inverse_rms(rows_f)
        unit = rows_f * scale
        grad = grad_norm[at, :].astype(jnp.bfloat16).astype(jnp.float32)
        gain_dst[...] += jnp.sum(grad * unit, axis=0, keepdims=True)
        grad = grad * gain[...]
        grad = scale * (grad - unit * jnp.mean(grad * unit, axis=-1, keepdims=True))
        dst[at, :] = (grad_res[at, :].astype(jnp.float32) + grad).astype(jnp.bfloat16)


def two_heads(rows):
    first = lax.broadcasted_iota(jnp.int32, rows.shape, 1) < HEAD_DIM
    zero = jnp.zeros_like(rows)
    return jnp.concatenate([jnp.where(first, rows, zero), jnp.where(first, zero, rows)], axis=0)


def one_pair(rows):
    half = rows.shape[0] // 2
    first = lax.broadcasted_iota(jnp.int32, (half, PAIR), 1) < HEAD_DIM
    return jnp.where(first, rows[:half], rows[half:])


def softmax_block(q_two, k_rows, block):
    n_keys = k_rows.shape[0]
    scores = dot_nt(q_two, k_rows) * HEAD_DIM ** -0.5
    last = scores[:, n_keys - Q_BLOCK:]
    row = lax.rem(lax.broadcasted_iota(jnp.int32, last.shape, 0), Q_BLOCK)
    last = jnp.where(row >= lax.broadcasted_iota(jnp.int32, last.shape, 1), last, -1e30)
    scores = last if block == 0 else jnp.concatenate([scores[:, :n_keys - Q_BLOCK], last], axis=1)
    weights = jnp.exp(scores - jnp.max(scores, axis=-1, keepdims=True))
    return weights * (1.0 / jnp.sum(weights, axis=-1, keepdims=True))


def attn_forward_kernel(x_ref, gain_ref, wq_ref, wk_ref, wv_ref, wo_ref, u_ref, q_ref, k_ref, v_ref, o_ref, h_ref, acc):
    step = pl.program_id(0)

    @pl.when(step == 0)
    def _():
        norm_forward(x_ref, gain_ref, u_ref)
        acc[...] = jnp.zeros_like(acc)

    for dst, weight in ((q_ref, wq_ref), (k_ref, wk_ref), (v_ref, wv_ref)):
        dst[...] = rounded(dot_nn(u_ref[...], weight[...]))
    for block in range(x_ref.shape[0] // Q_BLOCK):
        rows, keys = pl.ds(block * Q_BLOCK, Q_BLOCK), pl.ds(0, (block + 1) * Q_BLOCK)
        for pair in range(GROUP // PAIR):
            lanes = pl.ds(pair * PAIR, PAIR)
            prob = softmax_block(two_heads(q_ref[rows, lanes]), k_ref[keys, lanes], block)
            o_ref[rows, lanes] = one_pair(dot_nn(prob.astype(jnp.bfloat16), v_ref[keys, lanes])).astype(jnp.bfloat16)
    acc[...] += dot_nn(o_ref[...], wo_ref[...])

    @pl.when(step == pl.num_programs(0) - 1)
    def _():
        h_ref[...] = x_ref[...] + acc[...].astype(jnp.bfloat16)


def attn_backward_kernel(grad_ref, x_ref, gain_ref, q_ref, k_ref, v_ref, wo_ref, wq_ref, wk_ref, wv_ref, out_ref, dx_ref, dgain_ref, do_ref, k_acc, v_acc, acc):
    step = pl.program_id(0)
    seq_len, width = grad_ref.shape

    @pl.when(step == 0)
    def _():
        acc[...] = jnp.zeros_like(acc)

    do_ref[...] = rounded(dot_nt(grad_ref[...], wo_ref[...]))
    n_block = seq_len // Q_BLOCK

    def dest(which, lane, count):
        return pl.ds(pl.multiple_of(which * width + step * GROUP + lane, PAIR), count)

    for pair in range(GROUP // PAIR):
        lanes = pl.ds(pair * PAIR, PAIR)
        for block in reversed(range(n_block)):
            rows, keys = pl.ds(block * Q_BLOCK, Q_BLOCK), pl.ds(0, (block + 1) * Q_BLOCK)
            q_two, g_two = two_heads(q_ref[rows, lanes]), two_heads(do_ref[rows, lanes])
            k_rows = k_ref[keys, lanes]
            prob = softmax_block(q_two, k_rows, block)
            grad_prob = dot_nt(g_two, v_ref[keys, lanes])
            mean = jnp.sum(prob * grad_prob, axis=-1, keepdims=True)
            grad_s = (prob * (grad_prob - mean) * HEAD_DIM ** -0.5).astype(jnp.bfloat16)
            out_ref[rows, dest(0, pair * PAIR, PAIR)] = one_pair(dot_nn(grad_s, k_rows)).astype(jnp.bfloat16)
            k_part, v_part = dot_tn(grad_s, q_two), dot_tn(prob.astype(jnp.bfloat16), g_two)
            if block == n_block - 1:
                k_acc[:, lanes] = k_part
                v_acc[:, lanes] = v_part
            else:
                k_acc[keys, lanes] += k_part
                v_acc[keys, lanes] += v_part
    out_ref[:, dest(1, 0, GROUP)] = k_acc[...].astype(jnp.bfloat16)
    out_ref[:, dest(2, 0, GROUP)] = v_acc[...].astype(jnp.bfloat16)
    for which, weight in enumerate((wq_ref, wk_ref, wv_ref)):
        acc[...] += dot_nt(out_ref[:, dest(which, 0, GROUP)], weight[...])

    @pl.when(step == pl.num_programs(0) - 1)
    def _():
        norm_backward(x_ref, gain_ref, acc, grad_ref, dx_ref, dgain_ref)


def mlp_forward_kernel(has_down, h_ref, gain_ref, w1_ref, *refs):
    w2_ref, refs = (refs[0], refs[1:]) if has_down else (None, refs)
    u_ref, z_ref, a_ref = refs[:3]

    @pl.when(pl.program_id(0) == 0)
    def _():
        norm_forward(h_ref, gain_ref, u_ref)

    z_ref[...] = rounded(dot_nn(u_ref[...], w1_ref[...]))
    rows_f = z_ref[...].astype(jnp.float32)
    bend = jnp.tanh(GELU_C * (rows_f + GELU_D * (rows_f * rows_f * rows_f)))
    a_ref[...] = (rows_f * (0.5 * (1.0 + bend))).astype(jnp.bfloat16)
    if has_down:
        y_ref, acc = refs[3:]

        @pl.when(pl.program_id(0) == 0)
        def _():
            acc[...] = jnp.zeros_like(acc)

        acc[...] += dot_nn(a_ref[...], w2_ref[...])

        @pl.when(pl.program_id(0) == pl.num_programs(0) - 1)
        def _():
            y_ref[...] = h_ref[...] + acc[...].astype(jnp.bfloat16)


def mlp_backward_kernel(grad_ref, h_ref, gain_ref, z_ref, w2_ref, w1_ref, dz_ref, dh_ref, dgain_ref, acc):
    @pl.when(pl.program_id(0) == 0)
    def _():
        acc[...] = jnp.zeros_like(acc)

    grad_a = rounded(dot_nt(grad_ref[...], w2_ref[...])).astype(jnp.float32)
    rows_f = z_ref[...].astype(jnp.float32)
    square = rows_f * rows_f
    bend = jnp.tanh(GELU_C * (rows_f + GELU_D * (square * rows_f)))
    slope = 0.5 * (1.0 + bend) + (0.5 * GELU_C) * rows_f * (1.0 - bend * bend) * (1.0 + (3.0 * GELU_D) * square)
    dz_ref[...] = (slope * grad_a).astype(jnp.bfloat16)
    acc[...] += dot_nt(dz_ref[...], w1_ref[...])

    @pl.when(pl.program_id(0) == pl.num_programs(0) - 1)
    def _():
        norm_backward(h_ref, gain_ref, acc, grad_ref, dh_ref, dgain_ref)


def whole_spec(shape):
    return pl.BlockSpec(shape, lambda step: (0,) * len(shape))


def cols_spec(rows, cols):
    return pl.BlockSpec((rows, cols), lambda step: (0, step))


def weight_cols(layer, rows, cols, shift=0):
    return pl.BlockSpec((None, rows, cols), lambda step: (layer, 0, shift + step))


def weight_rows(layer, rows, cols):
    return pl.BlockSpec((None, rows, cols), lambda step: (layer, step, 0))


def lo(*shape):
    return jax.ShapeDtypeStruct(shape, jnp.bfloat16)


def block_call(kernel, grid, in_specs, out_specs, out_shape, scratch, flops, *args):
    return pl.pallas_call(kernel, grid=(grid,), in_specs=in_specs, out_specs=out_specs, out_shape=out_shape,
                          scratch_shapes=[pltpu.VMEM(shape, jnp.float32) if isinstance(shape, tuple) else shape for shape in scratch],
                          cost_estimate=pl.CostEstimate(flops=flops, bytes_accessed=flops // 500, transcendentals=0),
                          compiler_params=pltpu.CompilerParams(dimension_semantics=('arbitrary',), vmem_limit_bytes=48 * 1024 * 1024))(*args)


def attn_forward(layer, x_rows, gain, w_qkv, w_out):
    seq_len, width = x_rows.shape
    full, cols, steps = whole_spec((seq_len, width)), cols_spec(seq_len, GROUP), width // GROUP
    weights = [weight_cols(layer, width, GROUP, which * steps) for which in range(3)]
    return block_call(attn_forward_kernel, steps, [full, whole_spec((1, width))] + weights + [weight_rows(layer, GROUP, width)],
                      [full, cols, cols, cols, cols, full], [lo(seq_len, width)] * 6, [(seq_len, width)], 8 * seq_len * width * width,
                      x_rows, gain[None], w_qkv, w_qkv, w_qkv, w_out)


def attn_backward(layer, grad, x_rows, gain, q_rows, k_rows, v_rows, w_qkv, w_out):
    seq_len, width = grad.shape
    full, cols, steps = whole_spec((seq_len, width)), cols_spec(seq_len, GROUP), width // GROUP
    weights = [weight_cols(layer, width, GROUP, which * steps) for which in range(3)]
    return block_call(attn_backward_kernel, steps,
                      [full, full, whole_spec((1, width)), cols, cols, cols, weight_rows(layer, GROUP, width)] + weights,
                      [whole_spec((seq_len, 3 * width)), full, whole_spec((1, width))],
                      [lo(seq_len, 3 * width), lo(seq_len, width), jax.ShapeDtypeStruct((1, width), jnp.float32)],
                      [pltpu.VMEM((seq_len, GROUP), jnp.bfloat16), (seq_len, GROUP), (seq_len, GROUP), (seq_len, width)], 11 * seq_len * width * width,
                      grad, x_rows, gain[None], q_rows, k_rows, v_rows, w_out, w_qkv, w_qkv, w_qkv)


def mlp_forward(layer, h_rows, gain, w_up, w_down, has_down):
    seq_len, width = h_rows.shape
    inner = w_up.shape[2]
    full, cols = whole_spec((seq_len, width)), cols_spec(seq_len, FF_BLOCK)
    more = [weight_rows(layer, FF_BLOCK, width)] if has_down else []
    return block_call(functools.partial(mlp_forward_kernel, has_down), inner // FF_BLOCK, [full, whole_spec((1, width)), weight_cols(layer, width, FF_BLOCK)] + more,
                      [full, cols, cols] + [full] * has_down, [lo(seq_len, width), lo(seq_len, inner), lo(seq_len, inner)] + [lo(seq_len, width)] * has_down,
                      [(seq_len, width)] * has_down, (4 if has_down else 2) * seq_len * width * inner,
                      h_rows, gain[None], w_up, *([w_down] * has_down))


def mlp_backward(layer, grad, h_rows, gain, z_rows, w_up, w_down):
    seq_len, width = grad.shape
    inner = w_up.shape[2]
    full, cols = whole_spec((seq_len, width)), cols_spec(seq_len, FF_BLOCK)
    return block_call(mlp_backward_kernel, inner // FF_BLOCK,
                      [full, full, whole_spec((1, width)), cols, weight_rows(layer, FF_BLOCK, width), weight_cols(layer, width, FF_BLOCK)],
                      [cols, full, whole_spec((1, width))],
                      [lo(seq_len, inner), lo(seq_len, width), jax.ShapeDtypeStruct((1, width), jnp.float32)], [(seq_len, width)], 4 * seq_len * width * inner,
                      grad, h_rows, gain[None], z_rows, w_down, w_up)


MATRICES = ((1024, 1024, 0), (1024, 1024, 1), (256, 1024, 0), (1024, 768, 1))
KIND = ('yyYy', 'xxXX')
LATE = ((2, 0), (3, 0))
SEQ_LEN = 384
TOKENS = 4 * SEQ_LEN
TILE_ROWS = 256
STREAM_ROWS = 64
N_SEMS = 12
ADD_ROWS = 32


def read_chunks(text):
    found = []
    for mat, layer in zip(*[map(int, text)] * 2):
        found.append((mat, layer, sum(chunk[:2] == (mat, layer) for chunk in found)))
    return tuple(found)


CHUNKS = read_chunks(CHUNK_UNITS)


def first_axis(mat, layer):
    kind = KIND[layer][mat]
    return kind if kind in 'xy' else 'z'


def chunk_count(mat, layer):
    return sum(chunk[:2] == (mat, layer) for chunk in CHUNKS)


def add_rows(dst, src, cols, scale=None):
    rows = dst.shape[0]

    @pl.loop(0, rows // ADD_ROWS)
    def _(step):
        at = pl.ds(pl.multiple_of(step * ADD_ROWS, ADD_ROWS), ADD_ROWS)
        val = dst[at, cols] + src[at, :]
        dst[at, cols] = val if scale is None else val * scale


def flip(bit, by):
    return 1 - bit if by else bit


def combine_kernel(n_dev, n_layers, *refs):
    units = [(mat, layer) for layer in range(n_layers) for mat in range(len(MATRICES))]
    n_chunk = len(CHUNKS)
    refs = list(refs)

    def take(count):
        head, refs[:] = refs[:count], refs[count:]
        return head

    given = [take(2 if unit in LATE else 4) for unit in units]
    gain_in, = take(1)
    outs, (gain_out,) = take(len(MATRICES)), take(1)
    from_core, part_refs, from_chip = take(2 * len(units)), take(len(units)), take(2 * len(LATE))
    land_q, land_z, land_h = (take(n_chunk) for _ in range(3))
    row_op, col_op, product, stream, gain_buf, gain_land, send_sems, recv_sems, local_sems, stream_sems, gain_send, gain_recv, op_send, op_recv, op_local = refs

    me = lax.axis_index(AXIS)
    core, x_at, y_at, z_at = lax.rem(me, 2), lax.rem(lax.div(me, 2), 2), lax.rem(lax.div(me, 4), 2), lax.div(me, 8)
    half = lax.div(z_at, 2)
    middle = lax.div(z_at + 1, 2) == 1
    edge = lax.div(z_at + 1, 2) != 1
    place = {'x': x_at, 'y': y_at, 'z': lax.rem(z_at, 2)}
    to = {'core': me + 1 - 2 * core, 'x': me + 2 * (1 - 2 * x_at), 'y': me + 4 * (1 - 2 * y_at),
          'mid': me + 8 * (1 - 2 * half), 'end': me - 8 * (1 - 2 * half),
          'z': me + 8 * (1 - 2 * place['z']), 'far': me + 16 * (1 - 2 * half)}

    def remote(src, dst, i, sem, dev):
        return pltpu.make_async_remote_copy(src_ref=src, dst_ref=dst, send_sem=send_sems.at[i, sem], recv_sem=recv_sems.at[i, sem],
                                            device_id=(dev,), device_id_type=pl.DeviceIdType.MESH)

    def out_block(i, p_at, c_at, row, n_rows, h_at):
        mat, layer, k = CHUNKS[i]
        rows_all, cols, split = MATRICES[mat]
        quarter = p_at * 2 + c_at
        row = row + k * (rows_all // chunk_count(mat, layer)) + (quarter * rows_all if split == 0 else 0)
        col, n_cols = (0, cols) if h_at is None else (h_at * (cols // 2), cols // 2)
        if split == 1:
            col = col + quarter * cols
        return outs[mat].at[layer, pl.ds(pl.multiple_of(row, 8), n_rows), pl.ds(col if isinstance(col, int) else pl.multiple_of(col, 128), n_cols)]

    def stream_add(dst, src):
        rows, cols = dst.shape
        size = min(STREAM_ROWS, rows)
        steps = rows // size

        def fetch(step, slot):
            return pltpu.make_async_copy(src.at[pl.ds(pl.multiple_of(step * size, size), size), :], stream.at[slot, pl.ds(0, size), pl.ds(0, cols)], stream_sems.at[slot])

        fetch(0, 0).start()

        @pl.loop(0, steps)
        def _(step):
            slot = lax.rem(step, 2)

            @pl.when(step + 1 < steps)
            def _():
                fetch(step + 1, 1 - slot).start()

            fetch(step, slot).wait()
            at = pl.ds(pl.multiple_of(step * size, size), size)
            dst[at, :] = dst[at, :] + stream[slot, pl.ds(0, size), pl.ds(0, cols)]

    def run(i, stage, pending):
        mat, layer, k = CHUNKS[i]
        rows_all, cols, _ = MATRICES[mat]
        kind, p_name = KIND[layer][mat], first_axis(mat, layer)
        by_pairs = p_name == 'z'
        q_name = kind.lower() if by_pairs else 'xy'.replace(kind, '')
        r_name = 'xy'.replace(q_name, '')
        rows = rows_all // chunk_count(mat, layer)
        part = part_refs[layer * len(MATRICES) + mat]
        p_at, q_at, r_at = place[p_name], place[q_name], place[r_name]

        def go(src, dst, sem, dest, cond=None):
            remote(src(), dst(), i, sem, to[dest]).start()
            pending.append((cond, src, i, sem))

        def block(dp=0, dq=0, dc=0, dr=None, dh=None):
            def ref():
                row, count = flip(q_at, dq) * (rows // 2), rows // 2
                if dr is not None:
                    row, count = row + flip(r_at, dr) * (rows // 4), rows // 4
                return out_block(i, flip(p_at, dp), flip(core, dc), row, count, None if dh is None else flip(half, dh))

            return ref

        def pass_on(blk, sems, cond=None):
            for dest, sem in sems:
                go(blk, blk, sem, dest, cond)

        def arrived(blk, sem):
            remote(blk(), blk(), i, sem, me).wait_recv()

        def half_cols(by):
            return pl.ds(pl.multiple_of(flip(half, by) * (cols // 2), 128), cols // 2)

        def own_rows(by):
            return land_q[i].at[pl.ds(pl.multiple_of(flip(r_at, by) * (rows // 4), 8), rows // 4), :] if by_pairs else land_q[i]

        def own_half(by):
            return lambda: (land_q[i].at[pl.ds(pl.multiple_of(r_at * (rows // 4), 8), rows // 4), half_cols(by)] if by_pairs
                            else land_q[i].at[:, half_cols(by)])

        def rows_of(by):
            return lambda: part.at[pl.ds(pl.multiple_of(k * rows + flip(q_at, by) * (rows // 2), 8), rows // 2), :]

        last = dict(dr=0) if by_pairs else {}

        def keep():
            return pltpu.make_async_copy(own_half(0)(), block(dh=0, **last)(), local_sems.at[i])

        def whole(buf):
            return lambda: buf[i]

        def scale_and_send(dest):
            add_rows(own_rows(0), land_h[i], half_cols(0), 1.0 / n_dev)
            keep().start()
            go(own_half(0), block(dh=0, **last), 3, dest, None if by_pairs else middle)

        def spread(turn):
            if turn == 0:
                pass_on(block(), ((q_name, 5), (p_name, 6), ('core', 8)))
            elif turn == 1:
                arrived(block(dq=1), 5)
                pass_on(block(dq=1), ((p_name, 7), ('core', 9)))
            else:
                dq = turn - 2
                arrived(block(dp=1, dq=dq), turn + 4)
                pass_on(block(dp=1, dq=dq), (('core', turn + 8),))

        if stage == 0:
            go(rows_of(1), whole(land_q), 0, q_name)
        elif stage == 8:
            for turn in range(4):
                arrived(block(dp=turn // 2, dq=turn % 2, dc=1), 8 + turn)
        elif by_pairs:
            if stage == 1:
                arrived(whole(land_q), 0)
                stream_add(land_q[i], rows_of(0)())
                go(lambda: own_rows(1), whole(land_z), 1, r_name)
            elif stage == 2:
                arrived(whole(land_z), 1)
                add_rows(own_rows(0), land_z[i], slice(None))
                go(own_half(1), whole(land_h), 2, 'far')
            elif stage == 3:
                arrived(whole(land_h), 2)
                scale_and_send('far')
            elif stage == 4:
                keep().wait()
                arrived(block(dr=0, dh=1), 3)
                go(block(dr=0), block(dr=0), 4, r_name)
            else:
                if stage == 5:
                    arrived(block(dr=1), 4)
                spread(min(stage - 5, 3))
        elif stage == 1:
            arrived(whole(land_q), 0)
            stream_add(land_q[i], rows_of(0)())

            @pl.when(edge)
            def _():
                go(whole(land_q), whole(land_z), 1, 'mid', edge)
        elif stage in (2, 3):
            @pl.when(middle)
            def _():
                arrived(whole((land_z, land_h)[stage - 2]), stage - 1)
                if stage == 2:
                    add_rows(land_q[i], land_z[i], slice(None))
                    go(own_half(1), whole(land_h), 2, 'mid', middle)
                else:
                    scale_and_send('mid')
        else:
            if stage == 4:
                @pl.when(middle)
                def _():
                    keep().wait()
                    arrived(block(dh=1), 3)
                    pass_on(block(), (('end', 4),), middle)

                @pl.when(edge)
                def _():
                    arrived(block(), 4)
            spread(stage - 4)

    def unit_sizes(unit):
        rows, cols, split = MATRICES[unit[0]]
        p_name = first_axis(*unit)
        return (rows, cols, p_name, split) + ((rows, cols) if split == 0 else (cols, rows))

    def operand_copy(u, which, src, dst, dest):
        return pltpu.make_async_remote_copy(src_ref=src, dst_ref=dst, send_sem=op_send.at[u, which], recv_sem=op_recv.at[u, which],
                                            device_id=(to[dest],), device_id_type=pl.DeviceIdType.MESH)

    def operand_copies(u):
        unit = units[u]
        _, _, p_name, split, wide_w, _ = unit_sizes(unit)
        p_at = place[p_name]
        wide, thin = given[u][:2]
        core_wide, core_thin = from_core[2 * u:2 * u + 2]
        if unit in LATE:
            late = LATE.index(unit)
            chip_wide, chip_thin = from_chip[2 * late:2 * late + 2]
        else:
            chip_wide, chip_thin = given[u][2:]
        first, second = pl.ds(0, SEQ_LEN), pl.ds(SEQ_LEN, SEQ_LEN)

        def lanes(at, count):
            return pl.ds(pl.multiple_of(at, 128), count)

        other = 1 - core
        copies = {
            'own': (operand_copy(u, 0, wide.at[:, lanes((p_at * 2 + other) * wide_w, wide_w)], core_wide.at[first, :], 'core'),
                    operand_copy(u, 1, thin, core_thin.at[first, :], 'core')),
            'next': (operand_copy(u, 2, chip_wide.at[:, lanes(other * wide_w, wide_w)], core_wide.at[second, :], 'core'),
                     operand_copy(u, 3, chip_thin, core_thin.at[second, :], 'core')),
        }
        if unit in LATE:
            copies['chip'] = (operand_copy(u, 4, wide.at[:, lanes((1 - p_at) * 2 * wide_w, 2 * wide_w)], chip_wide, p_name),
                              operand_copy(u, 5, thin, chip_thin, p_name))
        wide_op, thin_op = (row_op, col_op) if split == 0 else (col_op, row_op)
        thin_w = thin.shape[1]
        loads = []
        for start, src in ((0, wide.at[:, lanes((p_at * 2 + core) * wide_w, wide_w)]), (SEQ_LEN, chip_wide.at[:, lanes(core * wide_w, wide_w)]),
                           (2 * SEQ_LEN, core_wide)):
            loads.append((src, wide_op.at[pl.ds(start, src.shape[0]), pl.ds(0, wide_w)]))
        for start, src in ((0, thin), (SEQ_LEN, chip_thin), (2 * SEQ_LEN, core_thin)):
            loads.append((src, thin_op.at[pl.ds(start, src.shape[0]), pl.ds(0, thin_w)]))
        copies['load'] = tuple(pltpu.make_async_copy(src, dst, op_local.at[u, n]) for n, (src, dst) in enumerate(loads))
        return copies

    def start_operands(u):
        copies = operand_copies(u)
        if units[u] in LATE:
            for copy in copies['chip']:
                copy.start()
        for copy in copies['own']:
            copy.start()
        if units[u] not in LATE:
            for copy in copies['next']:
                copy.start()

    def forward_operands(u):
        copies = operand_copies(u)
        for copy in copies['chip']:
            copy.wait_recv()
        for copy in copies['next']:
            copy.start()

    def multiply(u):
        rows, cols, _, _, _, _ = unit_sizes(units[u])
        copies = operand_copies(u)
        for copy in copies['own'] + copies['next']:
            copy.wait_recv()
        for copy in copies['load']:
            copy.start()
        for copy in copies['load']:
            copy.wait()
        tile = min(TILE_ROWS, rows)
        half_w = cols // 2

        @pl.loop(0, rows // tile)
        def _(step):
            at = pl.ds(pl.multiple_of(step * tile, tile), tile)
            for side in range(2):
                lanes = pl.ds(side * half_w, half_w)
                product[at, lanes] = dot_tn(row_op[:, at], col_op[:, lanes])

        store = pltpu.make_async_copy(product.at[pl.ds(0, rows), pl.ds(0, cols)], part_refs[u], op_local.at[u, 6])
        store.start()
        store.wait()

    def finish_operands(u):
        copies = operand_copies(u)
        for copy in copies['own'] + copies['next'] + copies.get('chip', ()):
            copy.wait_send()

    gain_steps = ('core', 'x', 'y', 'z', 'far')

    def gain_copy(step):
        return pltpu.make_async_remote_copy(src_ref=gain_buf.at[step], dst_ref=gain_land.at[step], send_sem=gain_send.at[step],
                                            recv_sem=gain_recv.at[step], device_id=(to[gain_steps[step]],), device_id_type=pl.DeviceIdType.MESH)

    def gain_next(step):
        copy = gain_copy(step)
        copy.wait()
        total = gain_buf[step] + gain_land[step]
        if step + 1 < len(gain_steps):
            gain_buf[step + 1] = total
            gain_copy(step + 1).start()
        else:
            gain_out[...] = total * (1.0 / n_dev)

    pending = []
    gain_buf[0] = gain_in[...]
    step = 0
    first_use = []
    for mat, layer, _ in CHUNKS:
        if units.index((mat, layer)) not in first_use:
            first_use.append(units.index((mat, layer)))
    for u in first_use:
        start_operands(u)
    for count, (letter, digit) in enumerate(zip(*[iter(''.join(ORDER))] * 2)):
        i, stage = ord(letter) - ord('a'), int(digit, 16)
        u = units.index(CHUNKS[i][:2])
        if stage == 9:
            multiply(u)
        elif stage == 10:
            forward_operands(u)
        else:
            run(i, stage, pending)
        if count == 1:
            gain_copy(0).start()
        if count >= 8 and count % 6 == 0 and step < len(gain_steps):
            gain_next(step)
            step += 1
    for u in range(len(units)):
        finish_operands(u)
    for cond, src, i, sem in pending:
        def finish(src=src, i=i, sem=sem):
            remote(src(), src(), i, sem, me).wait_send()

        if cond is None:
            finish()
        else:
            pl.when(cond)(finish)


def combine(operands, gains, n_dev, n_layers):
    f32, bf16 = jnp.float32, jnp.bfloat16
    units = [(mat, layer) for layer in range(n_layers) for mat in range(len(MATRICES))]
    outs = []
    for rows, cols, split in MATRICES:
        outs.append(jax.ShapeDtypeStruct((n_layers, rows * (4 if split == 0 else 1), cols * (4 if split == 1 else 1)), f32))
    outs.append(jax.ShapeDtypeStruct(gains.shape, f32))
    widths = [MATRICES[mat][:2] if MATRICES[mat][2] == 0 else MATRICES[mat][1::-1] for mat, _ in units]
    for wide_w, thin_w in widths:
        outs += [jax.ShapeDtypeStruct((2 * SEQ_LEN, wide_w), bf16), jax.ShapeDtypeStruct((2 * SEQ_LEN, thin_w), bf16)]
    outs += [jax.ShapeDtypeStruct(MATRICES[mat][:2], f32) for mat, _ in units]
    for unit in LATE:
        wide_w, thin_w = widths[units.index(unit)]
        outs += [jax.ShapeDtypeStruct((SEQ_LEN, 2 * wide_w), bf16), jax.ShapeDtypeStruct((SEQ_LEN, thin_w), bf16)]
    sizes = [(MATRICES[mat][0] // chunk_count(mat, layer) // 2, MATRICES[mat][1], first_axis(mat, layer) == 'z') for mat, layer, _ in CHUNKS]
    scratch = [pltpu.VMEM((r, c), f32) for r, c, _ in sizes]
    scratch += [pltpu.VMEM((r // 2 if pairs else r, c), f32) for r, c, pairs in sizes]
    scratch += [pltpu.VMEM((r // 2 if pairs else r, c // 2), f32) for r, c, pairs in sizes]
    n_chunk, n_unit = len(CHUNKS), len(units)
    most_rows, most_cols = max(m[0] for m in MATRICES), max(m[1] for m in MATRICES)
    scratch += [pltpu.VMEM((TOKENS, most_rows), bf16), pltpu.VMEM((TOKENS, most_cols), bf16), pltpu.VMEM((most_rows, most_cols), f32),
                pltpu.VMEM((2, STREAM_ROWS, most_cols), f32),
                pltpu.VMEM((5,) + gains.shape, f32), pltpu.VMEM((5,) + gains.shape, f32),
                pltpu.SemaphoreType.DMA((n_chunk, N_SEMS)), pltpu.SemaphoreType.DMA((n_chunk, N_SEMS)), pltpu.SemaphoreType.DMA((n_chunk,)), pltpu.SemaphoreType.DMA((2,)),
                pltpu.SemaphoreType.DMA((5,)), pltpu.SemaphoreType.DMA((5,)),
                pltpu.SemaphoreType.DMA((n_unit, 6)), pltpu.SemaphoreType.DMA((n_unit, 6)), pltpu.SemaphoreType.DMA((n_unit, 7))]
    hbm, vmem = pl.BlockSpec(memory_space=pl.ANY), pl.BlockSpec(memory_space=pltpu.VMEM)
    flat = [val for group in operands for val in group]
    results = pl.pallas_call(
        functools.partial(combine_kernel, n_dev, n_layers),
        out_shape=tuple(outs),
        in_specs=[hbm] * len(flat) + [vmem],
        out_specs=tuple([hbm] * 4 + [vmem] + [hbm] * (len(outs) - 5)),
        scratch_shapes=scratch,
        compiler_params=pltpu.CompilerParams(has_side_effects=True, vmem_limit_bytes=63 * 1024 * 1024),
    )(*flat, gains)
    return results[:5]


def solution(mesh):
    n_dev = mesh.shape[AXIS]

    def whole_step(x_loc, grad_y_loc, gain_one, gain_two, w_qkv, w_out, w_up, w_down):
        place = Place(n_dev)
        n_layers = w_qkv.shape[0]
        rows, saved = x_loc[0], []
        for layer in range(n_layers):
            u_one, q_all, k_all, v_all, mixed, hidden = attn_forward(layer, rows, gain_one[layer], w_qkv, w_out)
            u_two, pre, act, *after = mlp_forward(layer, hidden, gain_two[layer], w_up, w_down, layer + 1 < n_layers)
            saved.append((rows, u_one, q_all, k_all, v_all, mixed, hidden, u_two, pre, act))
            rows = after[0] if after else None
        operands = [None] * (n_layers * len(MATRICES))

        def reduce_grad(mat, layer_idx, lhs, rhs):
            color, split = first_axis(mat, layer_idx), MATRICES[mat][2]
            if (mat, layer_idx) in LATE:
                operands[layer_idx * len(MATRICES) + mat] = (lhs, rhs) if split == 0 else (rhs, lhs)
            else:
                operands[layer_idx * len(MATRICES) + mat] = neighbour_operands(place, color, split, lhs, rhs)

        gain_grads = [None] * (2 * n_layers)
        grad = grad_y_loc[0]
        for layer in reversed(range(n_layers)):
            rows, u_one, q_all, k_all, v_all, mixed, hidden, u_two, pre, act = saved[layer]
            reduce_grad(0, layer, act, grad)
            grad_pre, grad_hidden, gain_grads[n_layers + layer] = mlp_backward(layer, grad, hidden, gain_two[layer], pre, w_up, w_down)
            reduce_grad(1, layer, u_two, grad_pre)
            reduce_grad(2, layer, mixed, grad_hidden)
            grad_qkv, grad, gain_grads[layer] = attn_backward(layer, grad_hidden, rows, gain_one[layer], q_all, k_all, v_all, w_qkv, w_out)
            reduce_grad(3, layer, u_one, grad_qkv)
        gains = jnp.concatenate(gain_grads + [jnp.zeros((8 - 2 * n_layers, gain_grads[0].shape[1]), jnp.float32)])
        down, up, out, qkv, gains = combine(operands, gains, n_dev, n_layers)
        return (grad[None], gains[:n_layers], gains[n_layers:2 * n_layers], qkv, out, up, down)

    batch_spec = P(AXIS)
    full_spec = P()
    return jax.shard_map(whole_step, mesh=mesh, in_specs=(batch_spec, batch_spec) + (full_spec,) * 6, out_specs=(batch_spec,) + (full_spec,) * 6, check_vma=False)
```

```python
import functools

import jax
import jax.numpy as jnp
from jax import lax
from jax.experimental import pallas as pl
from jax.experimental.pallas import tpu as pltpu
from jax.sharding import PartitionSpec as P

NORM_EPS = 1e-6
HEAD_DIM = 64
AXIS = 'data'
CHUNK_UNITS = '003010111100300001102000313110102101'
ORDER = (
    'a9a0c9d9kaa1c0d0e0baa2c1f0b9b0a3c2f1g0d1a4i9c3h0f2b1i0f3c4e1',
    'k9g1j0k0d2f4a5h1a6d3b2i1m9l0m0c5j1b3e2d4n0c6k1o0f5g2f6b4e3l1',
    'q9p0h2g3a7a8m1q0h3i2e4c7c8j2d5k2g4l2n1f7h4f8r0d6i3b6j3o1k3l3',
    'm2b5o2p1k4e5i4p2j4n2o3m3l4q1p3e6g6n3m4h6r1o4d7n4r2d8p4g5b7r3',
    'b8h5i5r4q2j6q3i6e7q4k5e8l6m5j5o6k7l5n5m7p6o5g7g8p5n7h7h8r6i7',
    'q5i8r5k6q7j7j8m6kel7l8n6mem8o7k8o8p7p8q6ner7n8r8qeq8',
)
VMEM_LIMIT = 63 * 1024 * 1024


MATRICES = ((1024, 1024, 0), (1024, 1024, 1), (256, 1024, 0), (1024, 768, 1))
KIND = ('yyYy', 'xxXX')
LATE = ((2, 0), (3, 0))
SEQ_LEN = 384
TOKENS = 4 * SEQ_LEN
TILE_ROWS = 256
STREAM_ROWS = 64
N_SEMS = 12
ADD_ROWS = 32


def read_chunks(text):
    found = []
    for mat, layer in zip(*[map(int, text)] * 2):
        found.append((mat, layer, sum(chunk[:2] == (mat, layer) for chunk in found)))
    return tuple(found)


CHUNKS = read_chunks(CHUNK_UNITS)


def first_axis(mat, layer):
    kind = KIND[layer][mat]
    return kind if kind in 'xy' else 'z'


def chunk_count(mat, layer):
    return sum(chunk[:2] == (mat, layer) for chunk in CHUNKS)


PAIR = 2 * HEAD_DIM
GROUP = 2 * PAIR
Q_BLOCK = 128
FF_BLOCK = 512
NORM_ROWS = 64
GELU_C = 0.7978845608028654
GELU_D = 0.044715


def dot_with(dims):
    return lambda lhs, rhs: lax.dot_general(lhs, rhs, (dims, ((), ())), preferred_element_type=jnp.float32)


dot_nn, dot_nt, dot_tn = (dot_with(((left,), (right,))) for left, right in ((1, 0), (1, 1), (0, 0)))


def rounded(val):
    return val.astype(jnp.bfloat16)


def wide_float(val):
    return val.astype(jnp.float32)


def row_blocks(count):
    def wrap(body):
        @pl.loop(0, count // NORM_ROWS)
        def _(step):
            body(pl.ds(pl.multiple_of(step * NORM_ROWS, NORM_ROWS), NORM_ROWS))
    return wrap


def inverse_rms(rows_f):
    return lax.rsqrt(jnp.mean(rows_f * rows_f, axis=-1, keepdims=True) + NORM_EPS)


def norm_forward(src, gain, dst):
    @row_blocks(src.shape[0])
    def _(at):
        rows_f = wide_float(src[at, :])
        dst[at, :] = rounded(rows_f * inverse_rms(rows_f) * gain[...])


def norm_backward(src, gain, grad_norm, grad_res, dst, gain_dst):
    gain_dst[...] = jnp.zeros_like(gain_dst)

    @row_blocks(src.shape[0])
    def _(at):
        rows_f = wide_float(src[at, :])
        scale = inverse_rms(rows_f)
        unit = rows_f * scale
        grad = wide_float(rounded(grad_norm[at, :]))
        gain_dst[...] += jnp.sum(grad * unit, axis=0, keepdims=True)
        grad = grad * gain[...]
        grad = scale * (grad - unit * jnp.mean(grad * unit, axis=-1, keepdims=True))
        dst[at, :] = rounded(wide_float(grad_res[at, :]) + grad)


def two_heads(rows):
    first = lax.broadcasted_iota(jnp.int32, rows.shape, 1) < HEAD_DIM
    zero = jnp.zeros_like(rows)
    return jnp.concatenate([jnp.where(first, rows, zero), jnp.where(first, zero, rows)], axis=0)


def one_pair(rows):
    half = rows.shape[0] // 2
    first = lax.broadcasted_iota(jnp.int32, (half, PAIR), 1) < HEAD_DIM
    return jnp.where(first, rows[:half], rows[half:])


def softmax_block(q_two, k_rows, block):
    n_keys = k_rows.shape[0]
    scores = dot_nt(q_two, k_rows) * HEAD_DIM ** -0.5
    last = scores[:, n_keys - Q_BLOCK:]
    row = lax.rem(lax.broadcasted_iota(jnp.int32, last.shape, 0), Q_BLOCK)
    last = jnp.where(row >= lax.broadcasted_iota(jnp.int32, last.shape, 1), last, -1e30)
    scores = last if block == 0 else jnp.concatenate([scores[:, :n_keys - Q_BLOCK], last], axis=1)
    weights = jnp.exp(scores - jnp.max(scores, axis=-1, keepdims=True))
    return weights * (1.0 / jnp.sum(weights, axis=-1, keepdims=True))


def attend(q_ref, k_ref, v_ref, o_ref):
    for block in range(q_ref.shape[0] // Q_BLOCK):
        rows, keys = pl.ds(block * Q_BLOCK, Q_BLOCK), pl.ds(0, (block + 1) * Q_BLOCK)
        for pair in range(GROUP // PAIR):
            lanes = pl.ds(pair * PAIR, PAIR)
            prob = softmax_block(two_heads(q_ref[rows, lanes]), k_ref[keys, lanes], block)
            o_ref[rows, lanes] = rounded(one_pair(dot_nn(rounded(prob), v_ref[keys, lanes])))


def attend_backward(do_ref, q_ref, k_ref, v_ref, k_acc, v_acc):
    n_block = q_ref.shape[0] // Q_BLOCK
    for pair in range(GROUP // PAIR):
        lanes = pl.ds(pair * PAIR, PAIR)
        for block in reversed(range(n_block)):
            rows, keys = pl.ds(block * Q_BLOCK, Q_BLOCK), pl.ds(0, (block + 1) * Q_BLOCK)
            q_two, g_two = two_heads(q_ref[rows, lanes]), two_heads(do_ref[rows, lanes])
            k_rows = k_ref[keys, lanes]
            prob = softmax_block(q_two, k_rows, block)
            grad_prob = dot_nt(g_two, v_ref[keys, lanes])
            mean = jnp.sum(prob * grad_prob, axis=-1, keepdims=True)
            grad_s = rounded(prob * (grad_prob - mean) * HEAD_DIM ** -0.5)
            q_ref[rows, lanes] = rounded(one_pair(dot_nn(grad_s, k_rows)))
            k_part, v_part = dot_tn(grad_s, q_two), dot_tn(rounded(prob), g_two)
            if block == n_block - 1:
                k_acc[:, lanes] = k_part
                v_acc[:, lanes] = v_part
            else:
                k_acc[keys, lanes] += k_part
                v_acc[keys, lanes] += v_part
    k_ref[...] = rounded(k_acc[...])
    v_ref[...] = rounded(v_acc[...])


KEPT = {'u_one': 1, 'mixed': 1, 'u_two': 1, 'act': 4, 'grad_pre': 4, 'grad_hidden': 1, 'grad_qkv': 3, 'grad': 1}
FACTORS = (('act', 'grad'), ('u_two', 'grad_pre'), ('mixed', 'grad_hidden'), ('u_one', 'grad_qkv'))


def own_place(me):
    core, x_at, y_at, z_at = lax.rem(me, 2), lax.rem(lax.div(me, 2), 2), lax.rem(lax.div(me, 4), 2), lax.div(me, 8)
    half = lax.div(z_at, 2)
    place = {'core': core, 'x': x_at, 'y': y_at, 'z': lax.rem(z_at, 2), 'half': half}
    to = {}
    for name, stride in (('core', 1), ('x', 2), ('y', 4), ('z', 8)):
        to[name] = me + stride * (1 - 2 * place[name])
    inward = 8 * (1 - 2 * half)
    to.update(mid=me + inward, end=me - inward, far=me + 2 * inward)
    return place, to, lax.div(z_at + 1, 2) == 1, lax.div(z_at + 1, 2) != 1


def compute_kernel(n_layers, x_in, grad_in, gain_one, gain_two, w_qkv, w_out, w_up, w_down, *refs):
    refs = list(refs)

    def take(count):
        head, refs[:] = refs[:count], refs[count:]
        return head

    grad_out, gain_out = take(2)
    kept = [dict(zip(KEPT, take(len(KEPT)))) for _ in range(n_layers)]
    units = [(mat, layer) for layer in range(n_layers) for mat in range(len(MATRICES))]
    early = [unit for unit in units if unit not in LATE]
    from_chip = dict(zip(early, zip(take(len(early)), take(len(early)))))
    rows, hidden, qkv, pre = (take(n_layers) for _ in range(4))
    unit_rows, mixed, act, grad_hidden, grad, do_ref, k_acc, v_acc, acc, s_qkv, s_out, s_up, s_down = take(13)
    sem_qkv, sem_out, sem_up, sem_down, sem_in, sem_put, sem_send, sem_recv = refs
    place, to, _, _ = own_place(lax.axis_index(AXIS))
    n_group, n_ff = s_out.shape[0], s_up.shape[0]

    def fetch_group(layer, at):
        cols = [pl.ds(pl.multiple_of((which * n_group + at) * GROUP, GROUP), GROUP) for which in range(3)]
        pieces = [pltpu.make_async_copy(w_qkv.at[layer, :, cols[which]], s_qkv.at[which, at], sem_qkv.at[which, at]) for which in range(3)]
        return pieces + [pltpu.make_async_copy(w_out.at[layer, pl.ds(pl.multiple_of(at * GROUP, GROUP), GROUP), :], s_out.at[at], sem_out.at[at])]

    def fetch_up(layer, at):
        return pltpu.make_async_copy(w_up.at[layer, :, pl.ds(pl.multiple_of(at * FF_BLOCK, FF_BLOCK), FF_BLOCK)], s_up.at[at], sem_up.at[at])

    def fetch_down(layer, at):
        return pltpu.make_async_copy(w_down.at[layer, pl.ds(pl.multiple_of(at * FF_BLOCK, FF_BLOCK), FF_BLOCK), :], s_down.at[at], sem_down.at[at])

    def start_groups(layer):
        for at in range(n_group):
            for piece in fetch_group(layer, at):
                piece.start()

    def start_all(fetch, layer):
        for at in range(n_ff):
            fetch(layer, at).start()

    n_put, sent, waiting = [0], [], []

    def put(src, dst):
        copy = pltpu.make_async_copy(src, dst, sem_put.at[n_put[0]])
        n_put[0] += 1
        copy.start()
        return copy

    def put_blocks(src, dst):
        count, _, cols = src.shape
        return [put(src.at[at], dst.at[:, pl.ds(at * cols, cols)]) for at in range(count)]

    def exchange(mat, layer, which):
        if (mat, layer) in LATE:
            return
        axis, split = first_axis(mat, layer), MATRICES[mat][2]
        name = FACTORS[mat][which]
        src = grad_in.at[0] if (name, layer) == ('grad', n_layers - 1) else kept[layer][name]
        if which == split:
            dst = from_chip[(mat, layer)][0]
            src = src.at[:, pl.ds(pl.multiple_of((1 - place[axis]) * dst.shape[1], 128), dst.shape[1])]
        else:
            dst = from_chip[(mat, layer)][1]
        copy = pltpu.make_async_remote_copy(src_ref=src, dst_ref=dst, send_sem=sem_send.at[len(sent)], recv_sem=sem_recv.at[len(sent)],
                                            device_id=(to[axis],), device_id_type=pl.DeviceIdType.MESH)
        sent.append(copy)
        copy.start()

    def save(name, layer, copies):
        waiting.append((name, layer, copies))

    def flush():
        for name, layer, copies in waiting:
            for copy in copies:
                copy.wait()
            for mat, names in enumerate(FACTORS):
                if name in names:
                    exchange(mat, layer, names.index(name))
        waiting.clear()

    def gain_row(gain, layer):
        return gain.at[pl.ds(layer, 1), :]

    def attention_forward(layer):
        flush()
        norm_forward(rows[layer], gain_row(gain_one, layer), unit_rows)
        save('u_one', layer, [put(unit_rows, kept[layer]['u_one'])])
        acc[...] = jnp.zeros_like(acc)
        q_all, k_all, v_all = (qkv[layer].at[which] for which in range(3))

        @pl.loop(0, n_group)
        def _(at):
            for piece in fetch_group(layer, at):
                piece.wait()
            for which in range(3):
                qkv[layer][which, at] = rounded(dot_nn(unit_rows[...], s_qkv[which, at]))
            attend(q_all.at[at], k_all.at[at], v_all.at[at], mixed.at[at])
            acc[...] += dot_nn(mixed[at], s_out[at])
        save('mixed', layer, put_blocks(mixed, kept[layer]['mixed']))
        hidden[layer][...] = rows[layer][...] + rounded(acc[...])

    def mlp_forward(layer):
        last = layer + 1 == n_layers
        flush()
        norm_forward(hidden[layer], gain_row(gain_two, layer), unit_rows)
        save('u_two', layer, [put(unit_rows, kept[layer]['u_two'])])
        acc[...] = jnp.zeros_like(acc)

        @pl.loop(0, n_ff)
        def _(at):
            fetch_up(layer, at).wait()
            pre[layer][at] = rounded(dot_nn(unit_rows[...], s_up[at]))
            rows_f = wide_float(pre[layer][at])
            bend = jnp.tanh(GELU_C * (rows_f + GELU_D * (rows_f * rows_f * rows_f)))
            act[at] = rounded(rows_f * (0.5 * (1.0 + bend)))
            if not last:
                fetch_down(layer, at).wait()
                acc[...] += dot_nn(act[at], s_down[at])
        save('act', layer, put_blocks(act, kept[layer]['act']))
        if not last:
            rows[layer + 1][...] = hidden[layer][...] + rounded(acc[...])

    def mlp_backward(layer, fetched):
        acc[...] = jnp.zeros_like(acc)

        @pl.loop(0, n_ff)
        def _(at):
            fetch_down(layer, at).wait()
            if not fetched:
                fetch_up(layer, at).wait()
            grad_a = wide_float(rounded(dot_nt(grad[...], s_down[at])))
            rows_f = wide_float(pre[layer][at])
            square = rows_f * rows_f
            bend = jnp.tanh(GELU_C * (rows_f + GELU_D * (square * rows_f)))
            slope = 0.5 * (1.0 + bend) + (0.5 * GELU_C) * rows_f * (1.0 - bend * bend) * (1.0 + (3.0 * GELU_D) * square)
            pre[layer][at] = rounded(slope * grad_a)
            acc[...] += dot_nt(pre[layer][at], s_up[at])
        flush()
        save('grad_pre', layer, put_blocks(pre[layer], kept[layer]['grad_pre']))
        norm_backward(hidden[layer], gain_row(gain_two, layer), acc, grad, grad_hidden, gain_row(gain_out, n_layers + layer))
        save('grad_hidden', layer, [put(grad_hidden, kept[layer]['grad_hidden'])])

    def attention_backward(layer, fetched):
        acc[...] = jnp.zeros_like(acc)

        @pl.loop(0, n_group)
        def _(at):
            if not fetched:
                for piece in fetch_group(layer, at):
                    piece.wait()
            do_ref[...] = rounded(dot_nt(grad_hidden[...], s_out[at]))
            attend_backward(do_ref, *(qkv[layer].at[which, at] for which in range(3)), k_acc, v_acc)
            for which in range(3):
                acc[...] += dot_nt(qkv[layer][which, at], s_qkv[which, at])
        flush()
        copies = []
        for which in range(3):
            width = grad.shape[1]
            copies += [put(qkv[layer].at[which, at], kept[layer]['grad_qkv'].at[:, pl.ds(which * width + at * GROUP, GROUP)]) for at in range(n_group)]
        save('grad_qkv', layer, copies)
        norm_backward(rows[layer], gain_row(gain_one, layer), acc, grad_hidden, grad, gain_row(gain_out, layer))

    first = pltpu.make_async_copy(x_in.at[0], rows[0], sem_in.at[0])
    second = pltpu.make_async_copy(grad_in.at[0], grad, sem_in.at[1])
    first.start()
    start_groups(0)
    start_all(fetch_up, 0)
    start_all(fetch_down, 0)
    second.start()
    exchange(0, n_layers - 1, 1)
    gain_out[...] = jnp.zeros_like(gain_out)
    first.wait()
    for layer in range(n_layers):
        attention_forward(layer)
        if layer + 1 < n_layers:
            start_groups(layer + 1)
        mlp_forward(layer)
        if layer + 1 < n_layers:
            start_all(fetch_up, layer + 1)
            start_all(fetch_down, layer + 1)
    second.wait()
    flush()
    for layer in reversed(range(n_layers)):
        top = layer + 1 == n_layers
        mlp_backward(layer, top)
        if layer > 0:
            start_all(fetch_up, layer - 1)
            start_all(fetch_down, layer - 1)
        flush()
        attention_backward(layer, top)
        if layer > 0:
            start_groups(layer - 1)
            save('grad', layer - 1, [put(grad, kept[layer - 1]['grad'])])
            flush()
    done = put(grad, grad_out)
    flush()
    done.wait()
    for copy in sent:
        copy.wait()


def compute(x_loc, grad_loc, gain_one, gain_two, w_qkv, w_out, w_up, w_down):
    n_layers, width, inner = w_up.shape
    seq_len = x_loc.shape[1]
    f32, bf16 = jnp.float32, jnp.bfloat16
    n_group, n_ff = width // GROUP, inner // FF_BLOCK
    units = [(mat, layer) for layer in range(n_layers) for mat in range(len(MATRICES))]
    early = [unit for unit in units if unit not in LATE]

    def lo(*shape):
        return jax.ShapeDtypeStruct(shape, bf16)
    outs = [lo(seq_len, width), jax.ShapeDtypeStruct((8, width), f32)]
    outs += [lo(seq_len, cols * width) for _ in range(n_layers) for cols in KEPT.values()]
    shapes = [[KEPT[name] * width for name in FACTORS[mat]] for mat, _ in early]
    outs += [lo(seq_len, shape[MATRICES[mat][2]] // 2) for shape, (mat, _) in zip(shapes, early)]
    outs += [lo(seq_len, shape[1 - MATRICES[mat][2]]) for shape, (mat, _) in zip(shapes, early)]
    wide_rows, groups = (seq_len, width), (n_group, seq_len, GROUP)
    vmem = [wide_rows] * (2 * n_layers) + [(3,) + groups] * n_layers + [(n_ff, seq_len, FF_BLOCK)] * n_layers
    vmem += [wide_rows, groups, (n_ff, seq_len, FF_BLOCK), wide_rows, wide_rows, (seq_len, GROUP)]
    scratch = [pltpu.VMEM(shape, bf16) for shape in vmem] + [pltpu.VMEM(shape, f32) for shape in ((seq_len, GROUP), (seq_len, GROUP), wide_rows)]
    scratch += [pltpu.VMEM(shape, bf16) for shape in ((3, n_group, width, GROUP), (n_group, GROUP, width), (n_ff, width, FF_BLOCK), (n_ff, FF_BLOCK, width))]
    scratch += [pltpu.SemaphoreType.DMA(shape) for shape in ((3, n_group), (n_group,), (n_ff,), (n_ff,), (2,), (100,), (2 * len(early),), (2 * len(early),))]
    hbm, near = pl.BlockSpec(memory_space=pl.ANY), pl.BlockSpec(memory_space=pltpu.VMEM)
    results = pl.pallas_call(
        functools.partial(compute_kernel, n_layers), out_shape=tuple(outs), in_specs=[hbm, hbm, near, near] + [hbm] * 4,
        out_specs=tuple([hbm, near] + [hbm] * (len(outs) - 2)), scratch_shapes=scratch,
        compiler_params=pltpu.CompilerParams(has_side_effects=True, vmem_limit_bytes=VMEM_LIMIT),
    )(x_loc, grad_loc, gain_one, gain_two, w_qkv, w_out, w_up, w_down)
    grad_x, gains = results[:2]
    kept = [dict(zip(KEPT, results[2 + layer * len(KEPT):])) for layer in range(n_layers)]
    kept[-1]['grad'] = grad_loc[0]
    tail = results[2 + n_layers * len(KEPT):]
    from_chip = dict(zip(early, zip(tail, tail[len(early):])))
    operands = []
    for mat, layer in units:
        pair = [kept[layer][name] for name in FACTORS[mat]]
        split = MATRICES[mat][2]
        operands.append((pair[split], pair[1 - split]) + from_chip.get((mat, layer), ()))
    return grad_x, gains, operands


def add_rows(dst, src, cols, scale=None):
    rows = dst.shape[0]

    @pl.loop(0, rows // ADD_ROWS)
    def _(step):
        at = pl.ds(pl.multiple_of(step * ADD_ROWS, ADD_ROWS), ADD_ROWS)
        val = dst[at, cols] + src[at, :]
        dst[at, cols] = val if scale is None else val * scale


def flip(bit, by):
    return 1 - bit if by else bit


def combine_kernel(n_dev, n_layers, *refs):
    units = [(mat, layer) for layer in range(n_layers) for mat in range(len(MATRICES))]
    n_chunk = len(CHUNKS)
    refs = list(refs)

    def take(count):
        head, refs[:] = refs[:count], refs[count:]
        return head

    given = [take(2 if unit in LATE else 4) for unit in units]
    gain_in, = take(1)
    outs, (gain_out,) = take(len(MATRICES)), take(1)
    from_core, part_refs, from_chip = take(2 * len(units)), take(len(units)), take(2 * len(LATE))
    land_q, land_z, land_h = (take(n_chunk) for _ in range(3))
    row_op, col_op, product, stream, gain_buf, gain_land, send_sems, recv_sems, local_sems, stream_sems, gain_send, gain_recv, op_send, op_recv, op_local = refs

    me = lax.axis_index(AXIS)
    place, to, middle, edge = own_place(me)
    core, half = place['core'], place['half']

    def remote(src, dst, i, sem, dev):
        return pltpu.make_async_remote_copy(src_ref=src, dst_ref=dst, send_sem=send_sems.at[i, sem], recv_sem=recv_sems.at[i, sem],
                                            device_id=(dev,), device_id_type=pl.DeviceIdType.MESH)

    def out_block(i, p_at, c_at, row, n_rows, h_at):
        mat, layer, k = CHUNKS[i]
        rows_all, cols, split = MATRICES[mat]
        quarter = p_at * 2 + c_at
        row = row + k * (rows_all // chunk_count(mat, layer)) + (quarter * rows_all if split == 0 else 0)
        col, n_cols = (0, cols) if h_at is None else (h_at * (cols // 2), cols // 2)
        if split == 1:
            col = col + quarter * cols
        return outs[mat].at[layer, pl.ds(pl.multiple_of(row, 8), n_rows), pl.ds(col if isinstance(col, int) else pl.multiple_of(col, 128), n_cols)]

    def stream_add(dst, src):
        rows, cols = dst.shape
        size = min(STREAM_ROWS, rows)
        steps = rows // size

        def fetch(step, slot):
            return pltpu.make_async_copy(src.at[pl.ds(pl.multiple_of(step * size, size), size), :], stream.at[slot, pl.ds(0, size), pl.ds(0, cols)], stream_sems.at[slot])
        fetch(0, 0).start()

        @pl.loop(0, steps)
        def _(step):
            slot = lax.rem(step, 2)

            @pl.when(step + 1 < steps)
            def _():
                fetch(step + 1, 1 - slot).start()
            fetch(step, slot).wait()
            at = pl.ds(pl.multiple_of(step * size, size), size)
            dst[at, :] = dst[at, :] + stream[slot, pl.ds(0, size), pl.ds(0, cols)]

    def run(i, stage, pending):
        mat, layer, k = CHUNKS[i]
        rows_all, cols, _ = MATRICES[mat]
        kind, p_name = KIND[layer][mat], first_axis(mat, layer)
        by_pairs = p_name == 'z'
        q_name = kind.lower() if by_pairs else 'xy'.replace(kind, '')
        r_name = 'xy'.replace(q_name, '')
        rows = rows_all // chunk_count(mat, layer)
        part = part_refs[layer * len(MATRICES) + mat]
        p_at, q_at, r_at = place[p_name], place[q_name], place[r_name]

        def go(src, dst, sem, dest, cond=None):
            remote(src(), dst(), i, sem, to[dest]).start()
            pending.append((cond, src, i, sem))

        def block(dp=0, dq=0, dc=0, dr=None, dh=None):
            def ref():
                row, count = flip(q_at, dq) * (rows // 2), rows // 2
                if dr is not None:
                    row, count = row + flip(r_at, dr) * (rows // 4), rows // 4
                return out_block(i, flip(p_at, dp), flip(core, dc), row, count, None if dh is None else flip(half, dh))
            return ref

        def pass_on(blk, sems, cond=None):
            for dest, sem in sems:
                go(blk, blk, sem, dest, cond)

        def arrived(blk, sem):
            remote(blk(), blk(), i, sem, me).wait_recv()

        def half_cols(by):
            return pl.ds(pl.multiple_of(flip(half, by) * (cols // 2), 128), cols // 2)

        def own_rows(by):
            return land_q[i].at[pl.ds(pl.multiple_of(flip(r_at, by) * (rows // 4), 8), rows // 4), :] if by_pairs else land_q[i]

        def own_half(by):
            return lambda: (land_q[i].at[pl.ds(pl.multiple_of(r_at * (rows // 4), 8), rows // 4), half_cols(by)] if by_pairs
                            else land_q[i].at[:, half_cols(by)])

        def rows_of(by):
            return lambda: part.at[pl.ds(pl.multiple_of(k * rows + flip(q_at, by) * (rows // 2), 8), rows // 2), :]

        last = dict(dr=0) if by_pairs else {}

        def keep():
            return pltpu.make_async_copy(own_half(0)(), block(dh=0, **last)(), local_sems.at[i])

        def whole(buf):
            return lambda: buf[i]

        def scale_and_send(dest):
            add_rows(own_rows(0), land_h[i], half_cols(0), 1.0 / n_dev)
            keep().start()
            go(own_half(0), block(dh=0, **last), 3, dest, None if by_pairs else middle)

        def spread(turn):
            if turn == 0:
                pass_on(block(), ((q_name, 5), (p_name, 6), ('core', 8)))
            elif turn == 1:
                arrived(block(dq=1), 5)
                pass_on(block(dq=1), ((p_name, 7), ('core', 9)))
            else:
                dq = turn - 2
                arrived(block(dp=1, dq=dq), turn + 4)
                pass_on(block(dp=1, dq=dq), (('core', turn + 8),))

        if stage == 0:
            go(rows_of(1), whole(land_q), 0, q_name)
        elif stage == 8:
            for turn in range(4):
                arrived(block(dp=turn // 2, dq=turn % 2, dc=1), 8 + turn)
        elif by_pairs:
            if stage == 1:
                arrived(whole(land_q), 0)
                stream_add(land_q[i], rows_of(0)())
                go(lambda: own_rows(1), whole(land_z), 1, r_name)
            elif stage == 2:
                arrived(whole(land_z), 1)
                add_rows(own_rows(0), land_z[i], slice(None))
                go(own_half(1), whole(land_h), 2, 'far')
            elif stage == 3:
                arrived(whole(land_h), 2)
                scale_and_send('far')
            elif stage == 4:
                keep().wait()
                arrived(block(dr=0, dh=1), 3)
                go(block(dr=0), block(dr=0), 4, r_name)
            else:
                if stage == 5:
                    arrived(block(dr=1), 4)
                spread(min(stage - 5, 3))
        elif stage == 1:
            arrived(whole(land_q), 0)
            stream_add(land_q[i], rows_of(0)())

            @pl.when(edge)
            def _():
                go(whole(land_q), whole(land_z), 1, 'mid', edge)
        elif stage in (2, 3):
            @pl.when(middle)
            def _():
                arrived(whole((land_z, land_h)[stage - 2]), stage - 1)
                if stage == 2:
                    add_rows(land_q[i], land_z[i], slice(None))
                    go(own_half(1), whole(land_h), 2, 'mid', middle)
                else:
                    scale_and_send('mid')
        else:
            if stage == 4:
                @pl.when(middle)
                def _():
                    keep().wait()
                    arrived(block(dh=1), 3)
                    pass_on(block(), (('end', 4),), middle)

                @pl.when(edge)
                def _():
                    arrived(block(), 4)
            spread(stage - 4)

    def unit_sizes(unit):
        rows, cols, split = MATRICES[unit[0]]
        p_name = first_axis(*unit)
        return (rows, cols, p_name, split) + ((rows, cols) if split == 0 else (cols, rows))

    def operand_copy(u, which, src, dst, dest):
        return pltpu.make_async_remote_copy(src_ref=src, dst_ref=dst, send_sem=op_send.at[u, which], recv_sem=op_recv.at[u, which],
                                            device_id=(to[dest],), device_id_type=pl.DeviceIdType.MESH)

    def operand_copies(u):
        unit = units[u]
        rows, cols, p_name, split, wide_w, _ = unit_sizes(unit)
        p_at = place[p_name]
        wide, thin = given[u][:2]
        core_wide, core_thin = from_core[2 * u:2 * u + 2]
        if unit in LATE:
            late = LATE.index(unit)
            chip_wide, chip_thin = from_chip[2 * late:2 * late + 2]
        else:
            chip_wide, chip_thin = given[u][2:]
        first, second = pl.ds(0, SEQ_LEN), pl.ds(SEQ_LEN, SEQ_LEN)

        def lanes(at, count):
            return pl.ds(pl.multiple_of(at, 128), count)
        other = 1 - core
        copies = {
            'own': (operand_copy(u, 0, wide.at[:, lanes((p_at * 2 + other) * wide_w, wide_w)], core_wide.at[first, :], 'core'),
                    operand_copy(u, 1, thin, core_thin.at[first, :], 'core')),
            'next': (operand_copy(u, 2, chip_wide.at[:, lanes(other * wide_w, wide_w)], core_wide.at[second, :], 'core'),
                     operand_copy(u, 3, chip_thin, core_thin.at[second, :], 'core')),
        }
        if unit in LATE:
            copies['chip'] = (operand_copy(u, 4, wide.at[:, lanes((1 - p_at) * 2 * wide_w, 2 * wide_w)], chip_wide, p_name),
                              operand_copy(u, 5, thin, chip_thin, p_name))
        wide_op, thin_op = (row_op, col_op) if split == 0 else (col_op, row_op)
        thin_w = thin.shape[1]
        loads = []
        for start, src in ((0, wide.at[:, lanes((p_at * 2 + core) * wide_w, wide_w)]), (SEQ_LEN, chip_wide.at[:, lanes(core * wide_w, wide_w)]),
                           (2 * SEQ_LEN, core_wide)):
            loads.append((src, wide_op.at[pl.ds(start, src.shape[0]), pl.ds(0, wide_w)]))
        for start, src in ((0, thin), (SEQ_LEN, chip_thin), (2 * SEQ_LEN, core_thin)):
            loads.append((src, thin_op.at[pl.ds(start, src.shape[0]), pl.ds(0, thin_w)]))
        copies['load'] = tuple(pltpu.make_async_copy(src, dst, op_local.at[u, n]) for n, (src, dst) in enumerate(loads))
        return copies

    def start_operands(u):
        copies = operand_copies(u)
        if units[u] in LATE:
            for copy in copies['chip']:
                copy.start()
        for copy in copies['own']:
            copy.start()
        if units[u] not in LATE:
            for copy in copies['next']:
                copy.start()

    def forward_operands(u):
        copies = operand_copies(u)
        for copy in copies['chip']:
            copy.wait_recv()
        for copy in copies['next']:
            copy.start()

    def multiply(u):
        rows, cols, _, _, _, _ = unit_sizes(units[u])
        copies = operand_copies(u)
        for copy in copies['own'] + copies['next']:
            copy.wait_recv()
        for copy in copies['load']:
            copy.start()
        for copy in copies['load']:
            copy.wait()
        tile = min(TILE_ROWS, rows)
        half_w = cols // 2

        @pl.loop(0, rows // tile)
        def _(step):
            at = pl.ds(pl.multiple_of(step * tile, tile), tile)
            for side in range(2):
                lanes = pl.ds(side * half_w, half_w)
                product[at, lanes] = dot_tn(row_op[:, at], col_op[:, lanes])
        store = pltpu.make_async_copy(product.at[pl.ds(0, rows), pl.ds(0, cols)], part_refs[u], op_local.at[u, 6])
        store.start()
        store.wait()

    def finish_operands(u):
        copies = operand_copies(u)
        for copy in copies['own'] + copies['next'] + copies.get('chip', ()):
            copy.wait_send()

    gain_steps = ('core', 'x', 'y', 'z', 'far')

    def gain_copy(step):
        return pltpu.make_async_remote_copy(src_ref=gain_buf.at[step], dst_ref=gain_land.at[step], send_sem=gain_send.at[step],
                                            recv_sem=gain_recv.at[step], device_id=(to[gain_steps[step]],), device_id_type=pl.DeviceIdType.MESH)

    def gain_next(step):
        copy = gain_copy(step)
        copy.wait()
        total = gain_buf[step] + gain_land[step]
        if step + 1 < len(gain_steps):
            gain_buf[step + 1] = total
            gain_copy(step + 1).start()
        else:
            gain_out[...] = total * (1.0 / n_dev)

    pending = []
    gain_buf[0] = gain_in[...]
    step = 0
    first_use = []
    for mat, layer, _ in CHUNKS:
        if units.index((mat, layer)) not in first_use:
            first_use.append(units.index((mat, layer)))
    for u in first_use:
        start_operands(u)
    for count, (letter, digit) in enumerate(zip(*[iter(''.join(ORDER))] * 2)):
        i, stage = ord(letter) - ord('a'), int(digit, 16)
        u = units.index(CHUNKS[i][:2])
        if stage == 9:
            multiply(u)
        elif stage == 10:
            forward_operands(u)
        else:
            run(i, stage, pending)
        if count == 1:
            gain_copy(0).start()
        if count >= 8 and count % 6 == 0 and step < len(gain_steps):
            gain_next(step)
            step += 1
    for u in range(len(units)):
        finish_operands(u)
    for cond, src, i, sem in pending:
        def finish(src=src, i=i, sem=sem):
            remote(src(), src(), i, sem, me).wait_send()
        if cond is None:
            finish()
        else:
            pl.when(cond)(finish)


def combine(operands, gains, n_dev, n_layers):
    f32, bf16 = jnp.float32, jnp.bfloat16
    units = [(mat, layer) for layer in range(n_layers) for mat in range(len(MATRICES))]
    outs = []
    for rows, cols, split in MATRICES:
        outs.append(jax.ShapeDtypeStruct((n_layers, rows * (4 if split == 0 else 1), cols * (4 if split == 1 else 1)), f32))
    outs.append(jax.ShapeDtypeStruct(gains.shape, f32))
    widths = [MATRICES[mat][:2] if MATRICES[mat][2] == 0 else MATRICES[mat][1::-1] for mat, _ in units]
    for wide_w, thin_w in widths:
        outs += [jax.ShapeDtypeStruct((2 * SEQ_LEN, wide_w), bf16), jax.ShapeDtypeStruct((2 * SEQ_LEN, thin_w), bf16)]
    outs += [jax.ShapeDtypeStruct(MATRICES[mat][:2], f32) for mat, _ in units]
    for unit in LATE:
        wide_w, thin_w = widths[units.index(unit)]
        outs += [jax.ShapeDtypeStruct((SEQ_LEN, 2 * wide_w), bf16), jax.ShapeDtypeStruct((SEQ_LEN, thin_w), bf16)]
    sizes = [(MATRICES[mat][0] // chunk_count(mat, layer) // 2, MATRICES[mat][1], first_axis(mat, layer) == 'z') for mat, layer, _ in CHUNKS]
    scratch = [pltpu.VMEM((r, c), f32) for r, c, _ in sizes]
    scratch += [pltpu.VMEM((r // 2 if pairs else r, c), f32) for r, c, pairs in sizes]
    scratch += [pltpu.VMEM((r // 2 if pairs else r, c // 2), f32) for r, c, pairs in sizes]
    n_chunk, n_unit = len(CHUNKS), len(units)
    most_rows, most_cols = max(m[0] for m in MATRICES), max(m[1] for m in MATRICES)
    scratch += [pltpu.VMEM((TOKENS, most_rows), bf16), pltpu.VMEM((TOKENS, most_cols), bf16), pltpu.VMEM((most_rows, most_cols), f32),
                pltpu.VMEM((2, STREAM_ROWS, most_cols), f32),
                pltpu.VMEM((5,) + gains.shape, f32), pltpu.VMEM((5,) + gains.shape, f32),
                pltpu.SemaphoreType.DMA((n_chunk, N_SEMS)), pltpu.SemaphoreType.DMA((n_chunk, N_SEMS)), pltpu.SemaphoreType.DMA((n_chunk,)), pltpu.SemaphoreType.DMA((2,)),
                pltpu.SemaphoreType.DMA((5,)), pltpu.SemaphoreType.DMA((5,)),
                pltpu.SemaphoreType.DMA((n_unit, 6)), pltpu.SemaphoreType.DMA((n_unit, 6)), pltpu.SemaphoreType.DMA((n_unit, 7))]
    hbm, vmem = pl.BlockSpec(memory_space=pl.ANY), pl.BlockSpec(memory_space=pltpu.VMEM)
    flat = [val for group in operands for val in group]
    results = pl.pallas_call(
        functools.partial(combine_kernel, n_dev, n_layers),
        out_shape=tuple(outs),
        in_specs=[hbm] * len(flat) + [vmem],
        out_specs=tuple([hbm] * 4 + [vmem] + [hbm] * (len(outs) - 5)),
        scratch_shapes=scratch,
        compiler_params=pltpu.CompilerParams(has_side_effects=True, vmem_limit_bytes=VMEM_LIMIT),
    )(*flat, gains)
    return results[:5]


def solution(mesh):
    n_dev = mesh.shape[AXIS]

    def local_step(x_loc, grad_y_loc, gain_one, gain_two, w_qkv, w_out, w_up, w_down):
        n_layers = w_qkv.shape[0]
        grad_x, gains, operands = compute(x_loc, grad_y_loc, gain_one, gain_two, w_qkv, w_out, w_up, w_down)
        down, up, out, qkv, gains = combine(operands, gains, n_dev, n_layers)
        return (grad_x[None], gains[:n_layers], gains[n_layers:2 * n_layers], qkv, out, up, down)

    batch_spec = P(AXIS)
    full_spec = P()
    return jax.shard_map(local_step, mesh=mesh, in_specs=(batch_spec, batch_spec) + (full_spec,) * 6, out_specs=(batch_spec,) + (full_spec,) * 6, check_vma=False)
```

```python
import functools

import jax
import jax.numpy as jnp
from jax import lax
from jax.experimental import pallas as pl
from jax.experimental.pallas import tpu as pltpu
from jax.sharding import PartitionSpec as P

NORM_EPS = 1e-6
HEAD_DIM = 64
AXIS = 'data'
CHUNK_UNITS = '21011010113000000131100120011110'
ORDER = (
    'a9a0b9c9e9maa1b0c0d0e0a2fab1g9f9a3c1f0g0b2e1h0d1a4j9b3i0c2g1',
    'j0c3b4e2f1k0c4h1m9a5e3i1d2l0m0b5g2d3e4c5k1b6n0g3a7h2j1a6d4o0',
    'i2l1p0h3c6m1i3g4f2aek2a8b7b8n1l2e6c7h4c8j2e5f3m2d5k3n2i4d6l3',
    'o1p1m3g6f4j3p2g5n3k4o2h6e7e8h5d7d8j4p3l4i5i6m4f5o3n4g7k6k5g8',
    'l6p4m6i7f7i8h7n6o4h8j5l5k7m5k8j7p6n5f6o5j6l7l8p5m7fem8f8n7n8',
    'o6o7p7jeo8p8j8',
)
VMEM_LIMIT = 63 * 1024 * 1024


MATRICES = ((1024, 1024, 0), (1024, 1024, 1), (256, 1024, 0), (1024, 768, 1))
KIND = ('xyyX', 'yxXY')
LATE = ((2, 0), (3, 0))
SEQ_LEN = 384
TOKENS = 4 * SEQ_LEN
TILE_ROWS = 256
STREAM_ROWS = 64
N_SEMS = 12
ADD_ROWS = 32


def read_chunks(text):
    found = []
    for mat, layer in zip(*[map(int, text)] * 2):
        found.append((mat, layer, sum(chunk[:2] == (mat, layer) for chunk in found)))
    return tuple(found)


CHUNKS = read_chunks(CHUNK_UNITS)


def first_axis(mat, layer):
    kind = KIND[layer][mat]
    return kind if kind in 'xy' else 'z'


def chunk_count(mat, layer):
    return sum(chunk[:2] == (mat, layer) for chunk in CHUNKS)


PAIR = 2 * HEAD_DIM
GROUP = 2 * PAIR
Q_BLOCK = 128
FF_BLOCK = 512
NORM_ROWS = 64
FORWARD_STEPS = ((0, 1, 2),)
BACKWARD_STEPS = ((2, 1, 0),)
GELU_C = 0.7978845608028654
GELU_D = 0.044715


def dot_with(dims):
    return lambda lhs, rhs: lax.dot_general(lhs, rhs, (dims, ((), ())), preferred_element_type=jnp.float32)


dot_nn, dot_nt, dot_tn = (dot_with(((left,), (right,))) for left, right in ((1, 0), (1, 1), (0, 0)))


def rounded(val):
    return val.astype(jnp.bfloat16)


def wide_float(val):
    return val.astype(jnp.float32)


def row_blocks(count):
    def wrap(body):
        @pl.loop(0, count // NORM_ROWS)
        def _(step):
            body(pl.ds(pl.multiple_of(step * NORM_ROWS, NORM_ROWS), NORM_ROWS))
    return wrap


def inverse_rms(rows_f):
    return lax.rsqrt(jnp.mean(rows_f * rows_f, axis=-1, keepdims=True) + NORM_EPS)


def norm_forward(src, gain, dst):
    @row_blocks(src.shape[0])
    def _(at):
        rows_f = wide_float(src[at, :])
        dst[at, :] = rounded(rows_f * inverse_rms(rows_f) * gain[...])


def norm_backward(src, gain, grad_norm, grad_res, dst, gain_dst):
    gain_dst[...] = jnp.zeros_like(gain_dst)

    @row_blocks(src.shape[0])
    def _(at):
        rows_f = wide_float(src[at, :])
        scale = inverse_rms(rows_f)
        unit = rows_f * scale
        grad = wide_float(rounded(grad_norm[at, :]))
        gain_dst[...] += jnp.sum(grad * unit, axis=0, keepdims=True)
        grad = grad * gain[...]
        grad = scale * (grad - unit * jnp.mean(grad * unit, axis=-1, keepdims=True))
        dst[at, :] = rounded(wide_float(grad_res[at, :]) + grad)


def two_heads(rows):
    first = lax.broadcasted_iota(jnp.int32, rows.shape, 1) < HEAD_DIM
    zero = jnp.zeros_like(rows)
    return jnp.concatenate([jnp.where(first, rows, zero), jnp.where(first, zero, rows)], axis=0)


def one_pair(rows):
    half = rows.shape[0] // 2
    first = lax.broadcasted_iota(jnp.int32, (half, PAIR), 1) < HEAD_DIM
    return jnp.where(first, rows[:half], rows[half:])


def in_step(step, *lists):
    return [step(*args) for args in zip(*lists)]


def softmax_blocks(q_twos, k_all):
    scores = in_step(lambda q_two, k_rows: dot_nt(q_two, k_rows) * HEAD_DIM ** -0.5, q_twos, k_all)
    shape = (2 * Q_BLOCK, Q_BLOCK)
    seen = lax.rem(lax.broadcasted_iota(jnp.int32, shape, 0), Q_BLOCK) >= lax.broadcasted_iota(jnp.int32, shape, 1)

    def masked(score):
        before = score.shape[1] - Q_BLOCK
        last = jnp.where(seen, score[:, before:], -1e30)
        return jnp.concatenate([score[:, :before], last], axis=1) if before else last
    scores = in_step(masked, scores)
    peaks = in_step(lambda score: jnp.max(score, axis=-1, keepdims=True), scores)
    weights = in_step(lambda score, peak: jnp.exp(score - peak), scores, peaks)
    totals = in_step(lambda weight: 1.0 / jnp.sum(weight, axis=-1, keepdims=True), weights)
    return in_step(lambda weight, total: weight * total, weights, totals)


def jobs_of(blocks):
    return [(pl.ds(block * Q_BLOCK, Q_BLOCK), pl.ds(0, (block + 1) * Q_BLOCK), pl.ds(pair * PAIR, PAIR)) for block in blocks for pair in range(GROUP // PAIR)]


def attend(q_ref, k_ref, v_ref, o_ref):
    for blocks in FORWARD_STEPS:
        jobs = jobs_of(blocks)
        probs = softmax_blocks([two_heads(q_ref[rows, lanes]) for rows, _, lanes in jobs], [k_ref[keys, lanes] for _, keys, lanes in jobs])
        results = in_step(lambda prob, job: dot_nn(rounded(prob), v_ref[job[1], job[2]]), probs, jobs)
        for result, (rows, _, lanes) in zip(results, jobs):
            o_ref[rows, lanes] = rounded(one_pair(result))


def attend_backward(do_ref, q_ref, k_ref, v_ref, k_acc, v_acc):
    for blocks in BACKWARD_STEPS:
        jobs = jobs_of(blocks)
        q_twos, g_twos = ([two_heads(ref[rows, lanes]) for rows, _, lanes in jobs] for ref in (q_ref, do_ref))
        k_rows = [k_ref[keys, lanes] for _, keys, lanes in jobs]
        grad_probs = in_step(lambda g_two, job: dot_nt(g_two, v_ref[job[1], job[2]]), g_twos, jobs)
        probs = softmax_blocks(q_twos, k_rows)
        means = in_step(lambda prob, grad_prob: jnp.sum(prob * grad_prob, axis=-1, keepdims=True), probs, grad_probs)
        grad_s = in_step(lambda prob, grad_prob, mean: rounded(prob * (grad_prob - mean) * HEAD_DIM ** -0.5), probs, grad_probs, means)
        q_grads = in_step(dot_nn, grad_s, k_rows)
        k_parts = in_step(dot_tn, grad_s, q_twos)
        v_parts = in_step(lambda prob, g_two: dot_tn(rounded(prob), g_two), probs, g_twos)
        for q_grad, k_part, v_part, (rows, keys, lanes) in zip(q_grads, k_parts, v_parts, jobs):
            q_ref[rows, lanes] = rounded(one_pair(q_grad))
            if keys.size == q_ref.shape[0]:
                k_acc[:, lanes] = k_part
                v_acc[:, lanes] = v_part
            else:
                k_acc[keys, lanes] += k_part
                v_acc[keys, lanes] += v_part
    k_ref[...] = rounded(k_acc[...])
    v_ref[...] = rounded(v_acc[...])


KEPT = {'u_one': 1, 'mixed': 1, 'u_two': 1, 'act': 4, 'grad_pre': 4, 'grad_hidden': 1, 'grad_qkv': 3, 'grad': 1}
FACTORS = (('act', 'grad'), ('u_two', 'grad_pre'), ('mixed', 'grad_hidden'), ('u_one', 'grad_qkv'))


def own_place(me):
    core, x_at, y_at, z_at = lax.rem(me, 2), lax.rem(lax.div(me, 2), 2), lax.rem(lax.div(me, 4), 2), lax.div(me, 8)
    half = lax.div(z_at, 2)
    place = {'core': core, 'x': x_at, 'y': y_at, 'z': lax.rem(z_at, 2), 'half': half}
    to = {}
    for name, stride in (('core', 1), ('x', 2), ('y', 4), ('z', 8)):
        to[name] = me + stride * (1 - 2 * place[name])
    inward = 8 * (1 - 2 * half)
    to.update(mid=me + inward, end=me - inward, far=me + 2 * inward)
    return place, to, lax.div(z_at + 1, 2) == 1, lax.div(z_at + 1, 2) != 1


def compute_kernel(n_layers, x_in, grad_in, gain_one, gain_two, w_qkv, w_out, w_up, w_down, *refs):
    refs = list(refs)

    def take(count):
        head, refs[:] = refs[:count], refs[count:]
        return head

    grad_out, gain_out = take(2)
    kept = [dict(zip(KEPT, take(len(KEPT)))) for _ in range(n_layers)]
    units = [(mat, layer) for layer in range(n_layers) for mat in range(len(MATRICES))]
    early = [unit for unit in units if unit not in LATE]
    from_chip = dict(zip(early, zip(take(len(early)), take(len(early)))))
    rows, hidden, qkv, pre = (take(n_layers) for _ in range(4))
    unit_rows, mixed, act, grad_hidden, grad, do_ref, k_acc, v_acc, acc, s_qkv, s_out, s_up, s_down = take(13)
    sem_qkv, sem_out, sem_up, sem_down, sem_in, sem_put, sem_send, sem_recv = refs
    place, to, _, _ = own_place(lax.axis_index(AXIS))
    n_group, n_ff = s_out.shape[0], s_up.shape[0]

    def fetch_group(layer, at):
        cols = [pl.ds(pl.multiple_of((which * n_group + at) * GROUP, GROUP), GROUP) for which in range(3)]
        pieces = [pltpu.make_async_copy(w_qkv.at[layer, :, cols[which]], s_qkv.at[which, at], sem_qkv.at[which, at]) for which in range(3)]
        return pieces + [pltpu.make_async_copy(w_out.at[layer, pl.ds(pl.multiple_of(at * GROUP, GROUP), GROUP), :], s_out.at[at], sem_out.at[at])]

    def fetch_up(layer, at):
        return pltpu.make_async_copy(w_up.at[layer, :, pl.ds(pl.multiple_of(at * FF_BLOCK, FF_BLOCK), FF_BLOCK)], s_up.at[at], sem_up.at[at])

    def fetch_down(layer, at):
        return pltpu.make_async_copy(w_down.at[layer, pl.ds(pl.multiple_of(at * FF_BLOCK, FF_BLOCK), FF_BLOCK), :], s_down.at[at], sem_down.at[at])

    def start_groups(layer):
        for at in range(n_group):
            for piece in fetch_group(layer, at):
                piece.start()

    def start_all(fetch, layer):
        for at in range(n_ff):
            fetch(layer, at).start()

    n_put, sent, waiting = [0], [], []

    def put(src, dst):
        copy = pltpu.make_async_copy(src, dst, sem_put.at[n_put[0]])
        n_put[0] += 1
        copy.start()
        return copy

    def put_blocks(src, dst):
        count, _, cols = src.shape
        return [put(src.at[at], dst.at[:, pl.ds(at * cols, cols)]) for at in range(count)]

    def exchange(mat, layer, which):
        if (mat, layer) in LATE:
            return
        axis, split = first_axis(mat, layer), MATRICES[mat][2]
        name = FACTORS[mat][which]
        src = grad_in.at[0] if (name, layer) == ('grad', n_layers - 1) else kept[layer][name]
        if which == split:
            dst = from_chip[(mat, layer)][0]
            src = src.at[:, pl.ds(pl.multiple_of((1 - place[axis]) * dst.shape[1], 128), dst.shape[1])]
        else:
            dst = from_chip[(mat, layer)][1]
        copy = pltpu.make_async_remote_copy(src_ref=src, dst_ref=dst, send_sem=sem_send.at[len(sent)], recv_sem=sem_recv.at[len(sent)],
                                            device_id=(to[axis],), device_id_type=pl.DeviceIdType.MESH)
        sent.append(copy)
        copy.start()

    def save(name, layer, copies):
        waiting.append((name, layer, copies))

    def flush():
        for name, layer, copies in waiting:
            for copy in copies:
                copy.wait()
            for mat, names in enumerate(FACTORS):
                if name in names:
                    exchange(mat, layer, names.index(name))
        waiting.clear()

    def gain_row(gain, layer):
        return gain.at[pl.ds(layer, 1), :]

    def attention_forward(layer):
        flush()
        norm_forward(rows[layer], gain_row(gain_one, layer), unit_rows)
        save('u_one', layer, [put(unit_rows, kept[layer]['u_one'])])
        acc[...] = jnp.zeros_like(acc)
        q_all, k_all, v_all = (qkv[layer].at[which] for which in range(3))

        @pl.loop(0, n_group)
        def _(at):
            for piece in fetch_group(layer, at):
                piece.wait()
            for which in range(3):
                qkv[layer][which, at] = rounded(dot_nn(unit_rows[...], s_qkv[which, at]))
            attend(q_all.at[at], k_all.at[at], v_all.at[at], mixed.at[at])
            acc[...] += dot_nn(mixed[at], s_out[at])
        save('mixed', layer, put_blocks(mixed, kept[layer]['mixed']))
        hidden[layer][...] = rows[layer][...] + rounded(acc[...])

    def mlp_forward(layer):
        last = layer + 1 == n_layers
        flush()
        norm_forward(hidden[layer], gain_row(gain_two, layer), unit_rows)
        save('u_two', layer, [put(unit_rows, kept[layer]['u_two'])])
        acc[...] = jnp.zeros_like(acc)

        @pl.loop(0, n_ff)
        def _(at):
            fetch_up(layer, at).wait()
            pre[layer][at] = rounded(dot_nn(unit_rows[...], s_up[at]))
            rows_f = wide_float(pre[layer][at])
            bend = jnp.tanh(GELU_C * (rows_f + GELU_D * (rows_f * rows_f * rows_f)))
            act[at] = rounded(rows_f * (0.5 * (1.0 + bend)))
            if not last:
                fetch_down(layer, at).wait()
                acc[...] += dot_nn(act[at], s_down[at])
        save('act', layer, put_blocks(act, kept[layer]['act']))
        if not last:
            rows[layer + 1][...] = hidden[layer][...] + rounded(acc[...])

    def mlp_backward(layer, fetched):
        acc[...] = jnp.zeros_like(acc)

        @pl.loop(0, n_ff)
        def _(at):
            fetch_down(layer, at).wait()
            if not fetched:
                fetch_up(layer, at).wait()
            grad_a = wide_float(rounded(dot_nt(grad[...], s_down[at])))
            rows_f = wide_float(pre[layer][at])
            square = rows_f * rows_f
            bend = jnp.tanh(GELU_C * (rows_f + GELU_D * (square * rows_f)))
            slope = 0.5 * (1.0 + bend) + (0.5 * GELU_C) * rows_f * (1.0 - bend * bend) * (1.0 + (3.0 * GELU_D) * square)
            pre[layer][at] = rounded(slope * grad_a)
            acc[...] += dot_nt(pre[layer][at], s_up[at])
        flush()
        save('grad_pre', layer, put_blocks(pre[layer], kept[layer]['grad_pre']))
        norm_backward(hidden[layer], gain_row(gain_two, layer), acc, grad, grad_hidden, gain_row(gain_out, n_layers + layer))
        save('grad_hidden', layer, [put(grad_hidden, kept[layer]['grad_hidden'])])

    def attention_backward(layer, fetched):
        acc[...] = jnp.zeros_like(acc)

        @pl.loop(0, n_group)
        def _(at):
            if not fetched:
                for piece in fetch_group(layer, at):
                    piece.wait()
            do_ref[...] = rounded(dot_nt(grad_hidden[...], s_out[at]))
            attend_backward(do_ref, *(qkv[layer].at[which, at] for which in range(3)), k_acc, v_acc)
            for which in range(3):
                acc[...] += dot_nt(qkv[layer][which, at], s_qkv[which, at])
        flush()
        copies = []
        for which in range(3):
            width = grad.shape[1]
            copies += [put(qkv[layer].at[which, at], kept[layer]['grad_qkv'].at[:, pl.ds(which * width + at * GROUP, GROUP)]) for at in range(n_group)]
        save('grad_qkv', layer, copies)
        norm_backward(rows[layer], gain_row(gain_one, layer), acc, grad_hidden, grad, gain_row(gain_out, layer))

    first = pltpu.make_async_copy(x_in.at[0], rows[0], sem_in.at[0])
    second = pltpu.make_async_copy(grad_in.at[0], grad, sem_in.at[1])
    first.start()
    start_groups(0)
    start_all(fetch_up, 0)
    start_all(fetch_down, 0)
    second.start()
    exchange(0, n_layers - 1, 1)
    gain_out[...] = jnp.zeros_like(gain_out)
    first.wait()
    for layer in range(n_layers):
        attention_forward(layer)
        if layer + 1 < n_layers:
            start_groups(layer + 1)
        mlp_forward(layer)
        if layer + 1 < n_layers:
            start_all(fetch_up, layer + 1)
            start_all(fetch_down, layer + 1)
    second.wait()
    flush()
    for layer in reversed(range(n_layers)):
        top = layer + 1 == n_layers
        mlp_backward(layer, top)
        if layer > 0:
            start_all(fetch_up, layer - 1)
            start_all(fetch_down, layer - 1)
        flush()
        attention_backward(layer, top)
        if layer > 0:
            start_groups(layer - 1)
            save('grad', layer - 1, [put(grad, kept[layer - 1]['grad'])])
            flush()
    done = put(grad, grad_out)
    flush()
    done.wait()
    for copy in sent:
        copy.wait()


def compute(x_loc, grad_loc, gain_one, gain_two, w_qkv, w_out, w_up, w_down):
    n_layers, width, inner = w_up.shape
    seq_len = x_loc.shape[1]
    f32, bf16 = jnp.float32, jnp.bfloat16
    n_group, n_ff = width // GROUP, inner // FF_BLOCK
    units = [(mat, layer) for layer in range(n_layers) for mat in range(len(MATRICES))]
    early = [unit for unit in units if unit not in LATE]

    def lo(*shape):
        return jax.ShapeDtypeStruct(shape, bf16)
    outs = [lo(seq_len, width), jax.ShapeDtypeStruct((8, width), f32)]
    outs += [lo(seq_len, cols * width) for _ in range(n_layers) for cols in KEPT.values()]
    shapes = [[KEPT[name] * width for name in FACTORS[mat]] for mat, _ in early]
    outs += [lo(seq_len, shape[MATRICES[mat][2]] // 2) for shape, (mat, _) in zip(shapes, early)]
    outs += [lo(seq_len, shape[1 - MATRICES[mat][2]]) for shape, (mat, _) in zip(shapes, early)]
    wide_rows, groups = (seq_len, width), (n_group, seq_len, GROUP)
    vmem = [wide_rows] * (2 * n_layers) + [(3,) + groups] * n_layers + [(n_ff, seq_len, FF_BLOCK)] * n_layers
    vmem += [wide_rows, groups, (n_ff, seq_len, FF_BLOCK), wide_rows, wide_rows, (seq_len, GROUP)]
    scratch = [pltpu.VMEM(shape, bf16) for shape in vmem] + [pltpu.VMEM(shape, f32) for shape in ((seq_len, GROUP), (seq_len, GROUP), wide_rows)]
    scratch += [pltpu.VMEM(shape, bf16) for shape in ((3, n_group, width, GROUP), (n_group, GROUP, width), (n_ff, width, FF_BLOCK), (n_ff, FF_BLOCK, width))]
    scratch += [pltpu.SemaphoreType.DMA(shape) for shape in ((3, n_group), (n_group,), (n_ff,), (n_ff,), (2,), (100,), (2 * len(early),), (2 * len(early),))]
    hbm, near = pl.BlockSpec(memory_space=pl.ANY), pl.BlockSpec(memory_space=pltpu.VMEM)
    results = pl.pallas_call(
        functools.partial(compute_kernel, n_layers), out_shape=tuple(outs), in_specs=[hbm, hbm, near, near] + [hbm] * 4,
        out_specs=tuple([hbm, near] + [hbm] * (len(outs) - 2)), scratch_shapes=scratch,
        compiler_params=pltpu.CompilerParams(has_side_effects=True, vmem_limit_bytes=VMEM_LIMIT),
    )(x_loc, grad_loc, gain_one, gain_two, w_qkv, w_out, w_up, w_down)
    grad_x, gains = results[:2]
    kept = [dict(zip(KEPT, results[2 + layer * len(KEPT):])) for layer in range(n_layers)]
    kept[-1]['grad'] = grad_loc[0]
    tail = results[2 + n_layers * len(KEPT):]
    from_chip = dict(zip(early, zip(tail, tail[len(early):])))
    operands = []
    for mat, layer in units:
        pair = [kept[layer][name] for name in FACTORS[mat]]
        split = MATRICES[mat][2]
        operands.append((pair[split], pair[1 - split]) + from_chip.get((mat, layer), ()))
    return grad_x, gains, operands


def add_rows(dst, src, cols, scale=None):
    rows = dst.shape[0]

    @pl.loop(0, rows // ADD_ROWS)
    def _(step):
        at = pl.ds(pl.multiple_of(step * ADD_ROWS, ADD_ROWS), ADD_ROWS)
        val = dst[at, cols] + src[at, :]
        dst[at, cols] = val if scale is None else val * scale


def flip(bit, by):
    return 1 - bit if by else bit


def combine_kernel(n_dev, n_layers, *refs):
    units = [(mat, layer) for layer in range(n_layers) for mat in range(len(MATRICES))]
    n_chunk = len(CHUNKS)
    refs = list(refs)

    def take(count):
        head, refs[:] = refs[:count], refs[count:]
        return head

    given = [take(2 if unit in LATE else 4) for unit in units]
    gain_in, = take(1)
    outs, (gain_out,) = take(len(MATRICES)), take(1)
    from_core, part_refs, from_chip = take(2 * len(units)), take(len(units)), take(2 * len(LATE))
    land_q, land_z, land_h = (take(n_chunk) for _ in range(3))
    row_op, col_op, product, stream, gain_buf, gain_land, send_sems, recv_sems, local_sems, stream_sems, gain_send, gain_recv, op_send, op_recv, op_local = refs

    me = lax.axis_index(AXIS)
    place, to, middle, edge = own_place(me)
    core, half = place['core'], place['half']

    def remote(src, dst, i, sem, dev):
        return pltpu.make_async_remote_copy(src_ref=src, dst_ref=dst, send_sem=send_sems.at[i, sem], recv_sem=recv_sems.at[i, sem],
                                            device_id=(dev,), device_id_type=pl.DeviceIdType.MESH)

    def out_block(i, p_at, c_at, row, n_rows, h_at):
        mat, layer, k = CHUNKS[i]
        rows_all, cols, split = MATRICES[mat]
        quarter = p_at * 2 + c_at
        row = row + k * (rows_all // chunk_count(mat, layer)) + (quarter * rows_all if split == 0 else 0)
        col, n_cols = (0, cols) if h_at is None else (h_at * (cols // 2), cols // 2)
        if split == 1:
            col = col + quarter * cols
        return outs[mat].at[layer, pl.ds(pl.multiple_of(row, 8), n_rows), pl.ds(col if isinstance(col, int) else pl.multiple_of(col, 128), n_cols)]

    def stream_add(dst, src):
        rows, cols = dst.shape
        size = min(STREAM_ROWS, rows)
        steps = rows // size

        def fetch(step, slot):
            return pltpu.make_async_copy(src.at[pl.ds(pl.multiple_of(step * size, size), size), :], stream.at[slot, pl.ds(0, size), pl.ds(0, cols)], stream_sems.at[slot])
        fetch(0, 0).start()

        @pl.loop(0, steps)
        def _(step):
            slot = lax.rem(step, 2)

            @pl.when(step + 1 < steps)
            def _():
                fetch(step + 1, 1 - slot).start()
            fetch(step, slot).wait()
            at = pl.ds(pl.multiple_of(step * size, size), size)
            dst[at, :] = dst[at, :] + stream[slot, pl.ds(0, size), pl.ds(0, cols)]

    def run(i, stage, pending):
        mat, layer, k = CHUNKS[i]
        rows_all, cols, _ = MATRICES[mat]
        kind, p_name = KIND[layer][mat], first_axis(mat, layer)
        by_pairs = p_name == 'z'
        q_name = kind.lower() if by_pairs else 'xy'.replace(kind, '')
        r_name = 'xy'.replace(q_name, '')
        rows = rows_all // chunk_count(mat, layer)
        part = part_refs[layer * len(MATRICES) + mat]
        p_at, q_at, r_at = place[p_name], place[q_name], place[r_name]

        def go(src, dst, sem, dest, cond=None):
            remote(src(), dst(), i, sem, to[dest]).start()
            pending.append((cond, src, i, sem))

        def block(dp=0, dq=0, dc=0, dr=None, dh=None):
            def ref():
                row, count = flip(q_at, dq) * (rows // 2), rows // 2
                if dr is not None:
                    row, count = row + flip(r_at, dr) * (rows // 4), rows // 4
                return out_block(i, flip(p_at, dp), flip(core, dc), row, count, None if dh is None else flip(half, dh))
            return ref

        def pass_on(blk, sems, cond=None):
            for dest, sem in sems:
                go(blk, blk, sem, dest, cond)

        def arrived(blk, sem):
            remote(blk(), blk(), i, sem, me).wait_recv()

        def half_cols(by):
            return pl.ds(pl.multiple_of(flip(half, by) * (cols // 2), 128), cols // 2)

        def own_rows(by):
            return land_q[i].at[pl.ds(pl.multiple_of(flip(r_at, by) * (rows // 4), 8), rows // 4), :] if by_pairs else land_q[i]

        def own_half(by):
            return lambda: (land_q[i].at[pl.ds(pl.multiple_of(r_at * (rows // 4), 8), rows // 4), half_cols(by)] if by_pairs
                            else land_q[i].at[:, half_cols(by)])

        def rows_of(by):
            return lambda: part.at[pl.ds(pl.multiple_of(k * rows + flip(q_at, by) * (rows // 2), 8), rows // 2), :]

        last = dict(dr=0) if by_pairs else {}

        def keep():
            return pltpu.make_async_copy(own_half(0)(), block(dh=0, **last)(), local_sems.at[i])

        def whole(buf):
            return lambda: buf[i]

        def scale_and_send(dest):
            add_rows(own_rows(0), land_h[i], half_cols(0), 1.0 / n_dev)
            keep().start()
            go(own_half(0), block(dh=0, **last), 3, dest, None if by_pairs else middle)

        def spread(turn):
            if turn == 0:
                pass_on(block(), ((q_name, 5), (p_name, 6), ('core', 8)))
            elif turn == 1:
                arrived(block(dq=1), 5)
                pass_on(block(dq=1), ((p_name, 7), ('core', 9)))
            else:
                dq = turn - 2
                arrived(block(dp=1, dq=dq), turn + 4)
                pass_on(block(dp=1, dq=dq), (('core', turn + 8),))

        if stage == 0:
            go(rows_of(1), whole(land_q), 0, q_name)
        elif stage == 8:
            for turn in range(4):
                arrived(block(dp=turn // 2, dq=turn % 2, dc=1), 8 + turn)
        elif by_pairs:
            if stage == 1:
                arrived(whole(land_q), 0)
                stream_add(land_q[i], rows_of(0)())
                go(lambda: own_rows(1), whole(land_z), 1, r_name)
            elif stage == 2:
                arrived(whole(land_z), 1)
                add_rows(own_rows(0), land_z[i], slice(None))
                go(own_half(1), whole(land_h), 2, 'far')
            elif stage == 3:
                arrived(whole(land_h), 2)
                scale_and_send('far')
            elif stage == 4:
                keep().wait()
                arrived(block(dr=0, dh=1), 3)
                go(block(dr=0), block(dr=0), 4, r_name)
            else:
                if stage == 5:
                    arrived(block(dr=1), 4)
                spread(min(stage - 5, 3))
        elif stage == 1:
            arrived(whole(land_q), 0)
            stream_add(land_q[i], rows_of(0)())

            @pl.when(edge)
            def _():
                go(whole(land_q), whole(land_z), 1, 'mid', edge)
        elif stage in (2, 3):
            @pl.when(middle)
            def _():
                arrived(whole((land_z, land_h)[stage - 2]), stage - 1)
                if stage == 2:
                    add_rows(land_q[i], land_z[i], slice(None))
                    go(own_half(1), whole(land_h), 2, 'mid', middle)
                else:
                    scale_and_send('mid')
        else:
            if stage == 4:
                @pl.when(middle)
                def _():
                    keep().wait()
                    arrived(block(dh=1), 3)
                    pass_on(block(), (('end', 4),), middle)

                @pl.when(edge)
                def _():
                    arrived(block(), 4)
            spread(stage - 4)

    def unit_sizes(unit):
        rows, cols, split = MATRICES[unit[0]]
        p_name = first_axis(*unit)
        return (rows, cols, p_name, split) + ((rows, cols) if split == 0 else (cols, rows))

    def operand_copy(u, which, src, dst, dest):
        return pltpu.make_async_remote_copy(src_ref=src, dst_ref=dst, send_sem=op_send.at[u, which], recv_sem=op_recv.at[u, which],
                                            device_id=(to[dest],), device_id_type=pl.DeviceIdType.MESH)

    def operand_copies(u):
        unit = units[u]
        rows, cols, p_name, split, wide_w, _ = unit_sizes(unit)
        p_at = place[p_name]
        wide, thin = given[u][:2]
        core_wide, core_thin = from_core[2 * u:2 * u + 2]
        if unit in LATE:
            late = LATE.index(unit)
            chip_wide, chip_thin = from_chip[2 * late:2 * late + 2]
        else:
            chip_wide, chip_thin = given[u][2:]
        first, second = pl.ds(0, SEQ_LEN), pl.ds(SEQ_LEN, SEQ_LEN)

        def lanes(at, count):
            return pl.ds(pl.multiple_of(at, 128), count)
        other = 1 - core
        copies = {
            'own': (operand_copy(u, 0, wide.at[:, lanes((p_at * 2 + other) * wide_w, wide_w)], core_wide.at[first, :], 'core'),
                    operand_copy(u, 1, thin, core_thin.at[first, :], 'core')),
            'next': (operand_copy(u, 2, chip_wide.at[:, lanes(other * wide_w, wide_w)], core_wide.at[second, :], 'core'),
                     operand_copy(u, 3, chip_thin, core_thin.at[second, :], 'core')),
        }
        if unit in LATE:
            copies['chip'] = (operand_copy(u, 4, wide.at[:, lanes((1 - p_at) * 2 * wide_w, 2 * wide_w)], chip_wide, p_name),
                              operand_copy(u, 5, thin, chip_thin, p_name))
        wide_op, thin_op = (row_op, col_op) if split == 0 else (col_op, row_op)
        thin_w = thin.shape[1]
        loads = []
        for start, src in ((0, wide.at[:, lanes((p_at * 2 + core) * wide_w, wide_w)]), (SEQ_LEN, chip_wide.at[:, lanes(core * wide_w, wide_w)]),
                           (2 * SEQ_LEN, core_wide)):
            loads.append((src, wide_op.at[pl.ds(start, src.shape[0]), pl.ds(0, wide_w)]))
        for start, src in ((0, thin), (SEQ_LEN, chip_thin), (2 * SEQ_LEN, core_thin)):
            loads.append((src, thin_op.at[pl.ds(start, src.shape[0]), pl.ds(0, thin_w)]))
        copies['load'] = tuple(pltpu.make_async_copy(src, dst, op_local.at[u, n]) for n, (src, dst) in enumerate(loads))
        return copies

    def start_operands(u):
        copies = operand_copies(u)
        if units[u] in LATE:
            for copy in copies['chip']:
                copy.start()
        for copy in copies['own']:
            copy.start()
        if units[u] not in LATE:
            for copy in copies['next']:
                copy.start()

    def forward_operands(u):
        copies = operand_copies(u)
        for copy in copies['chip']:
            copy.wait_recv()
        for copy in copies['next']:
            copy.start()

    def multiply(u):
        rows, cols, _, _, _, _ = unit_sizes(units[u])
        copies = operand_copies(u)
        for copy in copies['own'] + copies['next']:
            copy.wait_recv()
        for copy in copies['load']:
            copy.start()
        for copy in copies['load']:
            copy.wait()
        tile = min(TILE_ROWS, rows)
        half_w = cols // 2

        @pl.loop(0, rows // tile)
        def _(step):
            at = pl.ds(pl.multiple_of(step * tile, tile), tile)
            for side in range(2):
                lanes = pl.ds(side * half_w, half_w)
                product[at, lanes] = dot_tn(row_op[:, at], col_op[:, lanes])
        store = pltpu.make_async_copy(product.at[pl.ds(0, rows), pl.ds(0, cols)], part_refs[u], op_local.at[u, 6])
        store.start()
        store.wait()

    def finish_operands(u):
        copies = operand_copies(u)
        for copy in copies['own'] + copies['next'] + copies.get('chip', ()):
            copy.wait_send()

    gain_steps = ('core', 'x', 'y', 'z', 'far')

    def gain_copy(step):
        return pltpu.make_async_remote_copy(src_ref=gain_buf.at[step], dst_ref=gain_land.at[step], send_sem=gain_send.at[step],
                                            recv_sem=gain_recv.at[step], device_id=(to[gain_steps[step]],), device_id_type=pl.DeviceIdType.MESH)

    def gain_next(step):
        copy = gain_copy(step)
        copy.wait()
        total = gain_buf[step] + gain_land[step]
        if step + 1 < len(gain_steps):
            gain_buf[step + 1] = total
            gain_copy(step + 1).start()
        else:
            gain_out[...] = total * (1.0 / n_dev)

    pending = []
    gain_buf[0] = gain_in[...]
    step = 0
    first_use = []
    for mat, layer, _ in CHUNKS:
        if units.index((mat, layer)) not in first_use:
            first_use.append(units.index((mat, layer)))
    for u in first_use:
        start_operands(u)
    for count, (letter, digit) in enumerate(zip(*[iter(''.join(ORDER))] * 2)):
        i, stage = ord(letter) - ord('a'), int(digit, 16)
        u = units.index(CHUNKS[i][:2])
        if stage == 9:
            multiply(u)
        elif stage == 10:
            forward_operands(u)
        else:
            run(i, stage, pending)
        if count == 1:
            gain_copy(0).start()
        if count >= 8 and count % 6 == 0 and step < len(gain_steps):
            gain_next(step)
            step += 1
    for u in range(len(units)):
        finish_operands(u)
    for cond, src, i, sem in pending:
        def finish(src=src, i=i, sem=sem):
            remote(src(), src(), i, sem, me).wait_send()
        if cond is None:
            finish()
        else:
            pl.when(cond)(finish)


def combine(operands, gains, n_dev, n_layers):
    f32, bf16 = jnp.float32, jnp.bfloat16
    units = [(mat, layer) for layer in range(n_layers) for mat in range(len(MATRICES))]
    outs = []
    for rows, cols, split in MATRICES:
        outs.append(jax.ShapeDtypeStruct((n_layers, rows * (4 if split == 0 else 1), cols * (4 if split == 1 else 1)), f32))
    outs.append(jax.ShapeDtypeStruct(gains.shape, f32))
    widths = [MATRICES[mat][:2] if MATRICES[mat][2] == 0 else MATRICES[mat][1::-1] for mat, _ in units]
    for wide_w, thin_w in widths:
        outs += [jax.ShapeDtypeStruct((2 * SEQ_LEN, wide_w), bf16), jax.ShapeDtypeStruct((2 * SEQ_LEN, thin_w), bf16)]
    outs += [jax.ShapeDtypeStruct(MATRICES[mat][:2], f32) for mat, _ in units]
    for unit in LATE:
        wide_w, thin_w = widths[units.index(unit)]
        outs += [jax.ShapeDtypeStruct((SEQ_LEN, 2 * wide_w), bf16), jax.ShapeDtypeStruct((SEQ_LEN, thin_w), bf16)]
    sizes = [(MATRICES[mat][0] // chunk_count(mat, layer) // 2, MATRICES[mat][1], first_axis(mat, layer) == 'z') for mat, layer, _ in CHUNKS]
    scratch = [pltpu.VMEM((r, c), f32) for r, c, _ in sizes]
    scratch += [pltpu.VMEM((r // 2 if pairs else r, c), f32) for r, c, pairs in sizes]
    scratch += [pltpu.VMEM((r // 2 if pairs else r, c // 2), f32) for r, c, pairs in sizes]
    n_chunk, n_unit = len(CHUNKS), len(units)
    most_rows, most_cols = max(m[0] for m in MATRICES), max(m[1] for m in MATRICES)
    scratch += [pltpu.VMEM((TOKENS, most_rows), bf16), pltpu.VMEM((TOKENS, most_cols), bf16), pltpu.VMEM((most_rows, most_cols), f32),
                pltpu.VMEM((2, STREAM_ROWS, most_cols), f32),
                pltpu.VMEM((5,) + gains.shape, f32), pltpu.VMEM((5,) + gains.shape, f32),
                pltpu.SemaphoreType.DMA((n_chunk, N_SEMS)), pltpu.SemaphoreType.DMA((n_chunk, N_SEMS)), pltpu.SemaphoreType.DMA((n_chunk,)), pltpu.SemaphoreType.DMA((2,)),
                pltpu.SemaphoreType.DMA((5,)), pltpu.SemaphoreType.DMA((5,)),
                pltpu.SemaphoreType.DMA((n_unit, 6)), pltpu.SemaphoreType.DMA((n_unit, 6)), pltpu.SemaphoreType.DMA((n_unit, 7))]
    hbm, vmem = pl.BlockSpec(memory_space=pl.ANY), pl.BlockSpec(memory_space=pltpu.VMEM)
    flat = [val for group in operands for val in group]
    results = pl.pallas_call(
        functools.partial(combine_kernel, n_dev, n_layers),
        out_shape=tuple(outs),
        in_specs=[hbm] * len(flat) + [vmem],
        out_specs=tuple([hbm] * 4 + [vmem] + [hbm] * (len(outs) - 5)),
        scratch_shapes=scratch,
        compiler_params=pltpu.CompilerParams(has_side_effects=True, vmem_limit_bytes=VMEM_LIMIT),
    )(*flat, gains)
    return results[:5]


def solution(mesh):
    n_dev = mesh.shape[AXIS]

    def local_step(x_loc, grad_y_loc, gain_one, gain_two, w_qkv, w_out, w_up, w_down):
        n_layers = w_qkv.shape[0]
        grad_x, gains, operands = compute(x_loc, grad_y_loc, gain_one, gain_two, w_qkv, w_out, w_up, w_down)
        down, up, out, qkv, gains = combine(operands, gains, n_dev, n_layers)
        return (grad_x[None], gains[:n_layers], gains[n_layers:2 * n_layers], qkv, out, up, down)

    batch_spec = P(AXIS)
    full_spec = P()
    return jax.shard_map(local_step, mesh=mesh, in_specs=(batch_spec, batch_spec) + (full_spec,) * 6, out_specs=(batch_spec,) + (full_spec,) * 6, check_vma=False)
```

```python
import functools

import jax
import jax.numpy as jnp
from jax import lax
from jax.experimental import pallas as pl
from jax.experimental.pallas import tpu as pltpu
from jax.sharding import PartitionSpec as P

NORM_EPS = 1e-6
HEAD_DIM = 64
AXIS = 'data'
CHUNK_UNITS = '1111110000100110012131303120113000003030'
ORDER = (
    'a9d9a0b0c0d0naa1f9e0lab1g9f0a2d1g0c1h0b2a3e1j9i0b3d2f1a4k9d3',
    'c2g1j0b4l9k0e2c3h1l0d4e3i1n9a5m0f2c4a6e4f3b5b6j1g2k1d6n0d5l1',
    'o0g3f4a7p0h2a8c6c5h3m1g4i2q0l2e5e6b7b8k2h4j2i3l3d7d8n1k3f6o1',
    'j3p1r0f5s0i4o2j4t0p2l4k4o3m2p3c7c8q1g5g6m3o4e7m4e8q2p4q3h5h6',
    'n2q4n3n4s1f7i6f8t1r1l5k5s2j5i5s3r2s4t2l6k7r3g7j7t3g8o6o5p5p6',
    'm5r4t4n5h7q6h8m7n7q5k6i7l7i8l8s5s6keo7j6o8k8r6p7m6r5jet5p8t6',
    'n6meq7m8q8j8r7s7r8nes8t7n8t8',
)
VMEM_LIMIT = 63 * 1024 * 1024


MATRICES = ((1024, 1024, 0), (1024, 1024, 1), (256, 1024, 0), (1024, 768, 1))
KIND = ('xyYy', 'xyYX')
LATE = ((2, 0), (3, 0))
SEQ_LEN = 384
TOKENS = 4 * SEQ_LEN
TILE_ROWS = 256
STREAM_ROWS = 64
N_SEMS = 12
ADD_ROWS = 32


def read_chunks(text):
    found = []
    for mat, layer in zip(*[map(int, text)] * 2):
        found.append((mat, layer, sum(chunk[:2] == (mat, layer) for chunk in found)))
    return tuple(found)


CHUNKS = read_chunks(CHUNK_UNITS)


def first_axis(mat, layer):
    kind = KIND[layer][mat]
    return kind if kind in 'xy' else 'z'


def chunk_count(mat, layer):
    return sum(chunk[:2] == (mat, layer) for chunk in CHUNKS)


PAIR = 2 * HEAD_DIM
GROUP = 2 * PAIR
Q_BLOCK = 128
FF_BLOCK = 512
NORM_ROWS = 128
FORWARD_STEPS = ((0, 1, 2),)
BACKWARD_STEPS = ((2, 1, 0),)
GELU_C = 0.7978845608028654
GELU_D = 0.044715


def dot_with(dims):
    return lambda lhs, rhs: lax.dot_general(lhs, rhs, (dims, ((), ())), preferred_element_type=jnp.float32)


dot_nn, dot_nt, dot_tn = (dot_with(((left,), (right,))) for left, right in ((1, 0), (1, 1), (0, 0)))


def rounded(val):
    return val.astype(jnp.bfloat16)


def wide_float(val):
    return val.astype(jnp.float32)


def row_blocks(count):
    def wrap(body):
        @pl.loop(0, count // NORM_ROWS)
        def _(step):
            body(pl.ds(pl.multiple_of(step * NORM_ROWS, NORM_ROWS), NORM_ROWS))
    return wrap


def inverse_rms(rows_f):
    return lax.rsqrt(jnp.mean(rows_f * rows_f, axis=-1, keepdims=True) + NORM_EPS)


def norm_forward(src, gain, dst):
    @row_blocks(src.shape[0])
    def _(at):
        rows_f = wide_float(src[at, :])
        dst[at, :] = rounded(rows_f * inverse_rms(rows_f) * gain[...])


def norm_backward(src, gain, grad_norm, grad_res, dst, gain_dst):
    gain_dst[...] = jnp.zeros_like(gain_dst)

    @row_blocks(src.shape[0])
    def _(at):
        rows_f = wide_float(src[at, :])
        scale = inverse_rms(rows_f)
        unit = rows_f * scale
        grad = wide_float(rounded(grad_norm[at, :]))
        gain_dst[...] += jnp.sum(grad * unit, axis=0, keepdims=True)
        grad = grad * gain[...]
        grad = scale * (grad - unit * jnp.mean(grad * unit, axis=-1, keepdims=True))
        dst[at, :] = rounded(wide_float(grad_res[at, :]) + grad)


def two_heads(rows):
    first = lax.broadcasted_iota(jnp.int32, rows.shape, 1) < HEAD_DIM
    zero = jnp.zeros_like(rows)
    return jnp.concatenate([jnp.where(first, rows, zero), jnp.where(first, zero, rows)], axis=0)


def one_pair(rows):
    half = rows.shape[0] // 2
    first = lax.broadcasted_iota(jnp.int32, (half, PAIR), 1) < HEAD_DIM
    return jnp.where(first, rows[:half], rows[half:])


def in_step(step, *lists):
    return [step(*args) for args in zip(*lists)]


def softmax_blocks(q_twos, k_all):
    scores = in_step(lambda q_two, k_rows: dot_nt(q_two, k_rows) * HEAD_DIM ** -0.5, q_twos, k_all)
    shape = (2 * Q_BLOCK, Q_BLOCK)
    seen = lax.rem(lax.broadcasted_iota(jnp.int32, shape, 0), Q_BLOCK) >= lax.broadcasted_iota(jnp.int32, shape, 1)

    def masked(score):
        before = score.shape[1] - Q_BLOCK
        last = jnp.where(seen, score[:, before:], -1e30)
        return jnp.concatenate([score[:, :before], last], axis=1) if before else last
    scores = in_step(masked, scores)
    peaks = in_step(lambda score: jnp.max(score, axis=-1, keepdims=True), scores)
    weights = in_step(lambda score, peak: jnp.exp(score - peak), scores, peaks)
    totals = in_step(lambda weight: 1.0 / jnp.sum(weight, axis=-1, keepdims=True), weights)
    return in_step(lambda weight, total: weight * total, weights, totals)


def jobs_of(blocks):
    return [(pl.ds(block * Q_BLOCK, Q_BLOCK), pl.ds(0, (block + 1) * Q_BLOCK), pl.ds(pair * PAIR, PAIR)) for block in blocks for pair in range(GROUP // PAIR)]


def attend(q_ref, k_ref, v_ref, o_ref):
    for blocks in FORWARD_STEPS:
        jobs = jobs_of(blocks)
        probs = softmax_blocks([two_heads(q_ref[rows, lanes]) for rows, _, lanes in jobs], [k_ref[keys, lanes] for _, keys, lanes in jobs])
        results = in_step(lambda prob, job: dot_nn(rounded(prob), v_ref[job[1], job[2]]), probs, jobs)
        for result, (rows, _, lanes) in zip(results, jobs):
            o_ref[rows, lanes] = rounded(one_pair(result))


def attend_backward(do_ref, q_ref, k_ref, v_ref, k_acc, v_acc):
    for blocks in BACKWARD_STEPS:
        jobs = jobs_of(blocks)
        q_twos, g_twos = ([two_heads(ref[rows, lanes]) for rows, _, lanes in jobs] for ref in (q_ref, do_ref))
        k_rows = [k_ref[keys, lanes] for _, keys, lanes in jobs]
        grad_probs = in_step(lambda g_two, job: dot_nt(g_two, v_ref[job[1], job[2]]), g_twos, jobs)
        probs = softmax_blocks(q_twos, k_rows)
        means = in_step(lambda prob, grad_prob: jnp.sum(prob * grad_prob, axis=-1, keepdims=True), probs, grad_probs)
        grad_s = in_step(lambda prob, grad_prob, mean: rounded(prob * (grad_prob - mean) * HEAD_DIM ** -0.5), probs, grad_probs, means)
        q_grads = in_step(dot_nn, grad_s, k_rows)
        k_parts = in_step(dot_tn, grad_s, q_twos)
        v_parts = in_step(lambda prob, g_two: dot_tn(rounded(prob), g_two), probs, g_twos)
        for q_grad, k_part, v_part, (rows, keys, lanes) in zip(q_grads, k_parts, v_parts, jobs):
            q_ref[rows, lanes] = rounded(one_pair(q_grad))
            if keys.size == q_ref.shape[0]:
                k_acc[:, lanes] = k_part
                v_acc[:, lanes] = v_part
            else:
                k_acc[keys, lanes] += k_part
                v_acc[keys, lanes] += v_part
    k_ref[...] = rounded(k_acc[...])
    v_ref[...] = rounded(v_acc[...])


KEPT = {'u_one': 1, 'mixed': 1, 'u_two': 1, 'act': 4, 'grad_pre': 4, 'grad_hidden': 1, 'grad_qkv': 3, 'grad': 1}
FACTORS = (('act', 'grad'), ('u_two', 'grad_pre'), ('mixed', 'grad_hidden'), ('u_one', 'grad_qkv'))


def own_place(me):
    core, x_at, y_at, z_at = lax.rem(me, 2), lax.rem(lax.div(me, 2), 2), lax.rem(lax.div(me, 4), 2), lax.div(me, 8)
    half = lax.div(z_at, 2)
    place = {'core': core, 'x': x_at, 'y': y_at, 'z': lax.rem(z_at, 2), 'half': half}
    to = {}
    for name, stride in (('core', 1), ('x', 2), ('y', 4), ('z', 8)):
        to[name] = me + stride * (1 - 2 * place[name])
    inward = 8 * (1 - 2 * half)
    to.update(mid=me + inward, end=me - inward, far=me + 2 * inward)
    return place, to, lax.div(z_at + 1, 2) == 1, lax.div(z_at + 1, 2) != 1


def compute_kernel(n_layers, x_in, grad_in, gain_one, gain_two, w_qkv, w_out, w_up, w_down, *refs):
    refs = list(refs)

    def take(count):
        head, refs[:] = refs[:count], refs[count:]
        return head

    grad_out, gain_out = take(2)
    kept = [dict(zip(KEPT, take(len(KEPT)))) for _ in range(n_layers)]
    units = [(mat, layer) for layer in range(n_layers) for mat in range(len(MATRICES))]
    early = [unit for unit in units if unit not in LATE]
    from_chip = dict(zip(early, zip(take(len(early)), take(len(early)))))
    rows, hidden, qkv, pre = (take(n_layers) for _ in range(4))
    unit_rows, mixed, act, grad_hidden, grad, do_ref, k_acc, v_acc, acc, s_qkv, s_out, s_up, s_down = take(13)
    sem_qkv, sem_out, sem_up, sem_down, sem_in, sem_put, sem_send, sem_recv, sem_out_blocks, sem_in_blocks = refs
    place, to, _, _ = own_place(lax.axis_index(AXIS))
    n_group, n_ff = s_out.shape[0], s_up.shape[0]

    def fetch_group(layer, at):
        cols = [pl.ds(pl.multiple_of((which * n_group + at) * GROUP, GROUP), GROUP) for which in range(3)]
        pieces = [pltpu.make_async_copy(w_qkv.at[layer, :, cols[which]], s_qkv.at[which, at], sem_qkv.at[which, at]) for which in range(3)]
        return pieces + [pltpu.make_async_copy(w_out.at[layer, pl.ds(pl.multiple_of(at * GROUP, GROUP), GROUP), :], s_out.at[at], sem_out.at[at])]

    def fetch_up(layer, at):
        return pltpu.make_async_copy(w_up.at[layer, :, pl.ds(pl.multiple_of(at * FF_BLOCK, FF_BLOCK), FF_BLOCK)], s_up.at[at], sem_up.at[at])

    def fetch_down(layer, at):
        return pltpu.make_async_copy(w_down.at[layer, pl.ds(pl.multiple_of(at * FF_BLOCK, FF_BLOCK), FF_BLOCK), :], s_down.at[at], sem_down.at[at])

    def start_groups(layer):
        for at in range(n_group):
            for piece in fetch_group(layer, at):
                piece.start()

    def start_all(fetch, layer):
        for at in range(n_ff):
            fetch(layer, at).start()

    n_put, sent, waiting, streams = [0], [], [], []

    def put(src, dst):
        copy = pltpu.make_async_copy(src, dst, sem_put.at[n_put[0]])
        n_put[0] += 1
        copy.start()
        return copy

    def put_blocks(src, dst):
        count, _, cols = src.shape
        return [put(src.at[at], dst.at[:, pl.ds(at * cols, cols)]) for at in range(count)]

    def exchange(mat, layer, which):
        if (mat, layer) in LATE or (mat, which) == (1, 1):
            return
        axis, split = first_axis(mat, layer), MATRICES[mat][2]
        name = FACTORS[mat][which]
        src = grad_in.at[0] if (name, layer) == ('grad', n_layers - 1) else kept[layer][name]
        if which == split:
            dst = from_chip[(mat, layer)][0]
            src = src.at[:, pl.ds(pl.multiple_of((1 - place[axis]) * dst.shape[1], 128), dst.shape[1])]
        else:
            dst = from_chip[(mat, layer)][1]
        copy = pltpu.make_async_remote_copy(src_ref=src, dst_ref=dst, send_sem=sem_send.at[len(sent)], recv_sem=sem_recv.at[len(sent)],
                                            device_id=(to[axis],), device_id_type=pl.DeviceIdType.MESH)
        sent.append(copy)
        copy.start()

    def save(name, layer, copies):
        waiting.append((name, layer, copies))

    def flush():
        for name, layer, copies in waiting:
            for copy in copies:
                copy.wait()
            for mat, names in enumerate(FACTORS):
                if name in names:
                    exchange(mat, layer, names.index(name))
        waiting.clear()

    def gain_row(gain, layer):
        return gain.at[pl.ds(layer, 1), :]

    def attention_forward(layer):
        flush()
        norm_forward(rows[layer], gain_row(gain_one, layer), unit_rows)
        if layer == 0:
            for piece in fetch_group(layer, n_group - 1):
                piece.wait()
            start_all(fetch_up, 0)
            start_all(fetch_down, 0)
            second.start()
        save('u_one', layer, [put(unit_rows, kept[layer]['u_one'])])
        acc[...] = jnp.zeros_like(acc)
        q_all, k_all, v_all = (qkv[layer].at[which] for which in range(3))

        @pl.loop(0, n_group)
        def _(at):
            if layer > 0:
                for piece in fetch_group(layer, at):
                    piece.wait()
            else:
                @pl.when(at < n_group - 1)
                def _():
                    for piece in fetch_group(layer, at):
                        piece.wait()
            for which in range(3):
                qkv[layer][which, at] = rounded(dot_nn(unit_rows[...], s_qkv[which, at]))
            attend(q_all.at[at], k_all.at[at], v_all.at[at], mixed.at[at])
            acc[...] += dot_nn(mixed[at], s_out[at])
        save('mixed', layer, put_blocks(mixed, kept[layer]['mixed']))
        hidden[layer][...] = rows[layer][...] + rounded(acc[...])

    def bent(rows_f):
        return jnp.tanh(GELU_C * (rows_f + GELU_D * (rows_f * rows_f * rows_f)))

    def gelu(rows_f, bend):
        return rounded(rows_f * (0.5 * (1.0 + bend)))

    def gelu_slope(rows_f, bend):
        return 0.5 * (1.0 + bend) + (0.5 * GELU_C) * rows_f * (1.0 - bend * bend) * (1.0 + (3.0 * GELU_D) * (rows_f * rows_f))

    def mlp_norm(layer):
        flush()
        norm_forward(hidden[layer], gain_row(gain_two, layer), unit_rows)
        save('u_two', layer, [put(unit_rows, kept[layer]['u_two'])])
        acc[...] = jnp.zeros_like(acc)

    def mlp_forward(layer):
        mlp_norm(layer)

        @pl.loop(0, n_ff)
        def _(at):
            fetch_up(layer, at).wait()
            fetch_down(layer, at).wait()
            pre[layer][at] = rounded(dot_nn(unit_rows[...], s_up[at]))
            rows_f = wide_float(pre[layer][at])
            act[at] = gelu(rows_f, bent(rows_f))
            acc[...] += dot_nn(act[at], s_down[at])
        save('act', layer, put_blocks(act, kept[layer]['act']))
        rows[layer + 1][...] = hidden[layer][...] + rounded(acc[...])

    def mlp_backward(layer, top):
        if top:
            mlp_norm(layer)
        acc[...] = jnp.zeros_like(acc)
        axis = first_axis(1, layer)

        def stream(step, at):
            return pltpu.make_async_remote_copy(
                src_ref=pre[layer].at[at], dst_ref=from_chip[(1, layer)][0].at[:, pl.ds(pl.multiple_of(step * FF_BLOCK, FF_BLOCK), FF_BLOCK)],
                send_sem=sem_out_blocks.at[layer, step], recv_sem=sem_in_blocks.at[layer, step], device_id=(to[axis],), device_id_type=pl.DeviceIdType.MESH)

        @pl.loop(0, n_ff)
        def _(step):
            at = lax.rem(step + (1 - place[axis]) * (n_ff // 2), n_ff)
            fetch_down(layer, at).wait()
            fetch_up(layer, at).wait()
            rows_f = wide_float(rounded(dot_nn(unit_rows[...], s_up[at])) if top else pre[layer][at])
            bend = bent(rows_f)
            if top:
                act[at] = gelu(rows_f, bend)
            grad_a = wide_float(rounded(dot_nt(grad[...], s_down[at])))
            pre[layer][at] = rounded(gelu_slope(rows_f, bend) * grad_a)
            acc[...] += dot_nt(pre[layer][at], s_up[at])
            if (1, layer) not in LATE:
                pl.when(step < n_ff // 2)(lambda: stream(step, at).start())
        if (1, layer) not in LATE:
            streams.extend(functools.partial(stream, step, step) for step in range(n_ff // 2))
        flush()
        if top:
            save('act', layer, put_blocks(act, kept[layer]['act']))
        save('grad_pre', layer, put_blocks(pre[layer], kept[layer]['grad_pre']))
        norm_backward(hidden[layer], gain_row(gain_two, layer), acc, grad, grad_hidden, gain_row(gain_out, n_layers + layer))
        save('grad_hidden', layer, [put(grad_hidden, kept[layer]['grad_hidden'])])

    def attention_backward(layer, fetched):
        acc[...] = jnp.zeros_like(acc)

        @pl.loop(0, n_group)
        def _(at):
            if not fetched:
                for piece in fetch_group(layer, at):
                    piece.wait()
            do_ref[...] = rounded(dot_nt(grad_hidden[...], s_out[at]))
            attend_backward(do_ref, *(qkv[layer].at[which, at] for which in range(3)), k_acc, v_acc)
            for which in range(3):
                acc[...] += dot_nt(qkv[layer][which, at], s_qkv[which, at])
        flush()
        copies = []
        for which in range(3):
            width = grad.shape[1]
            copies += [put(qkv[layer].at[which, at], kept[layer]['grad_qkv'].at[:, pl.ds(which * width + at * GROUP, GROUP)]) for at in range(n_group)]
        save('grad_qkv', layer, copies)
        norm_backward(rows[layer], gain_row(gain_one, layer), acc, grad_hidden, grad, gain_row(gain_out, layer))

    first = pltpu.make_async_copy(x_in.at[0], rows[0], sem_in.at[0])
    second = pltpu.make_async_copy(grad_in.at[0], grad, sem_in.at[1])
    first.start()
    start_groups(0)
    exchange(0, n_layers - 1, 1)
    gain_out[...] = jnp.zeros_like(gain_out)
    first.wait()
    for layer in range(n_layers):
        attention_forward(layer)
        if layer + 1 < n_layers:
            start_groups(layer + 1)
            mlp_forward(layer)
            start_all(fetch_up, layer + 1)
            start_all(fetch_down, layer + 1)
    second.wait()
    for layer in reversed(range(n_layers)):
        top = layer + 1 == n_layers
        mlp_backward(layer, top)
        if layer > 0:
            start_all(fetch_up, layer - 1)
            start_all(fetch_down, layer - 1)
        flush()
        attention_backward(layer, top)
        if layer > 0:
            start_groups(layer - 1)
            save('grad', layer - 1, [put(grad, kept[layer - 1]['grad'])])
            flush()
    done = put(grad, grad_out)
    flush()
    done.wait()
    for copy in sent + [make() for make in streams]:
        copy.wait()


def compute(x_loc, grad_loc, gain_one, gain_two, w_qkv, w_out, w_up, w_down):
    n_layers, width, inner = w_up.shape
    seq_len = x_loc.shape[1]
    f32, bf16 = jnp.float32, jnp.bfloat16
    n_group, n_ff = width // GROUP, inner // FF_BLOCK
    units = [(mat, layer) for layer in range(n_layers) for mat in range(len(MATRICES))]
    early = [unit for unit in units if unit not in LATE]

    def lo(*shape):
        return jax.ShapeDtypeStruct(shape, bf16)
    outs = [lo(seq_len, width), jax.ShapeDtypeStruct((8, width), f32)]
    outs += [lo(seq_len, cols * width) for _ in range(n_layers) for cols in KEPT.values()]
    shapes = [[KEPT[name] * width for name in FACTORS[mat]] for mat, _ in early]
    outs += [lo(seq_len, shape[MATRICES[mat][2]] // 2) for shape, (mat, _) in zip(shapes, early)]
    outs += [lo(seq_len, shape[1 - MATRICES[mat][2]]) for shape, (mat, _) in zip(shapes, early)]
    wide_rows, groups = (seq_len, width), (n_group, seq_len, GROUP)
    vmem = [wide_rows] * (2 * n_layers) + [(3,) + groups] * n_layers + [(n_ff, seq_len, FF_BLOCK)] * n_layers
    vmem += [wide_rows, groups, (n_ff, seq_len, FF_BLOCK), wide_rows, wide_rows, (seq_len, GROUP)]
    scratch = [pltpu.VMEM(shape, bf16) for shape in vmem] + [pltpu.VMEM(shape, f32) for shape in ((seq_len, GROUP), (seq_len, GROUP), wide_rows)]
    scratch += [pltpu.VMEM(shape, bf16) for shape in ((3, n_group, width, GROUP), (n_group, GROUP, width), (n_ff, width, FF_BLOCK), (n_ff, FF_BLOCK, width))]
    scratch += [pltpu.SemaphoreType.DMA(shape) for shape in ((3, n_group), (n_group,), (n_ff,), (n_ff,), (2,), (100,), (2 * len(early),), (2 * len(early),)) + ((n_layers, n_ff // 2),) * 2]
    hbm, near = pl.BlockSpec(memory_space=pl.ANY), pl.BlockSpec(memory_space=pltpu.VMEM)
    results = pl.pallas_call(
        functools.partial(compute_kernel, n_layers), out_shape=tuple(outs), in_specs=[hbm, hbm, near, near] + [hbm] * 4,
        out_specs=tuple([hbm, near] + [hbm] * (len(outs) - 2)), scratch_shapes=scratch,
        compiler_params=pltpu.CompilerParams(has_side_effects=True, vmem_limit_bytes=VMEM_LIMIT),
    )(x_loc, grad_loc, gain_one, gain_two, w_qkv, w_out, w_up, w_down)
    grad_x, gains = results[:2]
    kept = [dict(zip(KEPT, results[2 + layer * len(KEPT):])) for layer in range(n_layers)]
    kept[-1]['grad'] = grad_loc[0]
    tail = results[2 + n_layers * len(KEPT):]
    from_chip = dict(zip(early, zip(tail, tail[len(early):])))
    operands = []
    for mat, layer in units:
        pair = [kept[layer][name] for name in FACTORS[mat]]
        split = MATRICES[mat][2]
        operands.append((pair[split], pair[1 - split]) + from_chip.get((mat, layer), ()))
    return grad_x, gains, operands


def add_rows(dst, src, cols, scale=None):
    rows = dst.shape[0]

    @pl.loop(0, rows // ADD_ROWS)
    def _(step):
        at = pl.ds(pl.multiple_of(step * ADD_ROWS, ADD_ROWS), ADD_ROWS)
        val = dst[at, cols] + src[at, :]
        dst[at, cols] = val if scale is None else val * scale


def flip(bit, by):
    return 1 - bit if by else bit


def combine_kernel(n_dev, n_layers, *refs):
    units = [(mat, layer) for layer in range(n_layers) for mat in range(len(MATRICES))]
    n_chunk = len(CHUNKS)
    refs = list(refs)

    def take(count):
        head, refs[:] = refs[:count], refs[count:]
        return head

    given = [take(2 if unit in LATE else 4) for unit in units]
    gain_in, = take(1)
    outs, (gain_out,) = take(len(MATRICES)), take(1)
    from_core, part_refs, from_chip = take(2 * len(units)), take(len(units)), take(2 * len(LATE))
    land_q, land_z, land_h = (take(n_chunk) for _ in range(3))
    row_op, col_op, product, stream, gain_buf, gain_land, send_sems, recv_sems, local_sems, stream_sems, gain_send, gain_recv, op_send, op_recv, op_local = refs

    me = lax.axis_index(AXIS)
    place, to, middle, edge = own_place(me)
    core, half = place['core'], place['half']

    def remote(src, dst, i, sem, dev):
        return pltpu.make_async_remote_copy(src_ref=src, dst_ref=dst, send_sem=send_sems.at[i, sem], recv_sem=recv_sems.at[i, sem],
                                            device_id=(dev,), device_id_type=pl.DeviceIdType.MESH)

    def out_block(i, p_at, c_at, row, n_rows, h_at):
        mat, layer, k = CHUNKS[i]
        rows_all, cols, split = MATRICES[mat]
        quarter = p_at * 2 + c_at
        row = row + k * (rows_all // chunk_count(mat, layer)) + (quarter * rows_all if split == 0 else 0)
        col, n_cols = (0, cols) if h_at is None else (h_at * (cols // 2), cols // 2)
        if split == 1:
            col = col + quarter * cols
        return outs[mat].at[layer, pl.ds(pl.multiple_of(row, 8), n_rows), pl.ds(col if isinstance(col, int) else pl.multiple_of(col, 128), n_cols)]

    def stream_add(dst, src):
        rows, cols = dst.shape
        size = min(STREAM_ROWS, rows)
        steps = rows // size

        def fetch(step, slot):
            return pltpu.make_async_copy(src.at[pl.ds(pl.multiple_of(step * size, size), size), :], stream.at[slot, pl.ds(0, size), pl.ds(0, cols)], stream_sems.at[slot])
        fetch(0, 0).start()

        @pl.loop(0, steps)
        def _(step):
            slot = lax.rem(step, 2)

            @pl.when(step + 1 < steps)
            def _():
                fetch(step + 1, 1 - slot).start()
            fetch(step, slot).wait()
            at = pl.ds(pl.multiple_of(step * size, size), size)
            dst[at, :] = dst[at, :] + stream[slot, pl.ds(0, size), pl.ds(0, cols)]

    def run(i, stage, pending):
        mat, layer, k = CHUNKS[i]
        rows_all, cols, _ = MATRICES[mat]
        kind, p_name = KIND[layer][mat], first_axis(mat, layer)
        by_pairs = p_name == 'z'
        q_name = kind.lower() if by_pairs else 'xy'.replace(kind, '')
        r_name = 'xy'.replace(q_name, '')
        rows = rows_all // chunk_count(mat, layer)
        part = part_refs[layer * len(MATRICES) + mat]
        p_at, q_at, r_at = place[p_name], place[q_name], place[r_name]

        def go(src, dst, sem, dest, cond=None):
            remote(src(), dst(), i, sem, to[dest]).start()
            pending.append((cond, src, i, sem))

        def block(dp=0, dq=0, dc=0, dr=None, dh=None):
            def ref():
                row, count = flip(q_at, dq) * (rows // 2), rows // 2
                if dr is not None:
                    row, count = row + flip(r_at, dr) * (rows // 4), rows // 4
                return out_block(i, flip(p_at, dp), flip(core, dc), row, count, None if dh is None else flip(half, dh))
            return ref

        def pass_on(blk, sems, cond=None):
            for dest, sem in sems:
                go(blk, blk, sem, dest, cond)

        def arrived(blk, sem):
            remote(blk(), blk(), i, sem, me).wait_recv()

        def half_cols(by):
            return pl.ds(pl.multiple_of(flip(half, by) * (cols // 2), 128), cols // 2)

        def own_rows(by):
            return land_q[i].at[pl.ds(pl.multiple_of(flip(r_at, by) * (rows // 4), 8), rows // 4), :] if by_pairs else land_q[i]

        def own_half(by):
            return lambda: (land_q[i].at[pl.ds(pl.multiple_of(r_at * (rows // 4), 8), rows // 4), half_cols(by)] if by_pairs
                            else land_q[i].at[:, half_cols(by)])

        def rows_of(by):
            return lambda: part.at[pl.ds(pl.multiple_of(k * rows + flip(q_at, by) * (rows // 2), 8), rows // 2), :]

        last = dict(dr=0) if by_pairs else {}

        def keep():
            return pltpu.make_async_copy(own_half(0)(), block(dh=0, **last)(), local_sems.at[i])

        def whole(buf):
            return lambda: buf[i]

        def scale_and_send(dest):
            add_rows(own_rows(0), land_h[i], half_cols(0), 1.0 / n_dev)
            keep().start()
            go(own_half(0), block(dh=0, **last), 3, dest, None if by_pairs else middle)

        def spread(turn):
            if turn == 0:
                pass_on(block(), ((q_name, 5), (p_name, 6), ('core', 8)))
            elif turn == 1:
                arrived(block(dq=1), 5)
                pass_on(block(dq=1), ((p_name, 7), ('core', 9)))
            else:
                dq = turn - 2
                arrived(block(dp=1, dq=dq), turn + 4)
                pass_on(block(dp=1, dq=dq), (('core', turn + 8),))

        if stage == 0:
            go(rows_of(1), whole(land_q), 0, q_name)
        elif stage == 8:
            for turn in range(4):
                arrived(block(dp=turn // 2, dq=turn % 2, dc=1), 8 + turn)
        elif by_pairs:
            if stage == 1:
                arrived(whole(land_q), 0)
                stream_add(land_q[i], rows_of(0)())
                go(lambda: own_rows(1), whole(land_z), 1, r_name)
            elif stage == 2:
                arrived(whole(land_z), 1)
                add_rows(own_rows(0), land_z[i], slice(None))
                go(own_half(1), whole(land_h), 2, 'far')
            elif stage == 3:
                arrived(whole(land_h), 2)
                scale_and_send('far')
            elif stage == 4:
                keep().wait()
                arrived(block(dr=0, dh=1), 3)
                go(block(dr=0), block(dr=0), 4, r_name)
            else:
                if stage == 5:
                    arrived(block(dr=1), 4)
                spread(min(stage - 5, 3))
        elif stage == 1:
            arrived(whole(land_q), 0)
            stream_add(land_q[i], rows_of(0)())

            @pl.when(edge)
            def _():
                go(whole(land_q), whole(land_z), 1, 'mid', edge)
        elif stage in (2, 3):
            @pl.when(middle)
            def _():
                arrived(whole((land_z, land_h)[stage - 2]), stage - 1)
                if stage == 2:
                    add_rows(land_q[i], land_z[i], slice(None))
                    go(own_half(1), whole(land_h), 2, 'mid', middle)
                else:
                    scale_and_send('mid')
        else:
            if stage == 4:
                @pl.when(middle)
                def _():
                    keep().wait()
                    arrived(block(dh=1), 3)
                    pass_on(block(), (('end', 4),), middle)

                @pl.when(edge)
                def _():
                    arrived(block(), 4)
            spread(stage - 4)

    def unit_sizes(unit):
        rows, cols, split = MATRICES[unit[0]]
        p_name = first_axis(*unit)
        return (rows, cols, p_name, split) + ((rows, cols) if split == 0 else (cols, rows))

    def operand_copy(u, which, src, dst, dest):
        return pltpu.make_async_remote_copy(src_ref=src, dst_ref=dst, send_sem=op_send.at[u, which], recv_sem=op_recv.at[u, which],
                                            device_id=(to[dest],), device_id_type=pl.DeviceIdType.MESH)

    def operand_copies(u):
        unit = units[u]
        rows, cols, p_name, split, wide_w, _ = unit_sizes(unit)
        p_at = place[p_name]
        wide, thin = given[u][:2]
        core_wide, core_thin = from_core[2 * u:2 * u + 2]
        if unit in LATE:
            late = LATE.index(unit)
            chip_wide, chip_thin = from_chip[2 * late:2 * late + 2]
        else:
            chip_wide, chip_thin = given[u][2:]
        first, second = pl.ds(0, SEQ_LEN), pl.ds(SEQ_LEN, SEQ_LEN)

        def lanes(at, count):
            return pl.ds(pl.multiple_of(at, 128), count)
        other = 1 - core
        copies = {
            'own': (operand_copy(u, 0, wide.at[:, lanes((p_at * 2 + other) * wide_w, wide_w)], core_wide.at[first, :], 'core'),
                    operand_copy(u, 1, thin, core_thin.at[first, :], 'core')),
            'next': (operand_copy(u, 2, chip_wide.at[:, lanes(other * wide_w, wide_w)], core_wide.at[second, :], 'core'),
                     operand_copy(u, 3, chip_thin, core_thin.at[second, :], 'core')),
        }
        if unit in LATE:
            copies['chip'] = (operand_copy(u, 4, wide.at[:, lanes((1 - p_at) * 2 * wide_w, 2 * wide_w)], chip_wide, p_name),
                              operand_copy(u, 5, thin, chip_thin, p_name))
        wide_op, thin_op = (row_op, col_op) if split == 0 else (col_op, row_op)
        thin_w = thin.shape[1]
        loads = []
        for start, src in ((0, wide.at[:, lanes((p_at * 2 + core) * wide_w, wide_w)]), (SEQ_LEN, chip_wide.at[:, lanes(core * wide_w, wide_w)]),
                           (2 * SEQ_LEN, core_wide)):
            loads.append((src, wide_op.at[pl.ds(start, src.shape[0]), pl.ds(0, wide_w)]))
        for start, src in ((0, thin), (SEQ_LEN, chip_thin), (2 * SEQ_LEN, core_thin)):
            loads.append((src, thin_op.at[pl.ds(start, src.shape[0]), pl.ds(0, thin_w)]))
        copies['load'] = tuple(pltpu.make_async_copy(src, dst, op_local.at[u, n]) for n, (src, dst) in enumerate(loads))
        return copies

    def start_operands(u):
        copies = operand_copies(u)
        if units[u] in LATE:
            for copy in copies['chip']:
                copy.start()
        for copy in copies['own']:
            copy.start()
        if units[u] not in LATE:
            for copy in copies['next']:
                copy.start()

    def forward_operands(u):
        copies = operand_copies(u)
        for copy in copies['chip']:
            copy.wait_recv()
        for copy in copies['next']:
            copy.start()

    def multiply(u):
        rows, cols, _, _, _, _ = unit_sizes(units[u])
        copies = operand_copies(u)
        for copy in copies['own'] + copies['next']:
            copy.wait_recv()
        for copy in copies['load']:
            copy.start()
        for copy in copies['load']:
            copy.wait()
        tile = min(TILE_ROWS, rows)
        half_w = cols // 2

        @pl.loop(0, rows // tile)
        def _(step):
            at = pl.ds(pl.multiple_of(step * tile, tile), tile)
            for side in range(2):
                lanes = pl.ds(side * half_w, half_w)
                product[at, lanes] = dot_tn(row_op[:, at], col_op[:, lanes])
        store = pltpu.make_async_copy(product.at[pl.ds(0, rows), pl.ds(0, cols)], part_refs[u], op_local.at[u, 6])
        store.start()
        store.wait()

    def finish_operands(u):
        copies = operand_copies(u)
        for copy in copies['own'] + copies['next'] + copies.get('chip', ()):
            copy.wait_send()

    gain_steps = ('core', 'x', 'y', 'z', 'far')

    def gain_copy(step):
        return pltpu.make_async_remote_copy(src_ref=gain_buf.at[step], dst_ref=gain_land.at[step], send_sem=gain_send.at[step],
                                            recv_sem=gain_recv.at[step], device_id=(to[gain_steps[step]],), device_id_type=pl.DeviceIdType.MESH)

    def gain_next(step):
        copy = gain_copy(step)
        copy.wait()
        total = gain_buf[step] + gain_land[step]
        if step + 1 < len(gain_steps):
            gain_buf[step + 1] = total
            gain_copy(step + 1).start()
        else:
            gain_out[...] = total * (1.0 / n_dev)

    pending = []
    gain_buf[0] = gain_in[...]
    step = 0
    first_use = []
    for mat, layer, _ in CHUNKS:
        if units.index((mat, layer)) not in first_use:
            first_use.append(units.index((mat, layer)))
    for u in first_use:
        start_operands(u)
    for count, (letter, digit) in enumerate(zip(*[iter(''.join(ORDER))] * 2)):
        i, stage = ord(letter) - ord('a'), int(digit, 16)
        u = units.index(CHUNKS[i][:2])
        if stage == 9:
            multiply(u)
        elif stage == 10:
            forward_operands(u)
        else:
            run(i, stage, pending)
        if count == 1:
            gain_copy(0).start()
        if count >= 8 and count % 6 == 0 and step < len(gain_steps):
            gain_next(step)
            step += 1
    for u in range(len(units)):
        finish_operands(u)
    for cond, src, i, sem in pending:
        def finish(src=src, i=i, sem=sem):
            remote(src(), src(), i, sem, me).wait_send()
        if cond is None:
            finish()
        else:
            pl.when(cond)(finish)


def combine(operands, gains, n_dev, n_layers):
    f32, bf16 = jnp.float32, jnp.bfloat16
    units = [(mat, layer) for layer in range(n_layers) for mat in range(len(MATRICES))]
    outs = []
    for rows, cols, split in MATRICES:
        outs.append(jax.ShapeDtypeStruct((n_layers, rows * (4 if split == 0 else 1), cols * (4 if split == 1 else 1)), f32))
    outs.append(jax.ShapeDtypeStruct(gains.shape, f32))
    widths = [MATRICES[mat][:2] if MATRICES[mat][2] == 0 else MATRICES[mat][1::-1] for mat, _ in units]
    for wide_w, thin_w in widths:
        outs += [jax.ShapeDtypeStruct((2 * SEQ_LEN, wide_w), bf16), jax.ShapeDtypeStruct((2 * SEQ_LEN, thin_w), bf16)]
    outs += [jax.ShapeDtypeStruct(MATRICES[mat][:2], f32) for mat, _ in units]
    for unit in LATE:
        wide_w, thin_w = widths[units.index(unit)]
        outs += [jax.ShapeDtypeStruct((SEQ_LEN, 2 * wide_w), bf16), jax.ShapeDtypeStruct((SEQ_LEN, thin_w), bf16)]
    sizes = [(MATRICES[mat][0] // chunk_count(mat, layer) // 2, MATRICES[mat][1], first_axis(mat, layer) == 'z') for mat, layer, _ in CHUNKS]
    scratch = [pltpu.VMEM((r, c), f32) for r, c, _ in sizes]
    scratch += [pltpu.VMEM((r // 2 if pairs else r, c), f32) for r, c, pairs in sizes]
    scratch += [pltpu.VMEM((r // 2 if pairs else r, c // 2), f32) for r, c, pairs in sizes]
    n_chunk, n_unit = len(CHUNKS), len(units)
    most_rows, most_cols = max(m[0] for m in MATRICES), max(m[1] for m in MATRICES)
    scratch += [pltpu.VMEM((TOKENS, most_rows), bf16), pltpu.VMEM((TOKENS, most_cols), bf16), pltpu.VMEM((most_rows, most_cols), f32),
                pltpu.VMEM((2, STREAM_ROWS, most_cols), f32),
                pltpu.VMEM((5,) + gains.shape, f32), pltpu.VMEM((5,) + gains.shape, f32),
                pltpu.SemaphoreType.DMA((n_chunk, N_SEMS)), pltpu.SemaphoreType.DMA((n_chunk, N_SEMS)), pltpu.SemaphoreType.DMA((n_chunk,)), pltpu.SemaphoreType.DMA((2,)),
                pltpu.SemaphoreType.DMA((5,)), pltpu.SemaphoreType.DMA((5,)),
                pltpu.SemaphoreType.DMA((n_unit, 6)), pltpu.SemaphoreType.DMA((n_unit, 6)), pltpu.SemaphoreType.DMA((n_unit, 7))]
    hbm, vmem = pl.BlockSpec(memory_space=pl.ANY), pl.BlockSpec(memory_space=pltpu.VMEM)
    flat = [val for group in operands for val in group]
    results = pl.pallas_call(
        functools.partial(combine_kernel, n_dev, n_layers),
        out_shape=tuple(outs),
        in_specs=[hbm] * len(flat) + [vmem],
        out_specs=tuple([hbm] * 4 + [vmem] + [hbm] * (len(outs) - 5)),
        scratch_shapes=scratch,
        compiler_params=pltpu.CompilerParams(has_side_effects=True, vmem_limit_bytes=VMEM_LIMIT),
    )(*flat, gains)
    return results[:5]


def solution(mesh):
    n_dev = mesh.shape[AXIS]

    def local_step(x_loc, grad_y_loc, gain_one, gain_two, w_qkv, w_out, w_up, w_down):
        n_layers = w_qkv.shape[0]
        grad_x, gains, operands = compute(x_loc, grad_y_loc, gain_one, gain_two, w_qkv, w_out, w_up, w_down)
        down, up, out, qkv, gains = combine(operands, gains, n_dev, n_layers)
        return (grad_x[None], gains[:n_layers], gains[n_layers:2 * n_layers], qkv, out, up, down)

    batch_spec = P(AXIS)
    full_spec = P()
    return jax.shard_map(local_step, mesh=mesh, in_specs=(batch_spec, batch_spec) + (full_spec,) * 6, out_specs=(batch_spec,) + (full_spec,) * 6, check_vma=False)
```

```python
import functools

import jax
import jax.numpy as jnp
from jax import lax
from jax.experimental import pallas as pl
from jax.experimental.pallas import tpu as pltpu
from jax.sharding import PartitionSpec as P

NORM_EPS = 1e-6
HEAD_DIM = 64
AXIS = 'data'
CHUNK_UNITS = '1111110000100110012131303120113000003030'
ORDER = (
    'a9d9a0b0c0d0naa1f9e0lab1g9f0a2d1g0c1h0b2a3e1j9i0b3d2f1a4k9d3',
    'c2g1j0b4l9k0e2c3h1l0d4e3i1n9a5m0f2c4a6e4f3b5b6j1g2k1d6n0d5l1',
    'o0g3f4a7p0h2a8c6c5h3m1g4i2q0l2e5e6b7b8k2h4j2i3l3d7d8n1k3f6o1',
    'j3p1r0f5s0i4o2j4t0p2l4k4o3m2p3c7c8q1g5g6m3o4e7m4e8q2p4q3h5h6',
    'n2q4n3n4s1f7i6f8t1r1l5k5s2j5i5s3r2s4t2l6k7r3g7j7t3g8o6o5p5p6',
    'm5r4t4n5h7q6h8m7n7q5k6i7l7i8l8s5s6keo7j6o8k8r6p7m6r5jet5p8t6',
    'n6meq7m8q8j8r7s7r8nes8t7n8t8',
)
VMEM_LIMIT = 63 * 1024 * 1024


MATRICES = ((1024, 1024, 0), (1024, 1024, 1), (256, 1024, 0), (1024, 768, 1))
KIND = ('xyYy', 'xyYX')
LATE = ((2, 0), (3, 0))
SEQ_LEN = 384
TOKENS = 4 * SEQ_LEN
TILE_ROWS = 256
STREAM_ROWS = 64
N_SEMS = 12
ADD_ROWS = 32


def read_chunks(text):
    found = []
    for mat, layer in zip(*[map(int, text)] * 2):
        found.append((mat, layer, sum(chunk[:2] == (mat, layer) for chunk in found)))
    return tuple(found)


CHUNKS = read_chunks(CHUNK_UNITS)


def first_axis(mat, layer):
    kind = KIND[layer][mat]
    return kind if kind in 'xy' else 'z'


def chunk_count(mat, layer):
    return sum(chunk[:2] == (mat, layer) for chunk in CHUNKS)


PAIR = 2 * HEAD_DIM
GROUP = 2 * PAIR
Q_BLOCK = 128
FF_BLOCK = 512
NORM_ROWS = 128
FORWARD_STEPS = ((0, 1, 2),)
BACKWARD_STEPS = ((2, 1, 0),)
GELU_C = 0.7978845608028654
GELU_D = 0.044715


def dot_with(dims):
    return lambda lhs, rhs: lax.dot_general(lhs, rhs, (dims, ((), ())), preferred_element_type=jnp.float32)


dot_nn, dot_nt, dot_tn = (dot_with(((left,), (right,))) for left, right in ((1, 0), (1, 1), (0, 0)))


def rounded(val):
    return val.astype(jnp.bfloat16)


def wide_float(val):
    return val.astype(jnp.float32)


def row_blocks(count):
    def wrap(body):
        @pl.loop(0, count // NORM_ROWS)
        def _(step):
            body(pl.ds(pl.multiple_of(step * NORM_ROWS, NORM_ROWS), NORM_ROWS))
    return wrap


def inverse_rms(rows_f):
    return lax.rsqrt(jnp.mean(rows_f * rows_f, axis=-1, keepdims=True) + NORM_EPS)


def norm_forward(src, gain, dst):
    @row_blocks(src.shape[0])
    def _(at):
        rows_f = wide_float(src[at, :])
        dst[at, :] = rounded(rows_f * inverse_rms(rows_f) * gain[...])


def norm_backward(src, gain, grad_norm, grad_res, dst, gain_dst):
    gain_dst[...] = jnp.zeros_like(gain_dst)

    @row_blocks(src.shape[0])
    def _(at):
        rows_f = wide_float(src[at, :])
        scale = inverse_rms(rows_f)
        unit = rows_f * scale
        grad = wide_float(rounded(grad_norm[at, :]))
        gain_dst[...] += jnp.sum(grad * unit, axis=0, keepdims=True)
        grad = grad * gain[...]
        grad = scale * (grad - unit * jnp.mean(grad * unit, axis=-1, keepdims=True))
        dst[at, :] = rounded(wide_float(grad_res[at, :]) + grad)


def two_heads(rows):
    first = lax.broadcasted_iota(jnp.int32, rows.shape, 1) < HEAD_DIM
    zero = jnp.zeros_like(rows)
    return jnp.concatenate([jnp.where(first, rows, zero), jnp.where(first, zero, rows)], axis=0)


def one_pair(rows):
    half = rows.shape[0] // 2
    first = lax.broadcasted_iota(jnp.int32, (half, PAIR), 1) < HEAD_DIM
    return jnp.where(first, rows[:half], rows[half:])


def in_step(step, *lists):
    return [step(*args) for args in zip(*lists)]


def softmax_blocks(q_twos, k_all):
    scores = in_step(lambda q_two, k_rows: dot_nt(q_two, k_rows) * HEAD_DIM ** -0.5, q_twos, k_all)
    shape = (2 * Q_BLOCK, Q_BLOCK)
    seen = lax.rem(lax.broadcasted_iota(jnp.int32, shape, 0), Q_BLOCK) >= lax.broadcasted_iota(jnp.int32, shape, 1)

    def masked(score):
        before = score.shape[1] - Q_BLOCK
        last = jnp.where(seen, score[:, before:], -1e30)
        return jnp.concatenate([score[:, :before], last], axis=1) if before else last
    scores = in_step(masked, scores)
    peaks = in_step(lambda score: jnp.max(score, axis=-1, keepdims=True), scores)
    weights = in_step(lambda score, peak: jnp.exp(score - peak), scores, peaks)
    totals = in_step(lambda weight: 1.0 / jnp.sum(weight, axis=-1, keepdims=True), weights)
    return in_step(lambda weight, total: weight * total, weights, totals)


def jobs_of(blocks):
    return [(pl.ds(block * Q_BLOCK, Q_BLOCK), pl.ds(0, (block + 1) * Q_BLOCK), pl.ds(pair * PAIR, PAIR)) for block in blocks for pair in range(GROUP // PAIR)]


def attend(q_ref, k_ref, v_ref, o_ref):
    for blocks in FORWARD_STEPS:
        jobs = jobs_of(blocks)
        probs = softmax_blocks([two_heads(q_ref[rows, lanes]) for rows, _, lanes in jobs], [k_ref[keys, lanes] for _, keys, lanes in jobs])
        results = in_step(lambda prob, job: dot_nn(rounded(prob), v_ref[job[1], job[2]]), probs, jobs)
        for result, (rows, _, lanes) in zip(results, jobs):
            o_ref[rows, lanes] = rounded(one_pair(result))


def attend_backward(do_ref, q_ref, k_ref, v_ref, k_acc, v_acc):
    for blocks in BACKWARD_STEPS:
        jobs = jobs_of(blocks)
        q_twos, g_twos = ([two_heads(ref[rows, lanes]) for rows, _, lanes in jobs] for ref in (q_ref, do_ref))
        k_rows = [k_ref[keys, lanes] for _, keys, lanes in jobs]
        grad_probs = in_step(lambda g_two, job: dot_nt(g_two, v_ref[job[1], job[2]]), g_twos, jobs)
        probs = softmax_blocks(q_twos, k_rows)
        means = in_step(lambda prob, grad_prob: jnp.sum(prob * grad_prob, axis=-1, keepdims=True), probs, grad_probs)
        grad_s = in_step(lambda prob, grad_prob, mean: rounded(prob * (grad_prob - mean) * HEAD_DIM ** -0.5), probs, grad_probs, means)
        q_grads = in_step(dot_nn, grad_s, k_rows)
        k_parts = in_step(dot_tn, grad_s, q_twos)
        v_parts = in_step(lambda prob, g_two: dot_tn(rounded(prob), g_two), probs, g_twos)
        for q_grad, k_part, v_part, (rows, keys, lanes) in zip(q_grads, k_parts, v_parts, jobs):
            q_ref[rows, lanes] = rounded(one_pair(q_grad))
            if keys.size == q_ref.shape[0]:
                k_acc[:, lanes] = k_part
                v_acc[:, lanes] = v_part
            else:
                k_acc[keys, lanes] += k_part
                v_acc[keys, lanes] += v_part
    k_ref[...] = rounded(k_acc[...])
    v_ref[...] = rounded(v_acc[...])


KEPT = {'u_one': 1, 'mixed': 1, 'u_two': 1, 'act': 4, 'grad_pre': 4, 'grad_hidden': 1, 'grad_qkv': 3, 'grad': 1}
FACTORS = (('act', 'grad'), ('u_two', 'grad_pre'), ('mixed', 'grad_hidden'), ('u_one', 'grad_qkv'))


def own_place(me):
    core, x_at, y_at, z_at = lax.rem(me, 2), lax.rem(lax.div(me, 2), 2), lax.rem(lax.div(me, 4), 2), lax.div(me, 8)
    half = lax.div(z_at, 2)
    place = {'core': core, 'x': x_at, 'y': y_at, 'z': lax.rem(z_at, 2), 'half': half}
    to = {}
    for name, stride in (('core', 1), ('x', 2), ('y', 4), ('z', 8)):
        to[name] = me + stride * (1 - 2 * place[name])
    inward = 8 * (1 - 2 * half)
    to.update(mid=me + inward, end=me - inward, far=me + 2 * inward)
    return place, to, lax.div(z_at + 1, 2) == 1, lax.div(z_at + 1, 2) != 1


def compute_kernel(n_layers, x_in, grad_in, gain_one, gain_two, w_qkv, w_out, w_up, w_down, *refs):
    refs = list(refs)

    def take(count):
        head, refs[:] = refs[:count], refs[count:]
        return head

    grad_out, gain_out = take(2)
    kept = [dict(zip(KEPT, take(len(KEPT)))) for _ in range(n_layers)]
    units = [(mat, layer) for layer in range(n_layers) for mat in range(len(MATRICES))]
    early = [unit for unit in units if unit not in LATE]
    from_chip = dict(zip(early, zip(take(len(early)), take(len(early)))))
    rows, hidden, qkv, pre = (take(n_layers) for _ in range(4))
    unit_rows, mixed, act, grad_hidden, grad, do_ref, k_acc, v_acc, acc, s_qkv, s_out, s_up, s_down = take(13)
    sem_qkv, sem_out, sem_up, sem_down, sem_in, sem_put, sem_send, sem_recv, sem_out_blocks, sem_in_blocks = refs
    place, to, _, _ = own_place(lax.axis_index(AXIS))
    n_group, n_ff = s_out.shape[0], s_up.shape[0]

    def fetch_group(layer, at):
        cols = [pl.ds(pl.multiple_of((which * n_group + at) * GROUP, GROUP), GROUP) for which in range(3)]
        pieces = [pltpu.make_async_copy(w_qkv.at[layer, :, cols[which]], s_qkv.at[which, at], sem_qkv.at[which, at]) for which in range(3)]
        return pieces + [pltpu.make_async_copy(w_out.at[layer, pl.ds(pl.multiple_of(at * GROUP, GROUP), GROUP), :], s_out.at[at], sem_out.at[at])]

    def fetch_up(layer, at):
        return pltpu.make_async_copy(w_up.at[layer, :, pl.ds(pl.multiple_of(at * FF_BLOCK, FF_BLOCK), FF_BLOCK)], s_up.at[at], sem_up.at[at])

    def fetch_down(layer, at):
        return pltpu.make_async_copy(w_down.at[layer, pl.ds(pl.multiple_of(at * FF_BLOCK, FF_BLOCK), FF_BLOCK), :], s_down.at[at], sem_down.at[at])

    def start_groups(layer):
        for at in range(n_group):
            for piece in fetch_group(layer, at):
                piece.start()

    def start_all(fetch, layer):
        for at in range(n_ff):
            fetch(layer, at).start()

    n_put, sent, waiting, streams = [0], [], [], []

    def put(src, dst):
        copy = pltpu.make_async_copy(src, dst, sem_put.at[n_put[0]])
        n_put[0] += 1
        copy.start()
        return copy

    def put_blocks(src, dst):
        count, _, cols = src.shape
        return [put(src.at[at], dst.at[:, pl.ds(at * cols, cols)]) for at in range(count)]

    def exchange(mat, layer, which):
        if (mat, layer) in LATE or (mat, which) == (1, 1) or (mat, layer, which) == (0, n_layers - 1, 0):
            return []
        axis, split = first_axis(mat, layer), MATRICES[mat][2]
        name, order = FACTORS[mat][which], len(sent)

        def make():
            src = grad_in.at[0] if (name, layer) == ('grad', n_layers - 1) else kept[layer][name]
            dst = from_chip[(mat, layer)][which != split]
            if which == split:
                src = src.at[:, pl.ds(pl.multiple_of((1 - place[axis]) * dst.shape[1], 128), dst.shape[1])]
            return pltpu.make_async_remote_copy(src_ref=src, dst_ref=dst, send_sem=sem_send.at[order], recv_sem=sem_recv.at[order],
                                                device_id=(to[axis],), device_id_type=pl.DeviceIdType.MESH)
        sent.append(make)
        return [make]

    def save(name, layer, copies):
        waiting.append((name, layer, copies))

    def planned_flush():
        copies = [copy for _, _, group in waiting for copy in group]
        makes = []
        for name, layer, _ in waiting:
            for mat, names in enumerate(FACTORS):
                if name in names:
                    makes += exchange(mat, layer, names.index(name))
        waiting.clear()

        def run():
            for copy in copies:
                copy.wait()
            for make in makes:
                make().start()
        return run

    def gain_row(gain, layer):
        return gain.at[pl.ds(layer, 1), :]

    def attention_forward(layer):
        norm_forward(rows[layer], gain_row(gain_one, layer), unit_rows)
        save('u_one', layer, [put(unit_rows, kept[layer]['u_one'])])
        acc[...] = jnp.zeros_like(acc)
        flush = planned_flush()
        q_all, k_all, v_all = (qkv[layer].at[which] for which in range(3))

        @pl.loop(0, n_group)
        def _(at):
            for piece in fetch_group(layer, at):
                piece.wait()

            @pl.when(at == 1)
            def _():
                flush()
                if layer == 0:
                    start_all(fetch_up, 0)
                    start_all(fetch_down, 0)
                    second.start()
            for which in range(3):
                qkv[layer][which, at] = rounded(dot_nn(unit_rows[...], s_qkv[which, at]))
            attend(q_all.at[at], k_all.at[at], v_all.at[at], mixed.at[at])
            acc[...] += dot_nn(mixed[at], s_out[at])
        save('mixed', layer, put_blocks(mixed, kept[layer]['mixed']))
        hidden[layer][...] = rows[layer][...] + rounded(acc[...])

    def bent(rows_f):
        return jnp.tanh(GELU_C * (rows_f + GELU_D * (rows_f * rows_f * rows_f)))

    def gelu(rows_f, bend):
        return rounded(rows_f * (0.5 * (1.0 + bend)))

    def gelu_slope(rows_f, bend):
        return 0.5 * (1.0 + bend) + (0.5 * GELU_C) * rows_f * (1.0 - bend * bend) * (1.0 + (3.0 * GELU_D) * (rows_f * rows_f))

    def mlp_norm(layer):
        norm_forward(hidden[layer], gain_row(gain_two, layer), unit_rows)
        save('u_two', layer, [put(unit_rows, kept[layer]['u_two'])])
        acc[...] = jnp.zeros_like(acc)

    def mlp_forward(layer):
        mlp_norm(layer)
        flush = planned_flush()

        @pl.loop(0, n_ff)
        def _(at):
            fetch_up(layer, at).wait()
            fetch_down(layer, at).wait()
            pl.when(at == 1)(flush)
            pre[layer][at] = rounded(dot_nn(unit_rows[...], s_up[at]))
            rows_f = wide_float(pre[layer][at])
            act[at] = gelu(rows_f, bent(rows_f))
            acc[...] += dot_nn(act[at], s_down[at])
        save('act', layer, put_blocks(act, kept[layer]['act']))
        rows[layer + 1][...] = hidden[layer][...] + rounded(acc[...])

    def mlp_backward(layer, top):
        if top:
            mlp_norm(layer)
        acc[...] = jnp.zeros_like(acc)
        axis, axis_down = first_axis(1, layer), first_axis(0, layer)
        flush = planned_flush()

        def stream(mat, spot, at):
            line = layer if mat else n_layers
            return pltpu.make_async_remote_copy(
                src_ref=(act, pre[layer])[mat].at[at], dst_ref=from_chip[(mat, layer)][0].at[:, pl.ds(pl.multiple_of(spot * FF_BLOCK, FF_BLOCK), FF_BLOCK)],
                send_sem=sem_out_blocks.at[line, spot], recv_sem=sem_in_blocks.at[line, spot],
                device_id=(to[(axis_down, axis)[mat]],), device_id_type=pl.DeviceIdType.MESH)

        @pl.loop(0, n_ff)
        def _(step):
            at = lax.rem(step + (1 - place[axis]) * (n_ff // 2), n_ff)
            fetch_down(layer, at).wait()
            fetch_up(layer, at).wait()
            pl.when(step == 1)(flush)
            rows_f = wide_float(rounded(dot_nn(unit_rows[...], s_up[at])) if top else pre[layer][at])
            bend = bent(rows_f)
            if top:
                act[at] = gelu(rows_f, bend)
            grad_a = wide_float(rounded(dot_nt(grad[...], s_down[at])))
            pre[layer][at] = rounded(gelu_slope(rows_f, bend) * grad_a)
            acc[...] += dot_nt(pre[layer][at], s_up[at])
            pl.when(step < n_ff // 2)(lambda: stream(1, step, at).start())
            if top:
                pl.when(lax.div(at, n_ff // 2) == 1 - place[axis_down])(lambda: stream(0, lax.rem(at, n_ff // 2), at).start())
        streams.extend(functools.partial(stream, mat, spot, spot) for mat in ((0, 1) if top else (1,)) for spot in range(n_ff // 2))
        if top:
            save('act', layer, put_blocks(act, kept[layer]['act']))
        save('grad_pre', layer, put_blocks(pre[layer], kept[layer]['grad_pre']))
        norm_backward(hidden[layer], gain_row(gain_two, layer), acc, grad, grad_hidden, gain_row(gain_out, n_layers + layer))
        save('grad_hidden', layer, [put(grad_hidden, kept[layer]['grad_hidden'])])

    def attention_backward(layer, fetched):
        acc[...] = jnp.zeros_like(acc)
        flush = planned_flush()

        @pl.loop(0, n_group)
        def _(at):
            if not fetched:
                for piece in fetch_group(layer, at):
                    piece.wait()
            pl.when(at == 1)(flush)
            do_ref[...] = rounded(dot_nt(grad_hidden[...], s_out[at]))
            attend_backward(do_ref, *(qkv[layer].at[which, at] for which in range(3)), k_acc, v_acc)
            for which in range(3):
                acc[...] += dot_nt(qkv[layer][which, at], s_qkv[which, at])
        copies = []
        for which in range(3):
            width = grad.shape[1]
            copies += [put(qkv[layer].at[which, at], kept[layer]['grad_qkv'].at[:, pl.ds(which * width + at * GROUP, GROUP)]) for at in range(n_group)]
        save('grad_qkv', layer, copies)
        norm_backward(rows[layer], gain_row(gain_one, layer), acc, grad_hidden, grad, gain_row(gain_out, layer))

    first = pltpu.make_async_copy(x_in.at[0], rows[0], sem_in.at[0])
    second = pltpu.make_async_copy(grad_in.at[0], grad, sem_in.at[1])
    first.start()
    start_groups(0)
    exchange(0, n_layers - 1, 1)[0]().start()
    gain_out[...] = jnp.zeros_like(gain_out)
    first.wait()
    for layer in range(n_layers):
        attention_forward(layer)
        if layer + 1 < n_layers:
            start_groups(layer + 1)
            mlp_forward(layer)
            start_all(fetch_up, layer + 1)
            start_all(fetch_down, layer + 1)
    second.wait()
    for layer in reversed(range(n_layers)):
        top = layer + 1 == n_layers
        mlp_backward(layer, top)
        if layer > 0:
            start_all(fetch_up, layer - 1)
            start_all(fetch_down, layer - 1)
        attention_backward(layer, top)
        if layer > 0:
            start_groups(layer - 1)
            save('grad', layer - 1, [put(grad, kept[layer - 1]['grad'])])
    done = put(grad, grad_out)
    planned_flush()()
    done.wait()
    for make in sent + streams:
        make().wait()


def compute(x_loc, grad_loc, gain_one, gain_two, w_qkv, w_out, w_up, w_down):
    n_layers, width, inner = w_up.shape
    seq_len = x_loc.shape[1]
    f32, bf16 = jnp.float32, jnp.bfloat16
    n_group, n_ff = width // GROUP, inner // FF_BLOCK
    units = [(mat, layer) for layer in range(n_layers) for mat in range(len(MATRICES))]
    early = [unit for unit in units if unit not in LATE]

    def lo(*shape):
        return jax.ShapeDtypeStruct(shape, bf16)
    outs = [lo(seq_len, width), jax.ShapeDtypeStruct((8, width), f32)]
    outs += [lo(seq_len, cols * width) for _ in range(n_layers) for cols in KEPT.values()]
    shapes = [[KEPT[name] * width for name in FACTORS[mat]] for mat, _ in early]
    outs += [lo(seq_len, shape[MATRICES[mat][2]] // 2) for shape, (mat, _) in zip(shapes, early)]
    outs += [lo(seq_len, shape[1 - MATRICES[mat][2]]) for shape, (mat, _) in zip(shapes, early)]
    wide_rows, groups = (seq_len, width), (n_group, seq_len, GROUP)
    vmem = [wide_rows] * (2 * n_layers) + [(3,) + groups] * n_layers + [(n_ff, seq_len, FF_BLOCK)] * n_layers
    vmem += [wide_rows, groups, (n_ff, seq_len, FF_BLOCK), wide_rows, wide_rows, (seq_len, GROUP)]
    scratch = [pltpu.VMEM(shape, bf16) for shape in vmem] + [pltpu.VMEM(shape, f32) for shape in ((seq_len, GROUP), (seq_len, GROUP), wide_rows)]
    scratch += [pltpu.VMEM(shape, bf16) for shape in ((3, n_group, width, GROUP), (n_group, GROUP, width), (n_ff, width, FF_BLOCK), (n_ff, FF_BLOCK, width))]
    scratch += [pltpu.SemaphoreType.DMA(shape) for shape in ((3, n_group), (n_group,), (n_ff,), (n_ff,), (2,), (100,), (2 * len(early),), (2 * len(early),)) + ((n_layers + 1, n_ff // 2),) * 2]
    hbm, near = pl.BlockSpec(memory_space=pl.ANY), pl.BlockSpec(memory_space=pltpu.VMEM)
    results = pl.pallas_call(
        functools.partial(compute_kernel, n_layers), out_shape=tuple(outs), in_specs=[hbm, hbm, near, near] + [hbm] * 4,
        out_specs=tuple([hbm, near] + [hbm] * (len(outs) - 2)), scratch_shapes=scratch,
        compiler_params=pltpu.CompilerParams(has_side_effects=True, vmem_limit_bytes=VMEM_LIMIT),
    )(x_loc, grad_loc, gain_one, gain_two, w_qkv, w_out, w_up, w_down)
    grad_x, gains = results[:2]
    kept = [dict(zip(KEPT, results[2 + layer * len(KEPT):])) for layer in range(n_layers)]
    kept[-1]['grad'] = grad_loc[0]
    tail = results[2 + n_layers * len(KEPT):]
    from_chip = dict(zip(early, zip(tail, tail[len(early):])))
    operands = []
    for mat, layer in units:
        pair = [kept[layer][name] for name in FACTORS[mat]]
        split = MATRICES[mat][2]
        operands.append((pair[split], pair[1 - split]) + from_chip.get((mat, layer), ()))
    return grad_x, gains, operands


def add_rows(dst, src, cols, scale=None):
    rows = dst.shape[0]

    @pl.loop(0, rows // ADD_ROWS)
    def _(step):
        at = pl.ds(pl.multiple_of(step * ADD_ROWS, ADD_ROWS), ADD_ROWS)
        val = dst[at, cols] + src[at, :]
        dst[at, cols] = val if scale is None else val * scale


def flip(bit, by):
    return 1 - bit if by else bit


def combine_kernel(n_dev, n_layers, *refs):
    units = [(mat, layer) for layer in range(n_layers) for mat in range(len(MATRICES))]
    n_chunk = len(CHUNKS)
    refs = list(refs)

    def take(count):
        head, refs[:] = refs[:count], refs[count:]
        return head

    given = [take(2 if unit in LATE else 4) for unit in units]
    gain_in, = take(1)
    outs, (gain_out,) = take(len(MATRICES)), take(1)
    from_core, part_refs, from_chip = take(2 * len(units)), take(len(units)), take(2 * len(LATE))
    land_q, land_z, land_h = (take(n_chunk) for _ in range(3))
    row_op, col_op, product, stream, gain_buf, gain_land, send_sems, recv_sems, local_sems, stream_sems, gain_send, gain_recv, op_send, op_recv, op_local = refs

    me = lax.axis_index(AXIS)
    place, to, middle, edge = own_place(me)
    core, half = place['core'], place['half']

    def remote(src, dst, i, sem, dev):
        return pltpu.make_async_remote_copy(src_ref=src, dst_ref=dst, send_sem=send_sems.at[i, sem], recv_sem=recv_sems.at[i, sem],
                                            device_id=(dev,), device_id_type=pl.DeviceIdType.MESH)

    def out_block(i, p_at, c_at, row, n_rows, h_at):
        mat, layer, k = CHUNKS[i]
        rows_all, cols, split = MATRICES[mat]
        quarter = p_at * 2 + c_at
        row = row + k * (rows_all // chunk_count(mat, layer)) + (quarter * rows_all if split == 0 else 0)
        col, n_cols = (0, cols) if h_at is None else (h_at * (cols // 2), cols // 2)
        if split == 1:
            col = col + quarter * cols
        return outs[mat].at[layer, pl.ds(pl.multiple_of(row, 8), n_rows), pl.ds(col if isinstance(col, int) else pl.multiple_of(col, 128), n_cols)]

    def stream_add(dst, src):
        rows, cols = dst.shape
        size = min(STREAM_ROWS, rows)
        steps = rows // size

        def fetch(step, slot):
            return pltpu.make_async_copy(src.at[pl.ds(pl.multiple_of(step * size, size), size), :], stream.at[slot, pl.ds(0, size), pl.ds(0, cols)], stream_sems.at[slot])
        fetch(0, 0).start()

        @pl.loop(0, steps)
        def _(step):
            slot = lax.rem(step, 2)

            @pl.when(step + 1 < steps)
            def _():
                fetch(step + 1, 1 - slot).start()
            fetch(step, slot).wait()
            at = pl.ds(pl.multiple_of(step * size, size), size)
            dst[at, :] = dst[at, :] + stream[slot, pl.ds(0, size), pl.ds(0, cols)]

    def run(i, stage, pending):
        mat, layer, k = CHUNKS[i]
        rows_all, cols, _ = MATRICES[mat]
        kind, p_name = KIND[layer][mat], first_axis(mat, layer)
        by_pairs = p_name == 'z'
        q_name = kind.lower() if by_pairs else 'xy'.replace(kind, '')
        r_name = 'xy'.replace(q_name, '')
        rows = rows_all // chunk_count(mat, layer)
        part = part_refs[layer * len(MATRICES) + mat]
        p_at, q_at, r_at = place[p_name], place[q_name], place[r_name]

        def go(src, dst, sem, dest, cond=None):
            remote(src(), dst(), i, sem, to[dest]).start()
            pending.append((cond, src, i, sem))

        def block(dp=0, dq=0, dc=0, dr=None, dh=None):
            def ref():
                row, count = flip(q_at, dq) * (rows // 2), rows // 2
                if dr is not None:
                    row, count = row + flip(r_at, dr) * (rows // 4), rows // 4
                return out_block(i, flip(p_at, dp), flip(core, dc), row, count, None if dh is None else flip(half, dh))
            return ref

        def pass_on(blk, sems, cond=None):
            for dest, sem in sems:
                go(blk, blk, sem, dest, cond)

        def arrived(blk, sem):
            remote(blk(), blk(), i, sem, me).wait_recv()

        def half_cols(by):
            return pl.ds(pl.multiple_of(flip(half, by) * (cols // 2), 128), cols // 2)

        def own_rows(by):
            return land_q[i].at[pl.ds(pl.multiple_of(flip(r_at, by) * (rows // 4), 8), rows // 4), :] if by_pairs else land_q[i]

        def own_half(by):
            return lambda: (land_q[i].at[pl.ds(pl.multiple_of(r_at * (rows // 4), 8), rows // 4), half_cols(by)] if by_pairs
                            else land_q[i].at[:, half_cols(by)])

        def rows_of(by):
            return lambda: part.at[pl.ds(pl.multiple_of(k * rows + flip(q_at, by) * (rows // 2), 8), rows // 2), :]

        last = dict(dr=0) if by_pairs else {}

        def keep():
            return pltpu.make_async_copy(own_half(0)(), block(dh=0, **last)(), local_sems.at[i])

        def whole(buf):
            return lambda: buf[i]

        def scale_and_send(dest):
            add_rows(own_rows(0), land_h[i], half_cols(0), 1.0 / n_dev)
            keep().start()
            go(own_half(0), block(dh=0, **last), 3, dest, None if by_pairs else middle)

        def spread(turn):
            if turn == 0:
                pass_on(block(), ((q_name, 5), (p_name, 6), ('core', 8)))
            elif turn == 1:
                arrived(block(dq=1), 5)
                pass_on(block(dq=1), ((p_name, 7), ('core', 9)))
            else:
                dq = turn - 2
                arrived(block(dp=1, dq=dq), turn + 4)
                pass_on(block(dp=1, dq=dq), (('core', turn + 8),))

        if stage == 0:
            go(rows_of(1), whole(land_q), 0, q_name)
        elif stage == 8:
            for turn in range(4):
                arrived(block(dp=turn // 2, dq=turn % 2, dc=1), 8 + turn)
        elif by_pairs:
            if stage == 1:
                arrived(whole(land_q), 0)
                stream_add(land_q[i], rows_of(0)())
                go(lambda: own_rows(1), whole(land_z), 1, r_name)
            elif stage == 2:
                arrived(whole(land_z), 1)
                add_rows(own_rows(0), land_z[i], slice(None))
                go(own_half(1), whole(land_h), 2, 'far')
            elif stage == 3:
                arrived(whole(land_h), 2)
                scale_and_send('far')
            elif stage == 4:
                keep().wait()
                arrived(block(dr=0, dh=1), 3)
                go(block(dr=0), block(dr=0), 4, r_name)
            else:
                if stage == 5:
                    arrived(block(dr=1), 4)
                spread(min(stage - 5, 3))
        elif stage == 1:
            arrived(whole(land_q), 0)
            stream_add(land_q[i], rows_of(0)())

            @pl.when(edge)
            def _():
                go(whole(land_q), whole(land_z), 1, 'mid', edge)
        elif stage in (2, 3):
            @pl.when(middle)
            def _():
                arrived(whole((land_z, land_h)[stage - 2]), stage - 1)
                if stage == 2:
                    add_rows(land_q[i], land_z[i], slice(None))
                    go(own_half(1), whole(land_h), 2, 'mid', middle)
                else:
                    scale_and_send('mid')
        else:
            if stage == 4:
                @pl.when(middle)
                def _():
                    keep().wait()
                    arrived(block(dh=1), 3)
                    pass_on(block(), (('end', 4),), middle)

                @pl.when(edge)
                def _():
                    arrived(block(), 4)
            spread(stage - 4)

    def unit_sizes(unit):
        rows, cols, split = MATRICES[unit[0]]
        p_name = first_axis(*unit)
        return (rows, cols, p_name, split) + ((rows, cols) if split == 0 else (cols, rows))

    def operand_copy(u, which, src, dst, dest):
        return pltpu.make_async_remote_copy(src_ref=src, dst_ref=dst, send_sem=op_send.at[u, which], recv_sem=op_recv.at[u, which],
                                            device_id=(to[dest],), device_id_type=pl.DeviceIdType.MESH)

    def operand_copies(u):
        unit = units[u]
        rows, cols, p_name, split, wide_w, _ = unit_sizes(unit)
        p_at = place[p_name]
        wide, thin = given[u][:2]
        core_wide, core_thin = from_core[2 * u:2 * u + 2]
        if unit in LATE:
            late = LATE.index(unit)
            chip_wide, chip_thin = from_chip[2 * late:2 * late + 2]
        else:
            chip_wide, chip_thin = given[u][2:]
        first, second = pl.ds(0, SEQ_LEN), pl.ds(SEQ_LEN, SEQ_LEN)

        def lanes(at, count):
            return pl.ds(pl.multiple_of(at, 128), count)
        other = 1 - core
        copies = {
            'own': (operand_copy(u, 0, wide.at[:, lanes((p_at * 2 + other) * wide_w, wide_w)], core_wide.at[first, :], 'core'),
                    operand_copy(u, 1, thin, core_thin.at[first, :], 'core')),
            'next': (operand_copy(u, 2, chip_wide.at[:, lanes(other * wide_w, wide_w)], core_wide.at[second, :], 'core'),
                     operand_copy(u, 3, chip_thin, core_thin.at[second, :], 'core')),
        }
        if unit in LATE:
            copies['chip'] = (operand_copy(u, 4, wide.at[:, lanes((1 - p_at) * 2 * wide_w, 2 * wide_w)], chip_wide, p_name),
                              operand_copy(u, 5, thin, chip_thin, p_name))
        wide_op, thin_op = (row_op, col_op) if split == 0 else (col_op, row_op)
        thin_w = thin.shape[1]
        loads = []
        for start, src in ((0, wide.at[:, lanes((p_at * 2 + core) * wide_w, wide_w)]), (SEQ_LEN, chip_wide.at[:, lanes(core * wide_w, wide_w)]),
                           (2 * SEQ_LEN, core_wide)):
            loads.append((src, wide_op.at[pl.ds(start, src.shape[0]), pl.ds(0, wide_w)]))
        for start, src in ((0, thin), (SEQ_LEN, chip_thin), (2 * SEQ_LEN, core_thin)):
            loads.append((src, thin_op.at[pl.ds(start, src.shape[0]), pl.ds(0, thin_w)]))
        copies['load'] = tuple(pltpu.make_async_copy(src, dst, op_local.at[u, n]) for n, (src, dst) in enumerate(loads))
        return copies

    def start_operands(u):
        copies = operand_copies(u)
        if units[u] in LATE:
            for copy in copies['chip']:
                copy.start()
        for copy in copies['own']:
            copy.start()
        if units[u] not in LATE:
            for copy in copies['next']:
                copy.start()

    def forward_operands(u):
        copies = operand_copies(u)
        for copy in copies['chip']:
            copy.wait_recv()
        for copy in copies['next']:
            copy.start()

    def multiply(u):
        rows, cols, _, _, _, _ = unit_sizes(units[u])
        copies = operand_copies(u)
        for copy in copies['own'] + copies['next']:
            copy.wait_recv()
        for copy in copies['load']:
            copy.start()
        for copy in copies['load']:
            copy.wait()
        tile = min(TILE_ROWS, rows)
        half_w = cols // 2

        @pl.loop(0, rows // tile)
        def _(step):
            at = pl.ds(pl.multiple_of(step * tile, tile), tile)
            for side in range(2):
                lanes = pl.ds(side * half_w, half_w)
                product[at, lanes] = dot_tn(row_op[:, at], col_op[:, lanes])
        store = pltpu.make_async_copy(product.at[pl.ds(0, rows), pl.ds(0, cols)], part_refs[u], op_local.at[u, 6])
        store.start()
        store.wait()

    def finish_operands(u):
        copies = operand_copies(u)
        for copy in copies['own'] + copies['next'] + copies.get('chip', ()):
            copy.wait_send()

    gain_steps = ('core', 'x', 'y', 'z', 'far')

    def gain_copy(step):
        return pltpu.make_async_remote_copy(src_ref=gain_buf.at[step], dst_ref=gain_land.at[step], send_sem=gain_send.at[step],
                                            recv_sem=gain_recv.at[step], device_id=(to[gain_steps[step]],), device_id_type=pl.DeviceIdType.MESH)

    def gain_next(step):
        copy = gain_copy(step)
        copy.wait()
        total = gain_buf[step] + gain_land[step]
        if step + 1 < len(gain_steps):
            gain_buf[step + 1] = total
            gain_copy(step + 1).start()
        else:
            gain_out[...] = total * (1.0 / n_dev)

    pending = []
    gain_buf[0] = gain_in[...]
    step = 0
    first_use = []
    for mat, layer, _ in CHUNKS:
        if units.index((mat, layer)) not in first_use:
            first_use.append(units.index((mat, layer)))
    for u in first_use:
        start_operands(u)
    for count, (letter, digit) in enumerate(zip(*[iter(''.join(ORDER))] * 2)):
        i, stage = ord(letter) - ord('a'), int(digit, 16)
        u = units.index(CHUNKS[i][:2])
        if stage == 9:
            multiply(u)
        elif stage == 10:
            forward_operands(u)
        else:
            run(i, stage, pending)
        if count == 1:
            gain_copy(0).start()
        if count >= 8 and count % 6 == 0 and step < len(gain_steps):
            gain_next(step)
            step += 1
    for u in range(len(units)):
        finish_operands(u)
    for cond, src, i, sem in pending:
        def finish(src=src, i=i, sem=sem):
            remote(src(), src(), i, sem, me).wait_send()
        if cond is None:
            finish()
        else:
            pl.when(cond)(finish)


def combine(operands, gains, n_dev, n_layers):
    f32, bf16 = jnp.float32, jnp.bfloat16
    units = [(mat, layer) for layer in range(n_layers) for mat in range(len(MATRICES))]
    outs = []
    for rows, cols, split in MATRICES:
        outs.append(jax.ShapeDtypeStruct((n_layers, rows * (4 if split == 0 else 1), cols * (4 if split == 1 else 1)), f32))
    outs.append(jax.ShapeDtypeStruct(gains.shape, f32))
    widths = [MATRICES[mat][:2] if MATRICES[mat][2] == 0 else MATRICES[mat][1::-1] for mat, _ in units]
    for wide_w, thin_w in widths:
        outs += [jax.ShapeDtypeStruct((2 * SEQ_LEN, wide_w), bf16), jax.ShapeDtypeStruct((2 * SEQ_LEN, thin_w), bf16)]
    outs += [jax.ShapeDtypeStruct(MATRICES[mat][:2], f32) for mat, _ in units]
    for unit in LATE:
        wide_w, thin_w = widths[units.index(unit)]
        outs += [jax.ShapeDtypeStruct((SEQ_LEN, 2 * wide_w), bf16), jax.ShapeDtypeStruct((SEQ_LEN, thin_w), bf16)]
    sizes = [(MATRICES[mat][0] // chunk_count(mat, layer) // 2, MATRICES[mat][1], first_axis(mat, layer) == 'z') for mat, layer, _ in CHUNKS]
    scratch = [pltpu.VMEM((r, c), f32) for r, c, _ in sizes]
    scratch += [pltpu.VMEM((r // 2 if pairs else r, c), f32) for r, c, pairs in sizes]
    scratch += [pltpu.VMEM((r // 2 if pairs else r, c // 2), f32) for r, c, pairs in sizes]
    n_chunk, n_unit = len(CHUNKS), len(units)
    most_rows, most_cols = max(m[0] for m in MATRICES), max(m[1] for m in MATRICES)
    scratch += [pltpu.VMEM((TOKENS, most_rows), bf16), pltpu.VMEM((TOKENS, most_cols), bf16), pltpu.VMEM((most_rows, most_cols), f32),
                pltpu.VMEM((2, STREAM_ROWS, most_cols), f32),
                pltpu.VMEM((5,) + gains.shape, f32), pltpu.VMEM((5,) + gains.shape, f32),
                pltpu.SemaphoreType.DMA((n_chunk, N_SEMS)), pltpu.SemaphoreType.DMA((n_chunk, N_SEMS)), pltpu.SemaphoreType.DMA((n_chunk,)), pltpu.SemaphoreType.DMA((2,)),
                pltpu.SemaphoreType.DMA((5,)), pltpu.SemaphoreType.DMA((5,)),
                pltpu.SemaphoreType.DMA((n_unit, 6)), pltpu.SemaphoreType.DMA((n_unit, 6)), pltpu.SemaphoreType.DMA((n_unit, 7))]
    hbm, vmem = pl.BlockSpec(memory_space=pl.ANY), pl.BlockSpec(memory_space=pltpu.VMEM)
    flat = [val for group in operands for val in group]
    results = pl.pallas_call(
        functools.partial(combine_kernel, n_dev, n_layers),
        out_shape=tuple(outs),
        in_specs=[hbm] * len(flat) + [vmem],
        out_specs=tuple([hbm] * 4 + [vmem] + [hbm] * (len(outs) - 5)),
        scratch_shapes=scratch,
        compiler_params=pltpu.CompilerParams(has_side_effects=True, vmem_limit_bytes=VMEM_LIMIT),
    )(*flat, gains)
    return results[:5]


def solution(mesh):
    n_dev = mesh.shape[AXIS]

    def local_step(x_loc, grad_y_loc, gain_one, gain_two, w_qkv, w_out, w_up, w_down):
        n_layers = w_qkv.shape[0]
        grad_x, gains, operands = compute(x_loc, grad_y_loc, gain_one, gain_two, w_qkv, w_out, w_up, w_down)
        down, up, out, qkv, gains = combine(operands, gains, n_dev, n_layers)
        return (grad_x[None], gains[:n_layers], gains[n_layers:2 * n_layers], qkv, out, up, down)

    batch_spec = P(AXIS)
    full_spec = P()
    return jax.shard_map(local_step, mesh=mesh, in_specs=(batch_spec, batch_spec) + (full_spec,) * 6, out_specs=(batch_spec,) + (full_spec,) * 6, check_vma=False)
```

```python
import functools

import jax
import jax.numpy as jnp
from jax import lax
from jax.experimental import pallas as pl
from jax.experimental.pallas import tpu as pltpu
from jax.sharding import PartitionSpec as P

NORM_EPS = 1e-6
HEAD_DIM = 64
AXIS = 'data'
CHUNK_UNITS = '1111110000100110012131303120113000003030'
ORDER = (
    'a9d9a0b0c0d0naa1f9e0lab1g9f0a2d1g0c1h0b2a3e1j9i0b3d2f1a4k9d3',
    'c2g1j0b4l9k0e2c3h1l0d4e3i1n9a5m0f2c4a6e4f3b5b6j1g2k1d6n0d5l1',
    'o0g3f4a7p0h2a8c6c5h3m1g4i2q0l2e5e6b7b8k2h4j2i3l3d7d8n1k3f6o1',
    'j3p1r0f5s0i4o2j4t0p2l4k4o3m2p3c7c8q1g5g6m3o4e7m4e8q2p4q3h5h6',
    'n2q4n3n4s1f7i6f8t1r1l5k5s2j5i5s3r2s4t2l6k7r3g7j7t3g8o6o5p5p6',
    'm5r4t4n5h7q6h8m7n7q5k6i7l7i8l8s5s6keo7j6o8k8r6p7m6r5jet5p8t6',
    'n6meq7m8q8j8r7s7r8nes8t7n8t8',
)
VMEM_LIMIT = 63 * 1024 * 1024


MATRICES = ((1024, 1024, 0), (1024, 1024, 1), (256, 1024, 0), (1024, 768, 1))
KIND = ('xyYy', 'xyYX')
LATE = ((2, 0), (3, 0))
SEQ_LEN = 384
TOKENS = 4 * SEQ_LEN
TILE_ROWS = 256
STREAM_ROWS = 64
N_SEMS = 12
ADD_ROWS = 32


def read_chunks(text):
    found = []
    for mat, layer in zip(*[map(int, text)] * 2):
        found.append((mat, layer, sum(chunk[:2] == (mat, layer) for chunk in found)))
    return tuple(found)


CHUNKS = read_chunks(CHUNK_UNITS)


def first_axis(mat, layer):
    kind = KIND[layer][mat]
    return kind if kind in 'xy' else 'z'


def chunk_count(mat, layer):
    return sum(chunk[:2] == (mat, layer) for chunk in CHUNKS)


PAIR = 2 * HEAD_DIM
GROUP = 2 * PAIR
Q_BLOCK = 128
FF_BLOCK = 512
NORM_ROWS = 128
GELU_C = 0.7978845608028654
GELU_D = 0.044715


def dot_with(dims):
    return lambda lhs, rhs: lax.dot_general(lhs, rhs, (dims, ((), ())), preferred_element_type=jnp.float32)


dot_nn, dot_nt, dot_tn = (dot_with(((left,), (right,))) for left, right in ((1, 0), (1, 1), (0, 0)))


def rounded(val):
    return val.astype(jnp.bfloat16)


def wide_float(val):
    return val.astype(jnp.float32)


def row_blocks(count):
    def wrap(body):
        @pl.loop(0, count // NORM_ROWS)
        def _(step):
            body(pl.ds(pl.multiple_of(step * NORM_ROWS, NORM_ROWS), NORM_ROWS))
    return wrap


def inverse_rms(rows_f):
    return lax.rsqrt(jnp.mean(rows_f * rows_f, axis=-1, keepdims=True) + NORM_EPS)


def norm_forward(src, gain, dst):
    @row_blocks(src.shape[0])
    def _(at):
        rows_f = wide_float(src[at, :])
        dst[at, :] = rounded(rows_f * inverse_rms(rows_f) * gain[...])


def norm_backward(src, gain, grad_norm, grad_res, dst, gain_dst):
    gain_dst[...] = jnp.zeros_like(gain_dst)

    @row_blocks(src.shape[0])
    def _(at):
        rows_f = wide_float(src[at, :])
        scale = inverse_rms(rows_f)
        unit = rows_f * scale
        grad = wide_float(rounded(grad_norm[at, :]))
        gain_dst[...] += jnp.sum(grad * unit, axis=0, keepdims=True)
        grad = grad * gain[...]
        grad = scale * (grad - unit * jnp.mean(grad * unit, axis=-1, keepdims=True))
        dst[at, :] = rounded(wide_float(grad_res[at, :]) + grad)


def two_heads(rows):
    first = lax.broadcasted_iota(jnp.int32, rows.shape, 1) < HEAD_DIM
    zero = jnp.zeros_like(rows)
    return jnp.concatenate([jnp.where(first, rows, zero), jnp.where(first, zero, rows)], axis=0)


def one_pair(rows):
    half = rows.shape[0] // 2
    first = lax.broadcasted_iota(jnp.int32, (half, PAIR), 1) < HEAD_DIM
    return jnp.where(first, rows[:half], rows[half:])


def in_step(step, *lists):
    return [step(*args) for args in zip(*lists)]


def softmax_blocks(q_twos, k_all):
    scores = in_step(lambda q_two, k_rows: dot_nt(q_two, k_rows) * HEAD_DIM ** -0.5, q_twos, k_all)
    shape = (2 * Q_BLOCK, Q_BLOCK)
    seen = lax.rem(lax.broadcasted_iota(jnp.int32, shape, 0), Q_BLOCK) >= lax.broadcasted_iota(jnp.int32, shape, 1)

    def masked(score):
        before = score.shape[1] - Q_BLOCK
        last = jnp.where(seen, score[:, before:], -1e30)
        return jnp.concatenate([score[:, :before], last], axis=1) if before else last
    scores = in_step(masked, scores)
    peaks = in_step(lambda score: jnp.max(score, axis=-1, keepdims=True), scores)
    weights = in_step(lambda score, peak: jnp.exp(score - peak), scores, peaks)
    totals = in_step(lambda weight: 1.0 / jnp.sum(weight, axis=-1, keepdims=True), weights)
    return in_step(lambda weight, total: weight * total, weights, totals)


def jobs_of(blocks):
    return [(pl.ds(block * Q_BLOCK, Q_BLOCK), pl.ds(0, (block + 1) * Q_BLOCK), pl.ds(pair * PAIR, PAIR)) for block in blocks for pair in range(GROUP // PAIR)]


def attend(q_ref, k_ref, v_ref, o_ref):
    jobs = jobs_of(range(q_ref.shape[0] // Q_BLOCK))
    probs = softmax_blocks([two_heads(q_ref[rows, lanes]) for rows, _, lanes in jobs], [k_ref[keys, lanes] for _, keys, lanes in jobs])
    results = in_step(lambda prob, job: dot_nn(rounded(prob), v_ref[job[1], job[2]]), probs, jobs)
    for result, (rows, _, lanes) in zip(results, jobs):
        o_ref[rows, lanes] = rounded(one_pair(result))


def attend_backward(do_ref, q_ref, k_ref, v_ref, k_acc, v_acc):
    jobs = jobs_of(reversed(range(q_ref.shape[0] // Q_BLOCK)))
    q_twos, g_twos = ([two_heads(ref[rows, lanes]) for rows, _, lanes in jobs] for ref in (q_ref, do_ref))
    k_rows = [k_ref[keys, lanes] for _, keys, lanes in jobs]
    grad_probs = in_step(lambda g_two, job: dot_nt(g_two, v_ref[job[1], job[2]]), g_twos, jobs)
    probs = softmax_blocks(q_twos, k_rows)
    means = in_step(lambda prob, grad_prob: jnp.sum(prob * grad_prob, axis=-1, keepdims=True), probs, grad_probs)
    grad_s = in_step(lambda prob, grad_prob, mean: rounded(prob * (grad_prob - mean) * HEAD_DIM ** -0.5), probs, grad_probs, means)
    q_grads = in_step(dot_nn, grad_s, k_rows)
    k_parts = in_step(dot_tn, grad_s, q_twos)
    v_parts = in_step(lambda prob, g_two: dot_tn(rounded(prob), g_two), probs, g_twos)
    for q_grad, k_part, v_part, (rows, keys, lanes) in zip(q_grads, k_parts, v_parts, jobs):
        q_ref[rows, lanes] = rounded(one_pair(q_grad))
        if keys.size == q_ref.shape[0]:
            k_acc[:, lanes] = k_part
            v_acc[:, lanes] = v_part
        else:
            k_acc[keys, lanes] += k_part
            v_acc[keys, lanes] += v_part
    k_ref[...] = rounded(k_acc[...])
    v_ref[...] = rounded(v_acc[...])


KEPT = {'u_one': 1, 'mixed': 1, 'u_two': 1, 'act': 4, 'grad_pre': 4, 'grad_hidden': 1, 'grad_qkv': 3, 'grad': 1}
FACTORS = (('act', 'grad'), ('u_two', 'grad_pre'), ('mixed', 'grad_hidden'), ('u_one', 'grad_qkv'))


def own_place(me):
    core, x_at, y_at, z_at = lax.rem(me, 2), lax.rem(lax.div(me, 2), 2), lax.rem(lax.div(me, 4), 2), lax.div(me, 8)
    half = lax.div(z_at, 2)
    place = {'core': core, 'x': x_at, 'y': y_at, 'z': lax.rem(z_at, 2), 'half': half}
    to = {}
    for name, stride in (('core', 1), ('x', 2), ('y', 4), ('z', 8)):
        to[name] = me + stride * (1 - 2 * place[name])
    inward = 8 * (1 - 2 * half)
    to.update(mid=me + inward, end=me - inward, far=me + 2 * inward)
    return place, to, lax.div(z_at + 1, 2) == 1, lax.div(z_at + 1, 2) != 1


def compute_kernel(n_layers, x_in, grad_in, gain_one, gain_two, w_qkv, w_out, w_up, w_down, *refs):
    refs = list(refs)

    def take(count):
        head, refs[:] = refs[:count], refs[count:]
        return head

    grad_out, gain_out = take(2)
    kept = [dict(zip(KEPT, take(len(KEPT)))) for _ in range(n_layers)]
    units = [(mat, layer) for layer in range(n_layers) for mat in range(len(MATRICES))]
    early = [unit for unit in units if unit not in LATE]
    from_chip = dict(zip(early, zip(take(len(early)), take(len(early)))))
    rows, hidden, qkv, pre = (take(n_layers) for _ in range(4))
    unit_rows, mixed, act, grad_hidden, grad, do_ref, k_acc, v_acc, acc, s_qkv, s_out, s_up, s_down = take(13)
    sem_qkv, sem_out, sem_up, sem_down, sem_in, sem_put, sem_send, sem_recv, sem_out_blocks, sem_in_blocks = refs
    place, to, _, _ = own_place(lax.axis_index(AXIS))
    n_group, n_ff = s_out.shape[0], s_up.shape[0]

    def fetch_group(layer, at):
        cols = [pl.ds(pl.multiple_of((which * n_group + at) * GROUP, GROUP), GROUP) for which in range(3)]
        pieces = [pltpu.make_async_copy(w_qkv.at[layer, :, cols[which]], s_qkv.at[which, at], sem_qkv.at[which, at]) for which in range(3)]
        return pieces + [pltpu.make_async_copy(w_out.at[layer, pl.ds(pl.multiple_of(at * GROUP, GROUP), GROUP), :], s_out.at[at], sem_out.at[at])]

    def fetch_up(layer, at):
        return pltpu.make_async_copy(w_up.at[layer, :, pl.ds(pl.multiple_of(at * FF_BLOCK, FF_BLOCK), FF_BLOCK)], s_up.at[at], sem_up.at[at])

    def fetch_down(layer, at):
        return pltpu.make_async_copy(w_down.at[layer, pl.ds(pl.multiple_of(at * FF_BLOCK, FF_BLOCK), FF_BLOCK), :], s_down.at[at], sem_down.at[at])

    def start_groups(layer):
        for at in range(n_group):
            for piece in fetch_group(layer, at):
                piece.start()

    def start_all(fetch, layer):
        for at in range(n_ff):
            fetch(layer, at).start()

    n_put, sent, waiting, streams = [0], [], [], []

    def put(src, dst):
        copy = pltpu.make_async_copy(src, dst, sem_put.at[n_put[0]])
        n_put[0] += 1
        copy.start()
        return copy

    def put_blocks(src, dst):
        count, _, cols = src.shape
        return [put(src.at[at], dst.at[:, pl.ds(at * cols, cols)]) for at in range(count)]

    def exchange(mat, layer, which):
        if (mat, layer) in LATE or (mat, which) == (1, 1) or (mat, layer, which) == (0, n_layers - 1, 0):
            return []
        axis, split = first_axis(mat, layer), MATRICES[mat][2]
        name, order = FACTORS[mat][which], len(sent)

        def make():
            src = grad_in.at[0] if (name, layer) == ('grad', n_layers - 1) else kept[layer][name]
            dst = from_chip[(mat, layer)][which != split]
            if which == split:
                src = src.at[:, pl.ds(pl.multiple_of((1 - place[axis]) * dst.shape[1], 128), dst.shape[1])]
            return pltpu.make_async_remote_copy(src_ref=src, dst_ref=dst, send_sem=sem_send.at[order], recv_sem=sem_recv.at[order],
                                                device_id=(to[axis],), device_id_type=pl.DeviceIdType.MESH)
        sent.append(make)
        return [make]

    def save(name, layer, copies):
        waiting.append((name, layer, copies))

    def planned_flush():
        copies = [copy for _, _, group in waiting for copy in group]
        makes = []
        for name, layer, _ in waiting:
            for mat, names in enumerate(FACTORS):
                if name in names:
                    makes += exchange(mat, layer, names.index(name))
        waiting.clear()

        def run():
            for copy in copies:
                copy.wait()
            for make in makes:
                make().start()
        return run

    def gain_row(gain, layer):
        return gain.at[pl.ds(layer, 1), :]

    def attention_forward(layer):
        norm_forward(rows[layer], gain_row(gain_one, layer), unit_rows)
        save('u_one', layer, [put(unit_rows, kept[layer]['u_one'])])
        acc[...] = jnp.zeros_like(acc)
        flush = planned_flush()
        q_all, k_all, v_all = (qkv[layer].at[which] for which in range(3))

        @pl.loop(0, n_group)
        def _(at):
            for piece in fetch_group(layer, at):
                piece.wait()

            @pl.when(at == 1)
            def _():
                flush()
                if layer == 0:
                    start_all(fetch_up, 0)
                    start_all(fetch_down, 0)
                    second.start()
            for which in range(3):
                qkv[layer][which, at] = rounded(dot_nn(unit_rows[...], s_qkv[which, at]))
            attend(q_all.at[at], k_all.at[at], v_all.at[at], mixed.at[at])
            acc[...] += dot_nn(mixed[at], s_out[at])
        save('mixed', layer, put_blocks(mixed, kept[layer]['mixed']))
        hidden[layer][...] = rows[layer][...] + rounded(acc[...])

    def bent(rows_f):
        return jnp.tanh(GELU_C * (rows_f + GELU_D * (rows_f * rows_f * rows_f)))

    def gelu(rows_f, bend):
        return rounded(rows_f * (0.5 * (1.0 + bend)))

    def gelu_slope(rows_f, bend):
        return 0.5 * (1.0 + bend) + (0.5 * GELU_C) * rows_f * (1.0 - bend * bend) * (1.0 + (3.0 * GELU_D) * (rows_f * rows_f))

    def mlp_norm(layer):
        norm_forward(hidden[layer], gain_row(gain_two, layer), unit_rows)
        save('u_two', layer, [put(unit_rows, kept[layer]['u_two'])])
        acc[...] = jnp.zeros_like(acc)

    def mlp_forward(layer):
        mlp_norm(layer)
        flush = planned_flush()

        @pl.loop(0, n_ff)
        def _(at):
            fetch_up(layer, at).wait()
            fetch_down(layer, at).wait()
            pl.when(at == 1)(flush)
            pre[layer][at] = rounded(dot_nn(unit_rows[...], s_up[at]))
            rows_f = wide_float(pre[layer][at])
            act[at] = gelu(rows_f, bent(rows_f))
            acc[...] += dot_nn(act[at], s_down[at])
        save('act', layer, put_blocks(act, kept[layer]['act']))
        rows[layer + 1][...] = hidden[layer][...] + rounded(acc[...])

    def mlp_backward(layer, top):
        if top:
            mlp_norm(layer)
        acc[...] = jnp.zeros_like(acc)
        axis, axis_down = first_axis(1, layer), first_axis(0, layer)
        flush = planned_flush()

        def stream(mat, spot, at):
            line = layer if mat else n_layers
            return pltpu.make_async_remote_copy(
                src_ref=(act, pre[layer])[mat].at[at], dst_ref=from_chip[(mat, layer)][0].at[:, pl.ds(pl.multiple_of(spot * FF_BLOCK, FF_BLOCK), FF_BLOCK)],
                send_sem=sem_out_blocks.at[line, spot], recv_sem=sem_in_blocks.at[line, spot],
                device_id=(to[(axis_down, axis)[mat]],), device_id_type=pl.DeviceIdType.MESH)

        @pl.loop(0, n_ff)
        def _(step):
            at = lax.rem(step + (1 - place[axis]) * (n_ff // 2), n_ff)
            fetch_down(layer, at).wait()
            fetch_up(layer, at).wait()
            pl.when(step == 1)(flush)
            rows_f = wide_float(rounded(dot_nn(unit_rows[...], s_up[at])) if top else pre[layer][at])
            bend = bent(rows_f)
            if top:
                act[at] = gelu(rows_f, bend)
            grad_a = wide_float(rounded(dot_nt(grad[...], s_down[at])))
            pre[layer][at] = rounded(gelu_slope(rows_f, bend) * grad_a)
            acc[...] += dot_nt(pre[layer][at], s_up[at])
            pl.when(step < n_ff // 2)(lambda: stream(1, step, at).start())
            if top:
                pl.when(lax.div(at, n_ff // 2) == 1 - place[axis_down])(lambda: stream(0, lax.rem(at, n_ff // 2), at).start())
        streams.extend(functools.partial(stream, mat, spot, spot) for mat in ((0, 1) if top else (1,)) for spot in range(n_ff // 2))
        if top:
            save('act', layer, put_blocks(act, kept[layer]['act']))
        save('grad_pre', layer, put_blocks(pre[layer], kept[layer]['grad_pre']))
        norm_backward(hidden[layer], gain_row(gain_two, layer), acc, grad, grad_hidden, gain_row(gain_out, n_layers + layer))
        save('grad_hidden', layer, [put(grad_hidden, kept[layer]['grad_hidden'])])

    def attention_backward(layer, fetched):
        acc[...] = jnp.zeros_like(acc)
        flush = planned_flush()

        @pl.loop(0, n_group)
        def _(at):
            if not fetched:
                for piece in fetch_group(layer, at):
                    piece.wait()
            pl.when(at == 1)(flush)
            do_ref[...] = rounded(dot_nt(grad_hidden[...], s_out[at]))
            attend_backward(do_ref, *(qkv[layer].at[which, at] for which in range(3)), k_acc, v_acc)
            for which in range(3):
                acc[...] += dot_nt(qkv[layer][which, at], s_qkv[which, at])
        copies = []
        for which in range(3):
            width = grad.shape[1]
            copies += [put(qkv[layer].at[which, at], kept[layer]['grad_qkv'].at[:, pl.ds(which * width + at * GROUP, GROUP)]) for at in range(n_group)]
        save('grad_qkv', layer, copies)
        norm_backward(rows[layer], gain_row(gain_one, layer), acc, grad_hidden, grad, gain_row(gain_out, layer))

    first = pltpu.make_async_copy(x_in.at[0], rows[0], sem_in.at[0])
    second = pltpu.make_async_copy(grad_in.at[0], grad, sem_in.at[1])
    first.start()
    start_groups(0)
    exchange(0, n_layers - 1, 1)[0]().start()
    gain_out[...] = jnp.zeros_like(gain_out)
    first.wait()
    for layer in range(n_layers):
        attention_forward(layer)
        if layer + 1 < n_layers:
            start_groups(layer + 1)
            mlp_forward(layer)
            start_all(fetch_up, layer + 1)
            start_all(fetch_down, layer + 1)
    second.wait()
    for layer in reversed(range(n_layers)):
        top = layer + 1 == n_layers
        mlp_backward(layer, top)
        if layer > 0:
            start_all(fetch_up, layer - 1)
            start_all(fetch_down, layer - 1)
        attention_backward(layer, top)
        if layer > 0:
            start_groups(layer - 1)
            save('grad', layer - 1, [put(grad, kept[layer - 1]['grad'])])
    done = put(grad, grad_out)
    planned_flush()()
    done.wait()
    for make in sent + streams:
        make().wait()


def compute(x_loc, grad_loc, gain_one, gain_two, w_qkv, w_out, w_up, w_down):
    n_layers, width, inner = w_up.shape
    seq_len = x_loc.shape[1]
    f32, bf16 = jnp.float32, jnp.bfloat16
    n_group, n_ff = width // GROUP, inner // FF_BLOCK
    units = [(mat, layer) for layer in range(n_layers) for mat in range(len(MATRICES))]
    early = [unit for unit in units if unit not in LATE]

    def lo(*shape):
        return jax.ShapeDtypeStruct(shape, bf16)
    outs = [lo(seq_len, width), jax.ShapeDtypeStruct((8, width), f32)]
    outs += [lo(seq_len, cols * width) for _ in range(n_layers) for cols in KEPT.values()]
    shapes = [[KEPT[name] * width for name in FACTORS[mat]] for mat, _ in early]
    outs += [lo(seq_len, shape[MATRICES[mat][2]] // 2) for shape, (mat, _) in zip(shapes, early)]
    outs += [lo(seq_len, shape[1 - MATRICES[mat][2]]) for shape, (mat, _) in zip(shapes, early)]
    wide_rows, groups = (seq_len, width), (n_group, seq_len, GROUP)
    vmem = [wide_rows] * (2 * n_layers) + [(3,) + groups] * n_layers + [(n_ff, seq_len, FF_BLOCK)] * n_layers
    vmem += [wide_rows, groups, (n_ff, seq_len, FF_BLOCK), wide_rows, wide_rows, (seq_len, GROUP)]
    scratch = [pltpu.VMEM(shape, bf16) for shape in vmem] + [pltpu.VMEM(shape, f32) for shape in ((seq_len, GROUP), (seq_len, GROUP), wide_rows)]
    scratch += [pltpu.VMEM(shape, bf16) for shape in ((3, n_group, width, GROUP), (n_group, GROUP, width), (n_ff, width, FF_BLOCK), (n_ff, FF_BLOCK, width))]
    scratch += [pltpu.SemaphoreType.DMA(shape) for shape in ((3, n_group), (n_group,), (n_ff,), (n_ff,), (2,), (100,), (2 * len(early),), (2 * len(early),)) + ((n_layers + 1, n_ff // 2),) * 2]
    hbm, near = pl.BlockSpec(memory_space=pl.ANY), pl.BlockSpec(memory_space=pltpu.VMEM)
    results = pl.pallas_call(
        functools.partial(compute_kernel, n_layers), out_shape=tuple(outs), in_specs=[hbm, hbm, near, near] + [hbm] * 4,
        out_specs=tuple([hbm, near] + [hbm] * (len(outs) - 2)), scratch_shapes=scratch,
        compiler_params=pltpu.CompilerParams(has_side_effects=True, vmem_limit_bytes=VMEM_LIMIT),
    )(x_loc, grad_loc, gain_one, gain_two, w_qkv, w_out, w_up, w_down)
    grad_x, gains = results[:2]
    kept = [dict(zip(KEPT, results[2 + layer * len(KEPT):])) for layer in range(n_layers)]
    kept[-1]['grad'] = grad_loc[0]
    tail = results[2 + n_layers * len(KEPT):]
    from_chip = dict(zip(early, zip(tail, tail[len(early):])))
    operands = []
    for mat, layer in units:
        pair = [kept[layer][name] for name in FACTORS[mat]]
        split = MATRICES[mat][2]
        operands.append((pair[split], pair[1 - split]) + from_chip.get((mat, layer), ()))
    return grad_x, gains, operands


def add_rows(dst, src, cols, scale=None):
    rows = dst.shape[0]

    @pl.loop(0, rows // ADD_ROWS)
    def _(step):
        at = pl.ds(pl.multiple_of(step * ADD_ROWS, ADD_ROWS), ADD_ROWS)
        val = dst[at, cols] + src[at, :]
        dst[at, cols] = val if scale is None else val * scale


def flip(bit, by):
    return 1 - bit if by else bit


def combine_kernel(n_dev, n_layers, *refs):
    units = [(mat, layer) for layer in range(n_layers) for mat in range(len(MATRICES))]
    n_chunk = len(CHUNKS)
    refs = list(refs)

    def take(count):
        head, refs[:] = refs[:count], refs[count:]
        return head

    given = [take(2 if unit in LATE else 4) for unit in units]
    gain_in, = take(1)
    outs, (gain_out,) = take(len(MATRICES)), take(1)
    from_core, part_refs, from_chip = take(2 * len(units)), take(len(units)), take(2 * len(LATE))
    land_q, land_z, land_h = (take(n_chunk) for _ in range(3))
    row_op, col_op, product, stream, gain_buf, gain_land, send_sems, recv_sems, local_sems, stream_sems, gain_send, gain_recv, op_send, op_recv, op_local = refs

    me = lax.axis_index(AXIS)
    place, to, middle, edge = own_place(me)
    core, half = place['core'], place['half']

    def remote(src, dst, i, sem, dev):
        return pltpu.make_async_remote_copy(src_ref=src, dst_ref=dst, send_sem=send_sems.at[i, sem], recv_sem=recv_sems.at[i, sem],
                                            device_id=(dev,), device_id_type=pl.DeviceIdType.MESH)

    def out_block(i, p_at, c_at, row, n_rows, h_at):
        mat, layer, k = CHUNKS[i]
        rows_all, cols, split = MATRICES[mat]
        quarter = p_at * 2 + c_at
        row = row + k * (rows_all // chunk_count(mat, layer)) + (quarter * rows_all if split == 0 else 0)
        col, n_cols = (0, cols) if h_at is None else (h_at * (cols // 2), cols // 2)
        if split == 1:
            col = col + quarter * cols
        return outs[mat].at[layer, pl.ds(pl.multiple_of(row, 8), n_rows), pl.ds(col if isinstance(col, int) else pl.multiple_of(col, 128), n_cols)]

    def stream_add(dst, src):
        rows, cols = dst.shape
        size = min(STREAM_ROWS, rows)
        steps = rows // size

        def fetch(step, slot):
            return pltpu.make_async_copy(src.at[pl.ds(pl.multiple_of(step * size, size), size), :], stream.at[slot, pl.ds(0, size), pl.ds(0, cols)], stream_sems.at[slot])
        fetch(0, 0).start()

        @pl.loop(0, steps)
        def _(step):
            slot = lax.rem(step, 2)

            @pl.when(step + 1 < steps)
            def _():
                fetch(step + 1, 1 - slot).start()
            fetch(step, slot).wait()
            at = pl.ds(pl.multiple_of(step * size, size), size)
            dst[at, :] = dst[at, :] + stream[slot, pl.ds(0, size), pl.ds(0, cols)]

    def run(i, stage, pending):
        mat, layer, k = CHUNKS[i]
        rows_all, cols, _ = MATRICES[mat]
        kind, p_name = KIND[layer][mat], first_axis(mat, layer)
        by_pairs = p_name == 'z'
        q_name = kind.lower() if by_pairs else 'xy'.replace(kind, '')
        r_name = 'xy'.replace(q_name, '')
        rows = rows_all // chunk_count(mat, layer)
        part = part_refs[layer * len(MATRICES) + mat]
        p_at, q_at, r_at = place[p_name], place[q_name], place[r_name]

        def go(src, dst, sem, dest, cond=None):
            remote(src(), dst(), i, sem, to[dest]).start()
            pending.append((cond, src, i, sem))

        def block(dp=0, dq=0, dc=0, dr=None, dh=None):
            def ref():
                row, count = flip(q_at, dq) * (rows // 2), rows // 2
                if dr is not None:
                    row, count = row + flip(r_at, dr) * (rows // 4), rows // 4
                return out_block(i, flip(p_at, dp), flip(core, dc), row, count, None if dh is None else flip(half, dh))
            return ref

        def pass_on(blk, sems, cond=None):
            for dest, sem in sems:
                go(blk, blk, sem, dest, cond)

        def arrived(blk, sem):
            remote(blk(), blk(), i, sem, me).wait_recv()

        def half_cols(by):
            return pl.ds(pl.multiple_of(flip(half, by) * (cols // 2), 128), cols // 2)

        def own_rows(by):
            return land_q[i].at[pl.ds(pl.multiple_of(flip(r_at, by) * (rows // 4), 8), rows // 4), :] if by_pairs else land_q[i]

        def own_half(by):
            return lambda: (land_q[i].at[pl.ds(pl.multiple_of(r_at * (rows // 4), 8), rows // 4), half_cols(by)] if by_pairs
                            else land_q[i].at[:, half_cols(by)])

        def rows_of(by):
            return lambda: part.at[pl.ds(pl.multiple_of(k * rows + flip(q_at, by) * (rows // 2), 8), rows // 2), :]

        last = dict(dr=0) if by_pairs else {}

        def keep():
            return pltpu.make_async_copy(own_half(0)(), block(dh=0, **last)(), local_sems.at[i])

        def whole(buf):
            return lambda: buf[i]

        def scale_and_send(dest):
            add_rows(own_rows(0), land_h[i], half_cols(0), 1.0 / n_dev)
            keep().start()
            go(own_half(0), block(dh=0, **last), 3, dest, None if by_pairs else middle)

        def spread(turn):
            if turn == 0:
                pass_on(block(), ((q_name, 5), (p_name, 6), ('core', 8)))
            elif turn == 1:
                arrived(block(dq=1), 5)
                pass_on(block(dq=1), ((p_name, 7), ('core', 9)))
            else:
                dq = turn - 2
                arrived(block(dp=1, dq=dq), turn + 4)
                pass_on(block(dp=1, dq=dq), (('core', turn + 8),))

        if stage == 0:
            go(rows_of(1), whole(land_q), 0, q_name)
        elif stage == 8:
            for turn in range(4):
                arrived(block(dp=turn // 2, dq=turn % 2, dc=1), 8 + turn)
        elif by_pairs:
            if stage == 1:
                arrived(whole(land_q), 0)
                stream_add(land_q[i], rows_of(0)())
                go(lambda: own_rows(1), whole(land_z), 1, r_name)
            elif stage == 2:
                arrived(whole(land_z), 1)
                add_rows(own_rows(0), land_z[i], slice(None))
                go(own_half(1), whole(land_h), 2, 'far')
            elif stage == 3:
                arrived(whole(land_h), 2)
                scale_and_send('far')
            elif stage == 4:
                keep().wait()
                arrived(block(dr=0, dh=1), 3)
                go(block(dr=0), block(dr=0), 4, r_name)
            else:
                if stage == 5:
                    arrived(block(dr=1), 4)
                spread(min(stage - 5, 3))
        elif stage == 1:
            arrived(whole(land_q), 0)
            stream_add(land_q[i], rows_of(0)())

            @pl.when(edge)
            def _():
                go(whole(land_q), whole(land_z), 1, 'mid', edge)
        elif stage in (2, 3):
            @pl.when(middle)
            def _():
                arrived(whole((land_z, land_h)[stage - 2]), stage - 1)
                if stage == 2:
                    add_rows(land_q[i], land_z[i], slice(None))
                    go(own_half(1), whole(land_h), 2, 'mid', middle)
                else:
                    scale_and_send('mid')
        else:
            if stage == 4:
                @pl.when(middle)
                def _():
                    keep().wait()
                    arrived(block(dh=1), 3)
                    pass_on(block(), (('end', 4),), middle)

                @pl.when(edge)
                def _():
                    arrived(block(), 4)
            spread(stage - 4)

    def unit_sizes(unit):
        rows, cols, split = MATRICES[unit[0]]
        p_name = first_axis(*unit)
        return (rows, cols, p_name, split) + ((rows, cols) if split == 0 else (cols, rows))

    def operand_copy(u, which, src, dst, dest):
        return pltpu.make_async_remote_copy(src_ref=src, dst_ref=dst, send_sem=op_send.at[u, which], recv_sem=op_recv.at[u, which],
                                            device_id=(to[dest],), device_id_type=pl.DeviceIdType.MESH)

    def operand_copies(u):
        unit = units[u]
        rows, cols, p_name, split, wide_w, _ = unit_sizes(unit)
        p_at = place[p_name]
        wide, thin = given[u][:2]
        core_wide, core_thin = from_core[2 * u:2 * u + 2]
        if unit in LATE:
            late = LATE.index(unit)
            chip_wide, chip_thin = from_chip[2 * late:2 * late + 2]
        else:
            chip_wide, chip_thin = given[u][2:]
        first, second = pl.ds(0, SEQ_LEN), pl.ds(SEQ_LEN, SEQ_LEN)

        def lanes(at, count):
            return pl.ds(pl.multiple_of(at, 128), count)
        other = 1 - core
        copies = {
            'own': (operand_copy(u, 0, wide.at[:, lanes((p_at * 2 + other) * wide_w, wide_w)], core_wide.at[first, :], 'core'),
                    operand_copy(u, 1, thin, core_thin.at[first, :], 'core')),
            'next': (operand_copy(u, 2, chip_wide.at[:, lanes(other * wide_w, wide_w)], core_wide.at[second, :], 'core'),
                     operand_copy(u, 3, chip_thin, core_thin.at[second, :], 'core')),
        }
        if unit in LATE:
            copies['chip'] = (operand_copy(u, 4, wide.at[:, lanes((1 - p_at) * 2 * wide_w, 2 * wide_w)], chip_wide, p_name),
                              operand_copy(u, 5, thin, chip_thin, p_name))
        wide_op, thin_op = (row_op, col_op) if split == 0 else (col_op, row_op)
        thin_w = thin.shape[1]
        loads = []
        for start, src in ((0, wide.at[:, lanes((p_at * 2 + core) * wide_w, wide_w)]), (SEQ_LEN, chip_wide.at[:, lanes(core * wide_w, wide_w)]),
                           (2 * SEQ_LEN, core_wide)):
            loads.append((src, wide_op.at[pl.ds(start, src.shape[0]), pl.ds(0, wide_w)]))
        for start, src in ((0, thin), (SEQ_LEN, chip_thin), (2 * SEQ_LEN, core_thin)):
            loads.append((src, thin_op.at[pl.ds(start, src.shape[0]), pl.ds(0, thin_w)]))
        copies['load'] = tuple(pltpu.make_async_copy(src, dst, op_local.at[u, n]) for n, (src, dst) in enumerate(loads))
        return copies

    def start_operands(u):
        copies = operand_copies(u)
        if units[u] in LATE:
            for copy in copies['chip']:
                copy.start()
        for copy in copies['own']:
            copy.start()
        if units[u] not in LATE:
            for copy in copies['next']:
                copy.start()

    def forward_operands(u):
        copies = operand_copies(u)
        for copy in copies['chip']:
            copy.wait_recv()
        for copy in copies['next']:
            copy.start()

    def multiply(u):
        rows, cols, _, _, _, _ = unit_sizes(units[u])
        copies = operand_copies(u)
        for copy in copies['own'] + copies['next']:
            copy.wait_recv()
        for copy in copies['load']:
            copy.start()
        for copy in copies['load']:
            copy.wait()
        tile = min(TILE_ROWS, rows)
        half_w = cols // 2

        @pl.loop(0, rows // tile)
        def _(step):
            at = pl.ds(pl.multiple_of(step * tile, tile), tile)
            for side in range(2):
                lanes = pl.ds(side * half_w, half_w)
                product[at, lanes] = dot_tn(row_op[:, at], col_op[:, lanes])
        store = pltpu.make_async_copy(product.at[pl.ds(0, rows), pl.ds(0, cols)], part_refs[u], op_local.at[u, 6])
        store.start()
        store.wait()

    def finish_operands(u):
        copies = operand_copies(u)
        for copy in copies['own'] + copies['next'] + copies.get('chip', ()):
            copy.wait_send()

    gain_steps = ('core', 'x', 'y', 'z', 'far')

    def gain_copy(step):
        return pltpu.make_async_remote_copy(src_ref=gain_buf.at[step], dst_ref=gain_land.at[step], send_sem=gain_send.at[step],
                                            recv_sem=gain_recv.at[step], device_id=(to[gain_steps[step]],), device_id_type=pl.DeviceIdType.MESH)

    def gain_next(step):
        copy = gain_copy(step)
        copy.wait()
        total = gain_buf[step] + gain_land[step]
        if step + 1 < len(gain_steps):
            gain_buf[step + 1] = total
            gain_copy(step + 1).start()
        else:
            gain_out[...] = total * (1.0 / n_dev)

    pending = []
    gain_buf[0] = gain_in[...]
    step = 0
    first_use = []
    for mat, layer, _ in CHUNKS:
        if units.index((mat, layer)) not in first_use:
            first_use.append(units.index((mat, layer)))
    for u in first_use:
        start_operands(u)
    for count, (letter, digit) in enumerate(zip(*[iter(''.join(ORDER))] * 2)):
        i, stage = ord(letter) - ord('a'), int(digit, 16)
        u = units.index(CHUNKS[i][:2])
        if stage == 9:
            multiply(u)
        elif stage == 10:
            forward_operands(u)
        else:
            run(i, stage, pending)
        if count == 1:
            gain_copy(0).start()
        if count >= 8 and count % 6 == 0 and step < len(gain_steps):
            gain_next(step)
            step += 1
    for u in range(len(units)):
        finish_operands(u)
    for cond, src, i, sem in pending:
        def finish(src=src, i=i, sem=sem):
            remote(src(), src(), i, sem, me).wait_send()
        if cond is None:
            finish()
        else:
            pl.when(cond)(finish)


def combine(operands, gains, n_dev, n_layers):
    f32, bf16 = jnp.float32, jnp.bfloat16
    units = [(mat, layer) for layer in range(n_layers) for mat in range(len(MATRICES))]
    outs = []
    for rows, cols, split in MATRICES:
        outs.append(jax.ShapeDtypeStruct((n_layers, rows * (4 if split == 0 else 1), cols * (4 if split == 1 else 1)), f32))
    outs.append(jax.ShapeDtypeStruct(gains.shape, f32))
    widths = [MATRICES[mat][:2] if MATRICES[mat][2] == 0 else MATRICES[mat][1::-1] for mat, _ in units]
    for wide_w, thin_w in widths:
        outs += [jax.ShapeDtypeStruct((2 * SEQ_LEN, wide_w), bf16), jax.ShapeDtypeStruct((2 * SEQ_LEN, thin_w), bf16)]
    outs += [jax.ShapeDtypeStruct(MATRICES[mat][:2], f32) for mat, _ in units]
    for unit in LATE:
        wide_w, thin_w = widths[units.index(unit)]
        outs += [jax.ShapeDtypeStruct((SEQ_LEN, 2 * wide_w), bf16), jax.ShapeDtypeStruct((SEQ_LEN, thin_w), bf16)]
    sizes = [(MATRICES[mat][0] // chunk_count(mat, layer) // 2, MATRICES[mat][1], first_axis(mat, layer) == 'z') for mat, layer, _ in CHUNKS]
    scratch = [pltpu.VMEM((r, c), f32) for r, c, _ in sizes]
    scratch += [pltpu.VMEM((r // 2 if pairs else r, c), f32) for r, c, pairs in sizes]
    scratch += [pltpu.VMEM((r // 2 if pairs else r, c // 2), f32) for r, c, pairs in sizes]
    n_chunk, n_unit = len(CHUNKS), len(units)
    most_rows, most_cols = max(m[0] for m in MATRICES), max(m[1] for m in MATRICES)
    scratch += [pltpu.VMEM((TOKENS, most_rows), bf16), pltpu.VMEM((TOKENS, most_cols), bf16), pltpu.VMEM((most_rows, most_cols), f32),
                pltpu.VMEM((2, STREAM_ROWS, most_cols), f32),
                pltpu.VMEM((5,) + gains.shape, f32), pltpu.VMEM((5,) + gains.shape, f32),
                pltpu.SemaphoreType.DMA((n_chunk, N_SEMS)), pltpu.SemaphoreType.DMA((n_chunk, N_SEMS)), pltpu.SemaphoreType.DMA((n_chunk,)), pltpu.SemaphoreType.DMA((2,)),
                pltpu.SemaphoreType.DMA((5,)), pltpu.SemaphoreType.DMA((5,)),
                pltpu.SemaphoreType.DMA((n_unit, 6)), pltpu.SemaphoreType.DMA((n_unit, 6)), pltpu.SemaphoreType.DMA((n_unit, 7))]
    hbm, vmem = pl.BlockSpec(memory_space=pl.ANY), pl.BlockSpec(memory_space=pltpu.VMEM)
    flat = [val for group in operands for val in group]
    results = pl.pallas_call(
        functools.partial(combine_kernel, n_dev, n_layers),
        out_shape=tuple(outs),
        in_specs=[hbm] * len(flat) + [vmem],
        out_specs=tuple([hbm] * 4 + [vmem] + [hbm] * (len(outs) - 5)),
        scratch_shapes=scratch,
        compiler_params=pltpu.CompilerParams(has_side_effects=True, vmem_limit_bytes=VMEM_LIMIT),
    )(*flat, gains)
    return results[:5]


COPY_SLOTS = 8
COPY_AHEAD = COPY_SLOTS // 2
COPY_WORDS = 512 * 1024


def copy_kernel(n_job, *refs):
    count = len(MATRICES)
    pairs, (*slots, in_sems, out_sems) = zip(refs[:count], refs[count:count + count]), refs[count + count:]
    loads, stores, reused, used = [], [], [], {}
    for src, dst in pairs:
        layers, height, cols = src.shape
        slot, = [ref for ref in slots if ref.shape[-1] == cols]
        _, size, _ = slot.shape
        for layer in range(layers):
            for start in range(0, height, size):
                turn = used.setdefault(cols, [])
                at, rows, order = len(turn) % COPY_SLOTS, pl.ds(start, size), len(loads)
                reused.append(turn[-COPY_SLOTS] if len(turn) >= COPY_SLOTS else None)
                turn.append(order)
                loads.append(pltpu.make_async_copy(src.at[layer, rows, :], slot.at[at], in_sems.at[order]))
                stores.append(pltpu.make_async_copy(slot.at[at], dst.at[layer, rows, :], out_sems.at[order]))
    left = set(range(n_job))
    for step in range(n_job + COPY_AHEAD):
        if step < n_job:
            if reused[step] is not None:
                stores[reused[step]].wait()
                left.remove(reused[step])
            loads[step].start()
        if step >= COPY_AHEAD:
            loads[step - COPY_AHEAD].wait()
            stores[step - COPY_AHEAD].start()
    for order in sorted(left):
        stores[order].wait()


def copied(sums):
    rows_of = {val.shape[-1]: COPY_WORDS // val.shape[-1] // PAIR * PAIR for val in sums}
    n_job = sum(val.size // (rows_of[val.shape[-1]] * val.shape[-1]) for val in sums)
    hbm = pl.BlockSpec(memory_space=pl.ANY)
    return pl.pallas_call(
        functools.partial(copy_kernel, n_job), out_shape=tuple(jax.ShapeDtypeStruct(val.shape, val.dtype) for val in sums),
        in_specs=[hbm] * len(sums), out_specs=tuple([hbm] * len(sums)),
        scratch_shapes=[pltpu.VMEM((COPY_SLOTS, rows, width), jnp.float32) for width, rows in rows_of.items()] + [pltpu.SemaphoreType.DMA((n_job,))] * 2,
        compiler_params=pltpu.CompilerParams(vmem_limit_bytes=VMEM_LIMIT))(*sums)


def solution(mesh):
    n_dev = mesh.shape[AXIS]

    def local_step(x_loc, grad_y_loc, gain_one, gain_two, w_qkv, w_out, w_up, w_down):
        n_layers = w_qkv.shape[0]
        grad_x, gains, operands = compute(x_loc, grad_y_loc, gain_one, gain_two, w_qkv, w_out, w_up, w_down)
        *sums, gains = combine(operands, gains, n_dev, n_layers)
        down, up, out, qkv = copied(sums)
        return (grad_x[None], gains[:n_layers], gains[n_layers:2 * n_layers], qkv, out, up, down)

    batch_spec = P(AXIS)
    full_spec = P()
    return jax.shard_map(local_step, mesh=mesh, in_specs=(batch_spec, batch_spec) + (full_spec,) * 6, out_specs=(batch_spec,) + (full_spec,) * 6, check_vma=False)
```
